256 devices in a mesh: case: 8 (over z), gx: 8 (over y, core), gy: 4 (over x).
Axes of the slice: x: 4, y: 4, z: 8, core: 2. Of those that a mesh axis runs over, the one named last changes fastest.
Arguments:
- load: float32 [64, 24, 32, 128], P(('case', 'gx'), 'gy'), parts along dimension 0, may hold values from -4 to 4
- factors: bfloat16 [4, 64, 24, 128, 128], P(None, ('case', 'gx'), 'gy'), parts along dimension 1, may hold values from -6 to 6
- links: int32 [4, 64, 24], P(None, ('case', 'gx'), 'gy'), parts along dimension 1, may hold values from 0 to 1
- shift: float32 [64, 24, 128], P(('case', 'gx'), 'gy'), parts along dimension 0, may hold values from 0.25 to 2.5
Outputs:
- solution: float32 [64, 24, 32, 128], P(('case', 'gx'), 'gy'), parts along dimension 0
- residual: float32 [64, 24, 32, 128], P(('case', 'gx'), 'gy'), parts along dimension 0
The draws below stay inside these ranges and needn't reach their ends.
There are 8 independent parts, one for each index of `case`. The reference program is written for one: setup_inputs(seed, part) draws one part's arguments, and reference() takes and returns one part's arrays. A program takes and returns all parts, laid end to end along the dimension named above; each array names one. Nothing has to cross between parts.
All inputs are finite; a program needn't handle non-finite values.
Results may differ from the reference program's by a relative error of at most 0.008.
Values may be sent and summed in bfloat16 or wider, within the bound.
A program may use at most 64 MiB of HBM per device.

```python
import jax
import jax.numpy as jnp
from jax import lax

B = 128
NBX = 1
NBY = 6
NRHS = 32
ITERS = 8
NX = 8
NY = 24


OFFSETS = ((1, 0), (0, 1), (1, 1), (1, -1))


def displaced(array, step_x, step_y):
    padded = jnp.pad(array, ((1, 1), (1, 1)))
    return padded[1 + step_x:1 + step_x + NX, 1 + step_y:1 + step_y + NY]


def spike_plan(key):
    spike_key = jax.random.fold_in(key, 501)
    shards_x = NX // NBX
    shards_y = NY // NBY
    row_pick = jax.random.randint(jax.random.fold_in(spike_key, 1), (shards_x, shards_y), 0, NBX)
    column_pick = jax.random.randint(jax.random.fold_in(spike_key, 2), (shards_x, shards_y), 0, NBY - 1)
    active = jax.random.randint(jax.random.fold_in(spike_key, 3), (shards_x, shards_y), 0, 4)

    def expand(values):
        return jnp.repeat(jnp.repeat(values, NBX, axis=0), NBY, axis=1)
    local_x = jnp.arange(NX, dtype=jnp.int32) % NBX
    local_y = jnp.arange(NY, dtype=jnp.int32) % NBY
    chosen = (expand(active) > 0) & (local_x[:, None] == expand(row_pick)) & (local_y[None, :] == expand(column_pick))
    anchor = chosen.astype(jnp.int32)
    partner = displaced(anchor, 0, -1)
    marked = jnp.maximum(anchor, partner)
    return (anchor, marked)


def draw_load(key, part):
    sample = jax.random.normal(jax.random.fold_in(key, 11), (NX, NY, NRHS, B), jnp.float32)
    sample = jnp.clip(sample, -4.0, 4.0)
    return sample


def draw_links(key, part):
    anchor, marked = spike_plan(key)
    coupled = (jax.random.randint(jax.random.fold_in(key, 23), (4, NX, NY), 0, 4) > 0).astype(jnp.int32)
    touches = jnp.stack([jnp.maximum(marked, displaced(marked, step_x, step_y)) for step_x, step_y in OFFSETS])
    kept = coupled * (1 - touches)
    empty = jnp.zeros((NX, NY), jnp.int32)
    spiked = jnp.stack([empty, anchor, empty, empty])
    return jnp.maximum(kept, spiked).astype(jnp.int32)


def draw_factors(key, part):
    anchor, marked = spike_plan(key)
    noise = jax.random.normal(jax.random.fold_in(key, 37), (4, NX, NY, B, B), jnp.float32)
    noise = jnp.clip(noise, -6.0, 6.0)
    left = jax.random.randint(jax.random.fold_in(key, 43), (NX, NY, B), 0, 2).astype(jnp.float32) * 2.0 - 1.0
    right = jax.random.randint(jax.random.fold_in(key, 47), (NX, NY, B), 0, 2).astype(jnp.float32) * 2.0 - 1.0
    weight = 4.0 * anchor.astype(jnp.float32)[:, :, None, None]
    spike = weight * left[:, :, :, None] * right[:, :, None, :]
    noise = noise.at[1].add(spike)
    return jnp.clip(noise, -6.0, 6.0).astype(jnp.bfloat16)


def draw_shift(key, part):
    anchor, marked = spike_plan(key)
    values = jax.random.uniform(jax.random.fold_in(key, 41), (NX, NY, B), jnp.float32, 0.25, 2.5)
    return jnp.where(marked[:, :, None] > 0, 0.5, values).astype(jnp.float32)


def setup_inputs(seed: int = 0, part: int = 0) -> dict:
    arg_keys = jax.random.split(jax.random.key(seed), 5)
    own_keys = jax.random.split(jax.random.fold_in(arg_keys[4], part), 5)
    return {
        "load": draw_load(jax.random.fold_in(jax.random.fold_in(arg_keys[4], part), 71), part),
        "factors": draw_factors(jax.random.fold_in(jax.random.fold_in(arg_keys[4], part), 71), part),
        "links": draw_links(jax.random.fold_in(jax.random.fold_in(arg_keys[4], part), 71), part),
        "shift": draw_shift(jax.random.fold_in(jax.random.fold_in(arg_keys[4], part), 71), part),
    }


OFFSETS = ((1, 0), (0, 1), (1, 1), (1, -1))
PRECISE = lax.Precision.HIGHEST

def neighbour(array, step_x, step_y):
    count_x, count_y = (array.shape[0], array.shape[1])
    widths = ((1, 1), (1, 1)) + ((0, 0),) * (array.ndim - 2)
    padded = jnp.pad(array, widths)
    return padded[1 + step_x:1 + step_x + count_x, 1 + step_y:1 + step_y + count_y]

def apply_block(block, field):
    return jnp.einsum('xyab,xyrb->xyra', block.astype(jnp.float32), field.astype(jnp.float32), precision=PRECISE, preferred_element_type=jnp.float32)

def inner(left, right):
    return jnp.sum(left * right, axis=(0, 1, 3))

def spread(values):
    return values[None, None, :, None]

def reference(load, factors, links, shift):
    masked = factors.astype(jnp.float32) * links.astype(jnp.float32)[:, :, :, None, None]
    springs = jnp.einsum('dxyak,dxybk->dxyab', masked.astype(jnp.float32), masked.astype(jnp.float32), precision=PRECISE, preferred_element_type=jnp.float32) / B
    forward = [springs[offset] for offset in range(4)]
    backward = [neighbour(springs[offset], -OFFSETS[offset][0], -OFFSETS[offset][1]) for offset in range(4)]
    identity = jnp.eye(B, dtype=jnp.float32)
    diagonal = shift[..., None] * identity + sum(forward) + sum(backward)
    flat = diagonal.reshape(-1, B, B)
    lower = jnp.linalg.cholesky(flat)
    inverse = jax.vmap(lambda factor: jax.scipy.linalg.cho_solve((factor, True), identity))(lower).reshape(diagonal.shape)

    def operate(field):
        result = apply_block(diagonal, field)
        for offset in range(4):
            step_x, step_y = OFFSETS[offset]
            result = result - apply_block(forward[offset], neighbour(field, step_x, step_y))
            result = result - apply_block(backward[offset], neighbour(field, -step_x, -step_y))
        return result
    solution = jnp.zeros_like(load)
    residual = load
    precon = apply_block(inverse, residual)
    direction = precon
    rz_now = inner(residual, precon)
    for iteration in range(ITERS):
        image = operate(direction)
        alpha = rz_now / inner(direction, image)
        solution = solution + spread(alpha) * direction
        residual = residual - spread(alpha) * image
        precon = apply_block(inverse, residual)
        rz_next = inner(residual, precon)
        direction = precon + spread(rz_next / rz_now) * direction
        rz_now = rz_next
    return (solution, residual)
```

```python
import functools

import jax
import jax.numpy as jnp
from jax import lax
from jax.experimental import pallas as pl
from jax.experimental.pallas import tpu as pltpu
from jax.sharding import PartitionSpec as P

B = 128
N = 6
R = 32
ITERS = 8
NB = 8
ST = 136
GXN = 8
GYN = 4
PLANE = GXN * GYN
OFFSETS = ((1, 0), (0, 1), (1, 1), (1, -1))
SIDES = ((1, 0), (-1, 0), (0, 1), (0, -1), (1, 1), (1, -1), (-1, 1), (-1, -1))
f32 = jnp.float32
bf16 = jnp.bfloat16


def split3(x):
    a = x.astype(bf16)
    left = x - a.astype(f32)
    b = left.astype(bf16)
    c = (left - b.astype(f32)).astype(bf16)
    return a, b, c


def split2(x):
    a = x.astype(bf16)
    return a, (x - a.astype(f32)).astype(bf16)


def invert(mats):
    lane = lax.broadcasted_iota(jnp.int32, (8, B), 1)
    full_lane = lax.broadcasted_iota(jnp.int32, (B, B), 1)
    full_row = lax.broadcasted_iota(jnp.int32, (B, B), 0)

    def step(b, carry):
        base = b * NB
        rows = [mats[pl.ds(base + i, 8, stride=ST), :] for i in range(NB)]
        e = {}
        for j in range(NB):
            for i in range(j + 1):
                e[i, j] = jnp.sum(jnp.where(lane == base + j, rows[i], 0.0), axis=1, keepdims=True)
        at = lambda i, j: e[min(i, j), max(i, j)]
        for k in range(NB):
            p = 1.0 / e[k, k]
            col = [at(i, k) for i in range(NB)]
            scaled = [c * p for c in col]
            for i in range(NB):
                for j in range(i, NB):
                    if i != k and j != k:
                        e[i, j] = e[i, j] - scaled[i] * col[j]
            for i in range(NB):
                if i != k:
                    e[min(i, k), max(i, k)] = scaled[i]
            e[k, k] = -p
        inside = (lane >= base) & (lane < base + NB)
        sign = jnp.where(lane < base, -1.0, jnp.where(inside, 0.0, 1.0))
        panel = [jnp.where(lane == base + i, 1.0, jnp.where(inside, 0.0, rows[i])) for i in range(NB)]
        cols = []
        for m in range(N):
            cols.append(split3(mats[pl.ds(pl.multiple_of(m * ST + base, 8), 8), :] * sign))
        for j in range(NB):
            total = None
            for i in range(NB):
                term = at(i, j) * panel[i]
                total = term if total is None else total + term
            mats[pl.ds(base + j, 8, stride=ST), :] = -total
        clear = (full_lane >= base) & (full_lane < base + NB) & ((full_row < base) | (full_row >= base + NB))
        for m in range(N):
            r0, r1, r2 = split3(mats[pl.ds(pl.multiple_of(m * ST + base, 8), 8), :])
            c0, c1, c2 = cols[m]
            left = jnp.concatenate([c0, c0, c1, c1, c0, c2], axis=0)
            right = jnp.concatenate([r0, r1, r0, r1, r2, r0], axis=0)
            update = lax.dot_general(left, right, (((0,), (0,)), ((), ())), preferred_element_type=f32)
            span = pl.ds(m * ST, B)
            mats[span, :] = jnp.where(clear, 0.0, mats[span, :]) - update
        return carry

    lax.fori_loop(0, B // NB, step, 0)


def kernel(links, load, factors, shift, x_out, r_out, fac, rem, lm, rlm, mats, wts, pre, ext,
           res, dirn, along, img, dsend, drecv, lsem, fsend, frecv, hsend, hrecv, ssend, srecv):
    case = lax.axis_index("case")
    gx = lax.axis_index("gx")
    gy = lax.axis_index("gy")
    me = gx * GYN + gy

    def device(x, y):
        return (case, x, y)

    def exists(sx, sy):
        ok = None
        for pos, step, count in ((gx, sx, GXN), (gy, sy, GYN)):
            if step == 0:
                continue
            here = (pos + step >= 0) & (pos + step < count)
            ok = here if ok is None else ok & here
        return ok

    mine = pltpu.make_async_copy(factors, fac, lsem.at[0])
    mine.start()
    loaded = pltpu.make_async_copy(load, res, lsem.at[1])
    loaded.start()

    barrier = pltpu.get_barrier_semaphore()
    ext[...] = jnp.zeros_like(ext)
    rem[...] = jnp.zeros_like(rem)
    rlm[...] = jnp.zeros_like(rlm)
    for d in range(4):
        for j in range(N):
            lm[d * N + j : d * N + j + 1, :] = jnp.full((1, B), links[d, 0, j], jnp.int32).astype(f32) * (1.0 / B)

    peers = []
    for k in range(1, PLANE):
        q = lax.rem(me + k, PLANE)
        peers.append(device(q // GYN, lax.rem(q, GYN)))
    for peer in peers:
        pl.semaphore_signal(barrier, inc=1, device_id=peer, device_id_type=pl.DeviceIdType.MESH)
    pl.semaphore_wait(barrier, PLANE - 1)
    mine.wait()

    def remote(src, dst, ss, rs, sx, sy):
        return pltpu.make_async_remote_copy(
            src_ref=src, dst_ref=dst, send_sem=ss, recv_sem=rs,
            device_id=device(gx + sx, gy + sy), device_id_type=pl.DeviceIdType.MESH)

    moves = (
        (1, 0, ((0, 6, 0), (12, 5, 7), (19, 5, 12)), 0),
        (1, 1, ((17, 1, 6),), 1),
        (1, -1, ((18, 1, 17),), 2),
        (0, 1, ((11, 1, 18),), 3),
    )

    def rim_copies(sx, sy, blocks, n):
        copies = []
        for i, (src, count, dst) in enumerate(blocks):
            copies.append(remote(fac.at[pl.ds(src, count)], rem.at[pl.ds(dst, count)],
                                 fsend.at[n * 4 + i], frecv.at[n * 4 + i], sx, sy))
        copies.append(remote(lm, rlm.at[n], fsend.at[n * 4 + 3], frecv.at[n * 4 + 3], sx, sy))
        return copies

    for sx, sy, blocks, n in moves:
        @pl.when(exists(sx, sy))
        def _():
            for copy in rim_copies(sx, sy, blocks, n):
                copy.start()

    def square(block):
        return lax.dot_general(block, block, (((1,), (1,)), ((), ())), preferred_element_type=f32)

    def place(j, slot, s):
        a, b = split2(s)
        wts[j, slot * B : (slot + 1) * B, 0:B] = a
        wts[j, slot * B : (slot + 1) * B, B : 2 * B] = b

    row_id = lax.broadcasted_iota(jnp.int32, (B, B), 0)
    lane_id = lax.broadcasted_iota(jnp.int32, (B, B), 1)
    eye = row_id == lane_id

    def diag_at(j):
        return pl.ds(pl.multiple_of(j * ST, 8), B)

    for m in range(N):
        mats[m * ST : m * ST + B, :] = jnp.where(eye, shift[0, m : m + 1, :], 0.0)
    for m in range(N, 8):
        mats[m * ST : m * ST + B, :] = jnp.where(eye, 1.0, 0.0)

    def own(j, carry):
        total = mats[diag_at(j), :]
        for d in range(4):
            s = square(fac[d * N + j]) * lm[pl.ds(d * N + j, 1), :]
            place(j, d, s)
            total = total + s
            if d == 1:
                after = lax.rem(j + 1, N)
                place(after, 5, s)
                keep = jnp.where(j < N - 1, 1.0, 0.0)
                mats[diag_at(after), :] = mats[diag_at(after), :] + s * keep
        mats[diag_at(j), :] = total
        return carry

    lax.fori_loop(0, N, own, 0)

    for sx, sy, blocks, n in moves:
        @pl.when(exists(-sx, -sy))
        def _():
            for copy in rim_copies(sx, sy, blocks, n):
                copy.wait_recv()

    def theirs(j, carry):
        total = mats[diag_at(j), :]
        s = square(rem[j]) * rlm[0, pl.ds(j, 1), :]
        place(j, 4, s)
        total = total + s
        before = rlm[0, pl.ds(2 * N + jnp.maximum(j - 1, 0), 1), :]
        corner = rlm[1, pl.ds(2 * N + N - 1, 1), :]
        s = square(rem[N + j]) * jnp.where(j == 0, corner, before)
        place(j, 6, s)
        total = total + s
        after = rlm[0, pl.ds(3 * N + jnp.minimum(j + 1, N - 1), 1), :]
        corner = rlm[2, pl.ds(3 * N, 1), :]
        s = square(rem[2 * N + j]) * jnp.where(j == N - 1, corner, after)
        place(j, 7, s)
        mats[diag_at(j), :] = total + s
        return carry

    lax.fori_loop(0, N, theirs, 0)
    s = square(rem[3 * N]) * rlm[3, pl.ds(N + N - 1, 1), :]
    place(0, 5, s)
    mats[0:B, :] = mats[0:B, :] + s

    invert(mats)
    for m in range(N):
        a, b, c = split3(mats[m * ST : m * ST + B, :])
        pre[m, 0:B, 0:B] = a
        pre[m, 0:B, B : 2 * B] = b
        pre[m, B : 2 * B, 0:B] = c
        pre[m, B : 2 * B, B : 2 * B] = jnp.zeros((B, B), bf16)

    for sx, sy, blocks, n in moves:
        @pl.when(exists(sx, sy))
        def _():
            for copy in rim_copies(sx, sy, blocks, n):
                copy.wait_send()

    loaded.wait()
    x_out[...] = jnp.zeros_like(x_out)
    dirn[...] = jnp.zeros_like(dirn)
    along[...] = jnp.zeros_like(along)

    def fold(out):
        small = (out[64:96, 0:B] + out[64:96, B:]) + out[32:64, B:]
        return out[0:32, 0:B] + (out[32:64, 0:B] + (out[0:32, B:] + small))

    def precondition(v, m):
        a, b, c = split3(v)
        left = jnp.concatenate(
            [jnp.concatenate([t, t], axis=1) for t in (a, b, c)], axis=0)
        return fold(jnp.dot(left, pre[m], preferred_element_type=f32))

    def operate(par, j):
        centre = ext[par, 1, 1 + j]
        terms = []
        for sign in (1, -1):
            for sx, sy in OFFSETS:
                terms.append(split3(centre - ext[par, 1 + sign * sx, 1 + j + sign * sy]))
        left = jnp.concatenate(
            [jnp.concatenate([t[i] for t in terms], axis=1) for i in range(3)], axis=0)
        out = fold(jnp.dot(left, wts[j], preferred_element_type=f32))
        return out + shift[0, j : j + 1, :] * centre

    def halo(par):
        for n, (sx, sy) in enumerate(SIDES):
            if sy == 0:
                src = ext.at[par, 1, pl.ds(1, N)]
                dst = ext.at[par, 1 - sx, pl.ds(1, N)]
            else:
                src = ext.at[par, 1, N if sy == 1 else 1]
                dst = ext.at[par, 1 - sx, 0 if sy == 1 else N + 1]
            yield sx, sy, remote(src, dst, hsend.at[n], hrecv.at[par, n], sx, sy)

    lane = lax.broadcasted_iota(jnp.int32, (R, B), 1)
    rhs = lax.broadcasted_iota(jnp.int32, (R, B), 0)

    def iterate(it, carry):
        gamma_old, alpha_old = carry
        par = lax.rem(it, 2)
        for j in range(N):
            ext[par, 1, 1 + j] = precondition(res[0, j], j)
        for sx, sy, copy in halo(par):
            pl.when(exists(sx, sy))(copy.start)
        for sx, sy, copy in halo(par):
            pl.when(exists(-sx, -sy))(copy.wait_recv)
        gsum, dsum = None, None
        for j in range(N):
            w = operate(par, j)
            img[j] = w
            u = ext[par, 1, 1 + j]
            g, d = u * res[0, j], u * w
            gsum = g if gsum is None else gsum + g
            dsum = d if dsum is None else dsum + d
        gcol = jnp.sum(gsum, axis=1, keepdims=True)
        dcol = jnp.sum(dsum, axis=1, keepdims=True)
        spread = jnp.where(lane == rhs, gcol, jnp.where(lane == rhs + R, dcol, 0.0))
        row = jnp.sum(spread, axis=0, keepdims=True)
        dsend[pl.ds(par, 1), :] = row
        drecv[par, pl.ds(me, 1), :] = row

        def contribution(peer):
            return pltpu.make_async_remote_copy(
                src_ref=dsend.at[pl.ds(par, 1)], dst_ref=drecv.at[par, pl.ds(me, 1)],
                send_sem=ssend, recv_sem=srecv.at[par],
                device_id=peer, device_id_type=pl.DeviceIdType.MESH)

        for peer in peers:
            contribution(peer).start()
        everything = drecv.at[par, pl.ds(0, PLANE - 1)]
        pltpu.make_async_copy(everything, everything, srecv.at[par]).wait()
        pltpu.make_async_copy(everything, everything, ssend).wait()
        total = jnp.sum(drecv[par], axis=0, keepdims=True)
        gamma = jnp.sum(jnp.where(lane == rhs, total, 0.0), axis=1, keepdims=True)
        delta = jnp.sum(jnp.where(lane == rhs + R, total, 0.0), axis=1, keepdims=True)
        ratio = jnp.where(it == 0, 0.0, gamma / gamma_old)
        alpha = gamma / (delta - ratio * gamma / alpha_old)
        for j in range(N):
            p = ext[par, 1, 1 + j] + ratio * dirn[j]
            s = img[j] + ratio * along[j]
            dirn[j] = p
            along[j] = s
            x_out[0, j] = x_out[0, j] + alpha * p
            res[0, j] = res[0, j] - alpha * s
        for sx, sy, copy in halo(par):
            pl.when(exists(sx, sy))(copy.wait_send)
        return gamma, alpha

    one = jnp.ones((R, 1), f32)
    lax.fori_loop(0, ITERS, iterate, (one, one))
    r_out[...] = res[...]


def local(load, factors, links, shift):
    vmem = pl.BlockSpec(memory_space=pltpu.VMEM)
    anywhere = pl.BlockSpec(memory_space=pl.ANY)
    field = jax.ShapeDtypeStruct((1, N, R, B), f32)
    return pl.pallas_call(
        kernel,
        out_shape=(field, field),
        in_specs=[pl.BlockSpec(memory_space=pltpu.SMEM), anywhere, anywhere, vmem],
        out_specs=(vmem, vmem),
        scratch_shapes=[
            pltpu.VMEM((4 * N, B, B), bf16),
            pltpu.VMEM((3 * N + 1, B, B), bf16),
            pltpu.VMEM((4 * N, B), f32),
            pltpu.VMEM((4, 4 * N, B), f32),
            pltpu.VMEM((8 * ST, B), f32),
            pltpu.VMEM((N, 8 * B, 2 * B), bf16),
            pltpu.VMEM((N, 2 * B, 2 * B), bf16),
            pltpu.VMEM((2, 3, N + 2, R, B), f32),
            pltpu.VMEM((1, N, R, B), f32),
            pltpu.VMEM((N, R, B), f32),
            pltpu.VMEM((N, R, B), f32),
            pltpu.VMEM((N, R, B), f32),
            pltpu.VMEM((8, B), f32),
            pltpu.VMEM((2, PLANE, B), f32),
            pltpu.SemaphoreType.DMA((2,)),
            pltpu.SemaphoreType.DMA((16,)),
            pltpu.SemaphoreType.DMA((16,)),
            pltpu.SemaphoreType.DMA((8,)),
            pltpu.SemaphoreType.DMA((2, 8)),
            pltpu.SemaphoreType.DMA,
            pltpu.SemaphoreType.DMA((2,)),
        ],
        compiler_params=pltpu.CompilerParams(collective_id=0, has_side_effects=True),
        name="solve",
    )(links, load, factors.reshape(4 * N, B, B), shift)


def solution(mesh):
    placed = (
        P(("case", "gx"), "gy", None, None),
        P(None, ("case", "gx"), "gy", None, None),
        P(None, ("case", "gx"), "gy"),
        P(("case", "gx"), "gy", None),
    )
    return jax.shard_map(
        local,
        mesh=mesh,
        in_specs=placed,
        out_specs=(P(("case", "gx"), "gy", None, None), P(("case", "gx"), "gy", None, None)),
        check_vma=False,
    )
```

```python
import functools

import jax
import jax.numpy as jnp
from jax import lax
from jax.experimental import pallas as pl
from jax.experimental.pallas import tpu as pltpu
from jax.sharding import PartitionSpec as P

B = 128
N = 6
R = 32
ITERS = 8
NB = 8
ST = 136
GXN = 8
GYN = 4
PLANE = GXN * GYN
OFFSETS = ((1, 0), (0, 1), (1, 1), (1, -1))
SIDES = ((1, 1), (1, -1), (-1, 1), (-1, -1), (1, 0), (-1, 0), (0, 1), (0, -1))
f32 = jnp.float32
bf16 = jnp.bfloat16


def split3(x):
    a = x.astype(bf16)
    left = x - a.astype(f32)
    b = left.astype(bf16)
    c = (left - b.astype(f32)).astype(bf16)
    return a, b, c


def split2(x):
    a = x.astype(bf16)
    return a, (x - a.astype(f32)).astype(bf16)


def invert(mats):
    lane = lax.broadcasted_iota(jnp.int32, (8, B), 1)
    full_lane = lax.broadcasted_iota(jnp.int32, (B, B), 1)
    full_row = lax.broadcasted_iota(jnp.int32, (B, B), 0)

    def step(b, carry):
        base = b * NB
        rows = [mats[pl.ds(base + i, 8, stride=ST), :] for i in range(NB)]
        e = {}
        for j in range(NB):
            for i in range(j + 1):
                e[i, j] = jnp.sum(jnp.where(lane == base + j, rows[i], 0.0), axis=1, keepdims=True)
        at = lambda i, j: e[min(i, j), max(i, j)]
        for k in range(NB):
            p = 1.0 / e[k, k]
            col = [at(i, k) for i in range(NB)]
            scaled = [c * p for c in col]
            for i in range(NB):
                for j in range(i, NB):
                    if i != k and j != k:
                        e[i, j] = e[i, j] - scaled[i] * col[j]
            for i in range(NB):
                if i != k:
                    e[min(i, k), max(i, k)] = scaled[i]
            e[k, k] = -p
        inside = (lane >= base) & (lane < base + NB)
        sign = jnp.where(lane < base, -1.0, jnp.where(inside, 0.0, 1.0))
        panel = [jnp.where(lane == base + i, 1.0, jnp.where(inside, 0.0, rows[i])) for i in range(NB)]
        cols = []
        for m in range(N):
            cols.append(split3(mats[pl.ds(pl.multiple_of(m * ST + base, 8), 8), :] * sign))
        for j in range(NB):
            total = None
            for i in range(NB):
                term = at(i, j) * panel[i]
                total = term if total is None else total + term
            mats[pl.ds(base + j, 8, stride=ST), :] = -total
        clear = (full_lane >= base) & (full_lane < base + NB) & ((full_row < base) | (full_row >= base + NB))
        for m in range(N):
            r0, r1, r2 = split3(mats[pl.ds(pl.multiple_of(m * ST + base, 8), 8), :])
            c0, c1, c2 = cols[m]
            left = jnp.concatenate([c0, c0, c1, c1, c0, c2], axis=0)
            right = jnp.concatenate([r0, r1, r0, r1, r2, r0], axis=0)
            update = lax.dot_general(left, right, (((0,), (0,)), ((), ())), preferred_element_type=f32)
            span = pl.ds(m * ST, B)
            mats[span, :] = jnp.where(clear, 0.0, mats[span, :]) - update
        return carry

    lax.fori_loop(0, B // NB, step, 0)


def kernel(links, load, factors, shift, x_out, r_out, fac, rem, lm, rlm, mats, wts, pre, ext,
           field, push, res, dirn, along, img, dsend, drecv, lsem, fsend, frecv, hsend, hrecv, ssend, srecv):
    case = lax.axis_index("case")
    gx = lax.axis_index("gx")
    gy = lax.axis_index("gy")
    me = gx * GYN + gy

    def device(x, y):
        return (case, x, y)

    def exists(sx, sy):
        ok = None
        for pos, step, count in ((gx, sx, GXN), (gy, sy, GYN)):
            if step == 0:
                continue
            here = (pos + step >= 0) & (pos + step < count)
            ok = here if ok is None else ok & here
        return ok

    mine = pltpu.make_async_copy(factors, fac, lsem.at[0])
    mine.start()
    loaded = pltpu.make_async_copy(load, res, lsem.at[1])
    loaded.start()

    barrier = pltpu.get_barrier_semaphore()
    ext[...] = jnp.zeros_like(ext)
    rem[...] = jnp.zeros_like(rem)
    rlm[...] = jnp.zeros_like(rlm)
    for d in range(4):
        for j in range(N):
            lm[d * N + j : d * N + j + 1, :] = jnp.full((1, B), links[d, 0, j], jnp.int32).astype(f32) * (1.0 / B)

    peers = []
    for k in range(1, PLANE):
        q = lax.rem(me + k, PLANE)
        peers.append(device(q // GYN, lax.rem(q, GYN)))
    for peer in peers:
        pl.semaphore_signal(barrier, inc=1, device_id=peer, device_id_type=pl.DeviceIdType.MESH)
    pl.semaphore_wait(barrier, PLANE - 1)
    mine.wait()

    def remote(src, dst, ss, rs, sx, sy):
        return pltpu.make_async_remote_copy(
            src_ref=src, dst_ref=dst, send_sem=ss, recv_sem=rs,
            device_id=device(gx + sx, gy + sy), device_id_type=pl.DeviceIdType.MESH)

    moves = (
        (1, 0, ((0, 6, 0), (12, 5, 7), (19, 5, 12)), 0),
        (1, 1, ((17, 1, 6),), 1),
        (1, -1, ((18, 1, 17),), 2),
        (0, 1, ((11, 1, 18),), 3),
    )

    def rim_copies(sx, sy, blocks, n):
        copies = []
        for i, (src, count, dst) in enumerate(blocks):
            copies.append(remote(fac.at[pl.ds(src, count)], rem.at[pl.ds(dst, count)],
                                 fsend.at[n * 4 + i], frecv.at[n * 4 + i], sx, sy))
        copies.append(remote(lm, rlm.at[n], fsend.at[n * 4 + 3], frecv.at[n * 4 + 3], sx, sy))
        return copies

    for sx, sy, blocks, n in moves:
        @pl.when(exists(sx, sy))
        def _():
            for copy in rim_copies(sx, sy, blocks, n):
                copy.start()

    def square(block):
        return lax.dot_general(block, block, (((1,), (1,)), ((), ())), preferred_element_type=f32)

    def place(j, slot, s):
        a, b = split2(s)
        wts[j, slot * B : (slot + 1) * B, 0:B] = a
        wts[j, slot * B : (slot + 1) * B, B : 2 * B] = b
        return a.astype(f32) + b.astype(f32)

    row_id = lax.broadcasted_iota(jnp.int32, (B, B), 0)
    lane_id = lax.broadcasted_iota(jnp.int32, (B, B), 1)
    eye = row_id == lane_id

    def diag_at(j):
        return pl.ds(pl.multiple_of(j * ST, 8), B)

    for m in range(N):
        mats[m * ST : m * ST + B, :] = jnp.where(eye, shift[m], 0.0)
    for m in range(N, 8):
        mats[m * ST : m * ST + B, :] = jnp.where(eye, 1.0, 0.0)

    def own(j, carry):
        total = mats[diag_at(j), :]
        for d in range(4):
            s = square(fac[d * N + j]) * lm[pl.ds(d * N + j, 1), :]
            s = place(j, d, s)
            total = total + s
            if d == 1:
                after = lax.rem(j + 1, N)
                place(after, 5, s)
                keep = jnp.where(j < N - 1, 1.0, 0.0)
                mats[diag_at(after), :] = mats[diag_at(after), :] + s * keep
        mats[diag_at(j), :] = total
        return carry

    lax.fori_loop(0, N, own, 0)

    for sx, sy, blocks, n in moves:
        @pl.when(exists(-sx, -sy))
        def _():
            for copy in rim_copies(sx, sy, blocks, n):
                copy.wait_recv()

    def theirs(j, carry):
        total = mats[diag_at(j), :]
        s = square(rem[j]) * rlm[0, pl.ds(j, 1), :]
        s = place(j, 4, s)
        total = total + s
        before = rlm[0, pl.ds(2 * N + jnp.maximum(j - 1, 0), 1), :]
        corner = rlm[1, pl.ds(2 * N + N - 1, 1), :]
        s = square(rem[N + j]) * jnp.where(j == 0, corner, before)
        s = place(j, 6, s)
        total = total + s
        after = rlm[0, pl.ds(3 * N + jnp.minimum(j + 1, N - 1), 1), :]
        corner = rlm[2, pl.ds(3 * N, 1), :]
        s = square(rem[2 * N + j]) * jnp.where(j == N - 1, corner, after)
        s = place(j, 7, s)
        mats[diag_at(j), :] = total + s
        return carry

    lax.fori_loop(0, N, theirs, 0)
    s = square(rem[3 * N]) * rlm[3, pl.ds(N + N - 1, 1), :]
    s = place(0, 5, s)
    mats[0:B, :] = mats[0:B, :] + s

    invert(mats)
    for m in range(N):
        a, b, c = split3(mats[m * ST : m * ST + B, :].T)
        pre[m, 0:B, 0:B] = a
        pre[m, 0:B, B : 2 * B] = b
        pre[m, B : 2 * B, 0:B] = c
        pre[m, B : 2 * B, B : 2 * B] = jnp.zeros((B, B), bf16)

    for sx, sy, blocks, n in moves:
        @pl.when(exists(sx, sy))
        def _():
            for copy in rim_copies(sx, sy, blocks, n):
                copy.wait_send()

    loaded.wait()
    x_out[...] = jnp.zeros_like(x_out)
    dirn[...] = jnp.zeros_like(dirn)
    along[...] = jnp.zeros_like(along)
    push[...] = jnp.zeros_like(push)

    def fold(out):
        small = (out[64:96, 0:B] + out[64:96, B:]) + out[32:64, B:]
        return out[0:32, 0:B] + (out[32:64, 0:B] + (out[0:32, B:] + small))

    def precondition(v, m):
        a, b, c = split3(v)
        left = jnp.concatenate(
            [jnp.concatenate([t, t], axis=1) for t in (a, b, c)], axis=0)
        return fold(jnp.dot(left, pre[m], preferred_element_type=f32))

    def operate(j):
        centre = field[1, 1 + j]
        terms = []
        for sign in (1, -1):
            for sx, sy in OFFSETS:
                terms.append(split3(centre - field[1 + sign * sx, 1 + j + sign * sy]))
        left = jnp.concatenate(
            [jnp.concatenate([t[i] for t in terms], axis=1) for i in range(3)], axis=0)
        out = fold(jnp.dot(left, wts[j], preferred_element_type=f32))
        return out + shift[j] * centre

    def halo(par):
        for n, (sx, sy) in enumerate(SIDES):
            if sy == 0:
                src = ext.at[par, 1, pl.ds(1, N)]
                dst = ext.at[par, 1 - sx, pl.ds(1, N)]
            else:
                src = ext.at[par, 1, N if sy == 1 else 1]
                dst = ext.at[par, 1 - sx, 0 if sy == 1 else N + 1]
            yield sx, sy, remote(src, dst, hsend.at[n], hrecv.at[par, n], sx, sy)

    def halo_start(par):
        for sx, sy, copy in halo(par):
            pl.when(exists(sx, sy))(copy.start)

    def halo_wait(par):
        for sx, sy, copy in halo(par):
            pl.when(exists(-sx, -sy))(copy.wait_recv)

    def halo_sent(par):
        for sx, sy, copy in halo(par):
            pl.when(exists(sx, sy))(copy.wait_send)

    lane = lax.broadcasted_iota(jnp.int32, (R, B), 1)
    rhs = lax.broadcasted_iota(jnp.int32, (R, B), 0)

    def contribution(par, peer):
        return pltpu.make_async_remote_copy(
            src_ref=dsend.at[pl.ds(par, 1)], dst_ref=drecv.at[par, pl.ds(me, 1)],
            send_sem=ssend, recv_sem=srecv.at[par],
            device_id=peer, device_id_type=pl.DeviceIdType.MESH)

    def products(par):
        gsum, dsum = None, None
        for j in range(N):
            w = operate(j)
            img[j] = w
            u = field[1, 1 + j]
            g, d = u * res[0, j], u * w
            gsum = g if gsum is None else gsum + g
            dsum = d if dsum is None else dsum + d
        gcol = jnp.sum(gsum, axis=1, keepdims=True)
        dcol = jnp.sum(dsum, axis=1, keepdims=True)
        spread = jnp.where(lane == rhs, gcol, jnp.where(lane == rhs + R, dcol, 0.0))
        row = jnp.sum(spread, axis=0, keepdims=True)
        dsend[pl.ds(par, 1), :] = row
        drecv[par, pl.ds(me, 1), :] = row
        for peer in peers:
            contribution(par, peer).start()

    def totals(par, first, gamma_old, alpha_old):
        everything = drecv.at[par, pl.ds(0, PLANE - 1)]
        pltpu.make_async_copy(everything, everything, srecv.at[par]).wait()
        pltpu.make_async_copy(everything, everything, ssend).wait()
        total = jnp.sum(drecv[par], axis=0, keepdims=True)
        gamma = jnp.sum(jnp.where(lane == rhs, total, 0.0), axis=1, keepdims=True)
        delta = jnp.sum(jnp.where(lane == rhs + R, total, 0.0), axis=1, keepdims=True)
        ratio = jnp.where(first, 0.0, gamma / gamma_old)
        alpha = gamma / (delta - ratio * gamma / alpha_old)
        return gamma, ratio, alpha

    def advance(j, ratio, alpha):
        p = field[1, 1 + j] + ratio * dirn[j]
        s = img[j] + ratio * along[j]
        return p, s, x_out[0, j] + alpha * p, res[0, j] - alpha * s

    for j in range(N):
        ext[1, 1, 1 + j] = precondition(res[0, j], j)
    halo_start(1)
    halo_wait(1)
    field[...] = ext[1]
    halo_sent(1)

    def iterate(it, carry):
        gamma_old, alpha_old = carry
        par = lax.rem(it, 2)
        products(par)
        for j in range(N):
            ext[par, 1, 1 + j] = precondition(img[j], j)
        halo_start(par)
        gamma, ratio, alpha = totals(par, it == 0, gamma_old, alpha_old)
        for j in range(N):
            dirn[j], along[j], x_out[0, j], res[0, j] = advance(j, ratio, alpha)
        halo_wait(par)
        for a in range(3):
            for c in range(N + 2):
                q = ext[par, a, c] + ratio * push[a, c]
                push[a, c] = q
                field[a, c] = field[a, c] - alpha * q
        halo_sent(par)
        return gamma, alpha

    one = jnp.ones((R, 1), f32)
    gamma_old, alpha_old = lax.fori_loop(0, ITERS - 1, iterate, (one, one))
    last = (ITERS - 1) % 2
    products(last)
    gamma, ratio, alpha = totals(last, ITERS == 1, gamma_old, alpha_old)
    for j in range(N):
        _, _, x_out[0, j], r_out[0, j] = advance(j, ratio, alpha)


def local(load, factors, links, shift):
    vmem = pl.BlockSpec(memory_space=pltpu.VMEM)
    anywhere = pl.BlockSpec(memory_space=pl.ANY)
    field = jax.ShapeDtypeStruct((1, N, R, B), f32)
    return pl.pallas_call(
        kernel,
        out_shape=(field, field),
        in_specs=[pl.BlockSpec(memory_space=pltpu.SMEM), anywhere, anywhere, vmem],
        out_specs=(vmem, vmem),
        scratch_shapes=[
            pltpu.VMEM((4 * N, B, B), bf16),
            pltpu.VMEM((3 * N + 1, B, B), bf16),
            pltpu.VMEM((4 * N, B), f32),
            pltpu.VMEM((4, 4 * N, B), f32),
            pltpu.VMEM((8 * ST, B), f32),
            pltpu.VMEM((N, 8 * B, 2 * B), bf16),
            pltpu.VMEM((N, 2 * B, 2 * B), bf16),
            pltpu.VMEM((2, 3, N + 2, R, B), f32),
            pltpu.VMEM((3, N + 2, R, B), f32),
            pltpu.VMEM((3, N + 2, R, B), f32),
            pltpu.VMEM((1, N, R, B), f32),
            pltpu.VMEM((N, R, B), f32),
            pltpu.VMEM((N, R, B), f32),
            pltpu.VMEM((N, R, B), f32),
            pltpu.VMEM((8, B), f32),
            pltpu.VMEM((2, PLANE, B), f32),
            pltpu.SemaphoreType.DMA((2,)),
            pltpu.SemaphoreType.DMA((16,)),
            pltpu.SemaphoreType.DMA((16,)),
            pltpu.SemaphoreType.DMA((8,)),
            pltpu.SemaphoreType.DMA((2, 8)),
            pltpu.SemaphoreType.DMA,
            pltpu.SemaphoreType.DMA((2,)),
        ],
        compiler_params=pltpu.CompilerParams(collective_id=0, has_side_effects=True),
        name="solve",
    )(links, load, factors.reshape(4 * N, B, B), shift.reshape(N, 1, B))


def solution(mesh):
    placed = (
        P(("case", "gx"), "gy", None, None),
        P(None, ("case", "gx"), "gy", None, None),
        P(None, ("case", "gx"), "gy"),
        P(("case", "gx"), "gy", None),
    )
    return jax.shard_map(
        local,
        mesh=mesh,
        in_specs=placed,
        out_specs=(P(("case", "gx"), "gy", None, None), P(("case", "gx"), "gy", None, None)),
        check_vma=False,
    )
```

```python
import functools

import jax
import jax.numpy as jnp
from jax import lax
from jax.experimental import pallas as pl
from jax.experimental.pallas import tpu as pltpu
from jax.sharding import PartitionSpec as P

B = 128
N = 6
R = 32
ITERS = 8
NB = 8
ST = 136
GXN = 8
GYN = 4
PLANE = GXN * GYN
OFFSETS = ((1, 0), (0, 1), (1, 1), (1, -1))
SIDES = ((1, 1), (1, -1), (-1, 1), (-1, -1), (1, 0), (-1, 0), (0, 1), (0, -1))
f32 = jnp.float32
bf16 = jnp.bfloat16


def split3(x):
    a = x.astype(bf16)
    left = x - a.astype(f32)
    b = left.astype(bf16)
    c = (left - b.astype(f32)).astype(bf16)
    return a, b, c


def split2(x):
    a = x.astype(bf16)
    return a, (x - a.astype(f32)).astype(bf16)


def invert(mats, rpan):
    lane = lax.broadcasted_iota(jnp.int32, (8, B), 1)
    def step(b, carry):
        base = b * NB
        rows = [mats[pl.ds(base + i, 8, stride=ST), :] for i in range(NB)]
        inside = (lane >= base) & (lane < base + NB)
        sign = jnp.where(lane < base, -1.0, jnp.where(inside, 0.0, 1.0))
        cols = []
        for m in range(N):
            c0, c1, c2 = split3(mats[pl.ds(pl.multiple_of(m * ST + base, 8), 8), :] * sign)
            cols.append(jnp.concatenate([c0, c0, c1, c1, c0, c2], axis=0))
        e = {}
        for j in range(NB):
            for i in range(j + 1):
                e[i, j] = jnp.sum(jnp.where(lane == base + j, rows[i], 0.0), axis=1, keepdims=True)
        at = lambda i, j: e[min(i, j), max(i, j)]
        for k in range(NB):
            p = 1.0 / e[k, k]
            col = [at(i, k) for i in range(NB)]
            scaled = [c * p for c in col]
            for i in range(NB):
                for j in range(i, NB):
                    if i != k and j != k:
                        e[i, j] = e[i, j] - scaled[i] * col[j]
            for i in range(NB):
                if i != k:
                    e[min(i, k), max(i, k)] = scaled[i]
            e[k, k] = -p
        panel = [jnp.where(lane == base + i, 1.0, jnp.where(inside, 0.0, rows[i])) for i in range(NB)]
        for j in range(NB):
            total = None
            for i in range(NB):
                term = at(i, j) * panel[i]
                total = term if total is None else total + term
            rpan[pl.ds(j, 8, stride=NB), :] = -total
        ups = []
        for m in range(N):
            r0, r1, r2 = split3(rpan[m * NB : (m + 1) * NB, :])
            right = jnp.concatenate([r0, r1, r0, r1, r2, r0], axis=0)
            ups.append(lax.dot_general(cols[m], right, (((0,), (0,)), ((), ())), preferred_element_type=f32))
        new = [jnp.where(inside[0:1, :], 0.0, mats[m * ST : m * ST + B, :]) - ups[m] for m in range(N)]
        for m in range(N):
            mats[m * ST : m * ST + B, :] = new[m]
        for m in range(N):
            mats[pl.ds(pl.multiple_of(m * ST + base, 8), 8), :] = rpan[m * NB : (m + 1) * NB, :]
        return carry
    lax.fori_loop(0, B // NB, step, 0)


def kernel(links_in, load, factors, shift_in, x_out, r_out, links, shift, fac, rem, lm, rlm, mats, rpan, dpan, wts, pre, ext,
           field, push, res, dirn, along, img, dsend, drecv, lsem, fsend, frecv, hsend, hrecv, ssend, srecv):
    case = lax.axis_index("case")
    gx = lax.axis_index("gx")
    gy = lax.axis_index("gy")
    me = gx * GYN + gy

    def device(x, y):
        return (case, x, y)

    def exists(sx, sy):
        ok = None
        for pos, step, count in ((gx, sx, GXN), (gy, sy, GYN)):
            if step == 0:
                continue
            here = (pos + step >= 0) & (pos + step < count)
            ok = here if ok is None else ok & here
        return ok

    barrier = pltpu.get_barrier_semaphore()
    peers = []
    for a in (4, 3, 5, 2, 6, 1, 7, 0):
        for c in (2, 1, 3, 0):
            if a or c:
                peers.append(device(lax.rem(gx + a, GXN), lax.rem(gy + c, GYN)))

    ext[...] = jnp.zeros_like(ext)
    rem[...] = jnp.zeros_like(rem)
    rlm[...] = jnp.zeros_like(rlm)
    for peer in peers:
        pl.semaphore_signal(barrier, inc=1, device_id=peer, device_id_type=pl.DeviceIdType.MESH)
    copies = [
        pltpu.make_async_copy(factors, fac, lsem.at[0]),
        pltpu.make_async_copy(links_in, links, lsem.at[1]),
        pltpu.make_async_copy(shift_in, shift, lsem.at[2]),
        pltpu.make_async_copy(load, res, lsem.at[3]),
    ]
    for copy in copies:
        copy.start()
    copies[1].wait()
    for d in range(4):
        for j in range(N):
            lm[d * N + j : d * N + j + 1, :] = jnp.full((1, B), links[d, 0, j], jnp.int32).astype(f32) * (1.0 / B)
    copies[0].wait()
    pl.semaphore_wait(barrier, PLANE - 1)

    def remote(src, dst, ss, rs, sx, sy):
        return pltpu.make_async_remote_copy(
            src_ref=src, dst_ref=dst, send_sem=ss, recv_sem=rs,
            device_id=device(gx + sx, gy + sy), device_id_type=pl.DeviceIdType.MESH)

    moves = (
        (1, 1, ((17, 1, 6),), 1),
        (1, -1, ((18, 1, 17),), 2),
        (0, 1, ((11, 1, 18),), 3),
        (1, 0, ((0, 6, 0), (12, 5, 7), (19, 5, 12)), 0),
    )

    def rim_copies(sx, sy, blocks, n, low=0, high=4):
        parts = [(lm, rlm.at[n], n * 4 + 3)]
        for i, (src, count, dst) in enumerate(blocks):
            parts.append((fac.at[pl.ds(src, count)], rem.at[pl.ds(dst, count)], n * 4 + i))
        return [remote(src, dst, fsend.at[i], frecv.at[i], sx, sy) for src, dst, i in parts[low:high]]

    for sx, sy, blocks, n in moves:
        @pl.when(exists(sx, sy))
        def _():
            for copy in rim_copies(sx, sy, blocks, n):
                copy.start()

    copies[2].wait()

    def square(block):
        return lax.dot_general(block, block, (((1,), (1,)), ((), ())), preferred_element_type=f32)

    def place(j, slot, s):
        a, b = split2(s)
        wts[j, slot * B : (slot + 1) * B, 0:B] = a
        wts[j, slot * B : (slot + 1) * B, B : 2 * B] = b
        return a.astype(f32) + b.astype(f32)

    row_id = lax.broadcasted_iota(jnp.int32, (B, B), 0)
    lane_id = lax.broadcasted_iota(jnp.int32, (B, B), 1)
    eye = row_id == lane_id

    def diag_at(j):
        return pl.ds(pl.multiple_of(j * ST, 8), B)

    for m in range(N):
        mats[m * ST : m * ST + B, :] = jnp.where(eye, shift[m], 0.0)
    for m in range(N, 8):
        mats[m * ST : m * ST + B, :] = jnp.where(eye, 1.0, 0.0)

    def own(j, carry):
        total = mats[diag_at(j), :]
        for d in range(4):
            s = square(fac[d * N + j]) * lm[pl.ds(d * N + j, 1), :]
            s = place(j, d, s)
            total = total + s
            if d == 1:
                after = lax.rem(j + 1, N)
                place(after, 5, s)
                keep = jnp.where(j < N - 1, 1.0, 0.0)
                mats[diag_at(after), :] = mats[diag_at(after), :] + s * keep
        mats[diag_at(j), :] = total
        return carry

    lax.fori_loop(0, N, own, 0)

    def arrived(n, low, high):
        sx, sy, blocks, _ = moves[n]
        @pl.when(exists(-sx, -sy))
        def _():
            for copy in rim_copies(*moves[n], low, high):
                copy.wait_recv()

    def term(j, slot, block, scale):
        return j, place(j, slot, square(rem[block]) * scale)

    def collect(terms):
        for j, s in terms:
            mats[j * ST : j * ST + B, :] = mats[j * ST : j * ST + B, :] + s

    arrived(0, 0, 2)
    arrived(1, 0, 2)
    arrived(2, 0, 2)
    collect([
        term(0, 6, N, rlm[1, 3 * N - 1 : 3 * N, :]),
        term(N - 1, 7, 3 * N - 1, rlm[2, 3 * N : 3 * N + 1, :]),
        term(0, 5, 3 * N, rlm[3, 2 * N - 1 : 2 * N, :]),
    ])
    arrived(3, 0, 2)
    collect([term(j, 4, j, rlm[0, j : j + 1, :]) for j in range(N)])
    arrived(3, 2, 3)
    collect([term(j, 6, N + j, rlm[0, 2 * N + j - 1 : 2 * N + j, :]) for j in range(1, N)])
    arrived(3, 3, 4)
    collect([term(j, 7, 2 * N + j, rlm[0, 3 * N + j + 1 : 3 * N + j + 2, :]) for j in range(N - 1)])

    for m in range(N):
        a, b, c = split3(mats[m * ST : m * ST + B, :])
        dpan[m, 0:B, 0:B] = a
        dpan[m, 0:B, B : 2 * B] = b
        dpan[m, B : 2 * B, 0:B] = c
        dpan[m, B : 2 * B, B : 2 * B] = jnp.zeros((B, B), bf16)
    invert(mats, rpan)

    def pairs(terms):
        return jnp.concatenate([jnp.concatenate([t, t], axis=1) for t in terms], axis=0)

    def fold(out, h):
        small = (out[2 * h :, 0:B] + out[2 * h :, B:]) + out[h : 2 * h, B:]
        return out[0:h, 0:B] + (out[h : 2 * h, 0:B] + (out[0:h, B:] + small))

    better = []
    for m in range(N):
        inv = mats[m * ST : m * ST + B, :]
        terms = split3(inv)
        product = fold(jnp.dot(pairs(terms), dpan[m], preferred_element_type=f32), B)
        error = (jnp.where(eye, 1.0, 0.0) - product).astype(bf16)
        fix = jnp.dot(error, jnp.concatenate(terms[0:2], axis=1), preferred_element_type=f32)
        better.append(inv + (fix[:, 0:B] + fix[:, B:]))
    for m in range(N):
        a, b, c = split3(better[m])
        pre[m, 0:B, 0:B] = a
        pre[m, 0:B, B : 2 * B] = b
        pre[m, B : 2 * B, 0:B] = c
        pre[m, B : 2 * B, B : 2 * B] = jnp.zeros((B, B), bf16)

    for sx, sy, blocks, n in moves:
        @pl.when(exists(sx, sy))
        def _():
            for copy in rim_copies(sx, sy, blocks, n):
                copy.wait_send()

    copies[3].wait()
    x_out[...] = jnp.zeros_like(x_out)
    dirn[...] = jnp.zeros_like(dirn)
    along[...] = jnp.zeros_like(along)
    push[...] = jnp.zeros_like(push)

    def precondition(v, m):
        return fold(jnp.dot(pairs(split3(v)), pre[m], preferred_element_type=f32), R)

    def operate(j):
        centre = field[1, 1 + j]
        terms = []
        for sign in (1, -1):
            for sx, sy in OFFSETS:
                terms.append(split3(centre - field[1 + sign * sx, 1 + j + sign * sy]))
        left = jnp.concatenate(
            [jnp.concatenate([t[i] for t in terms], axis=1) for i in range(3)], axis=0)
        out = fold(jnp.dot(left, wts[j], preferred_element_type=f32), R)
        return out + shift[j] * centre

    def halo(par):
        for n, (sx, sy) in enumerate(SIDES):
            if sy == 0:
                src = ext.at[par, 1, pl.ds(1, N)]
                dst = ext.at[par, 1 - sx, pl.ds(1, N)]
            else:
                src = ext.at[par, 1, N if sy == 1 else 1]
                dst = ext.at[par, 1 - sx, 0 if sy == 1 else N + 1]
            yield sx, sy, remote(src, dst, hsend.at[n], hrecv.at[par, n], sx, sy)

    def halo_start(par):
        for sx, sy, copy in halo(par):
            pl.when(exists(sx, sy))(copy.start)

    def halo_wait(par):
        for sx, sy, copy in halo(par):
            pl.when(exists(-sx, -sy))(copy.wait_recv)

    def halo_sent(par):
        for sx, sy, copy in halo(par):
            pl.when(exists(sx, sy))(copy.wait_send)

    lane = lax.broadcasted_iota(jnp.int32, (R, B), 1)
    rhs = lax.broadcasted_iota(jnp.int32, (R, B), 0)

    def contribution(par, peer):
        return pltpu.make_async_remote_copy(
            src_ref=dsend.at[pl.ds(par, 1)], dst_ref=drecv.at[par, pl.ds(me, 1)],
            send_sem=ssend, recv_sem=srecv.at[par],
            device_id=peer, device_id_type=pl.DeviceIdType.MESH)

    def products(par):
        gsum, dsum = None, None
        for j in range(N):
            w = operate(j)
            img[j] = w
            u = field[1, 1 + j]
            g, d = u * res[0, j], u * w
            gsum = g if gsum is None else gsum + g
            dsum = d if dsum is None else dsum + d
        gcol = jnp.sum(gsum, axis=1, keepdims=True)
        dcol = jnp.sum(dsum, axis=1, keepdims=True)
        spread = jnp.where(lane == rhs, gcol, jnp.where(lane == rhs + R, dcol, 0.0))
        row = jnp.sum(spread, axis=0, keepdims=True)
        dsend[pl.ds(par, 1), :] = row
        drecv[par, pl.ds(me, 1), :] = row
        for peer in peers:
            contribution(par, peer).start()

    def totals(par, first, gamma_old, alpha_old):
        everything = drecv.at[par, pl.ds(0, PLANE - 1)]
        pltpu.make_async_copy(everything, everything, srecv.at[par]).wait()
        pltpu.make_async_copy(everything, everything, ssend).wait()
        total = jnp.sum(drecv[par], axis=0, keepdims=True)
        gamma = jnp.sum(jnp.where(lane == rhs, total, 0.0), axis=1, keepdims=True)
        delta = jnp.sum(jnp.where(lane == rhs + R, total, 0.0), axis=1, keepdims=True)
        ratio = jnp.where(first, 0.0, gamma / gamma_old)
        alpha = gamma / (delta - ratio * gamma / alpha_old)
        return gamma, ratio, alpha

    def advance(j, ratio, alpha):
        p = field[1, 1 + j] + ratio * dirn[j]
        s = img[j] + ratio * along[j]
        return p, s, x_out[0, j] + alpha * p, res[0, j] - alpha * s

    for j in range(N):
        ext[1, 1, 1 + j] = precondition(res[0, j], j)
    halo_start(1)
    halo_wait(1)
    field[...] = ext[1]
    halo_sent(1)

    def iterate(it, carry):
        gamma_old, alpha_old = carry
        par = lax.rem(it, 2)
        products(par)
        for j in range(N):
            ext[par, 1, 1 + j] = precondition(img[j], j)
        halo_start(par)
        gamma, ratio, alpha = totals(par, it == 0, gamma_old, alpha_old)
        for j in range(N):
            dirn[j], along[j], x_out[0, j], res[0, j] = advance(j, ratio, alpha)
        halo_wait(par)
        for a in range(3):
            for c in range(N + 2):
                q = ext[par, a, c] + ratio * push[a, c]
                push[a, c] = q
                field[a, c] = field[a, c] - alpha * q
        halo_sent(par)
        return gamma, alpha

    one = jnp.ones((R, 1), f32)
    gamma_old, alpha_old = lax.fori_loop(0, ITERS - 1, iterate, (one, one))
    last = (ITERS - 1) % 2
    products(last)
    gamma, ratio, alpha = totals(last, ITERS == 1, gamma_old, alpha_old)
    for j in range(N):
        _, _, x_out[0, j], r_out[0, j] = advance(j, ratio, alpha)


def local(load, factors, links, shift):
    vmem = pl.BlockSpec(memory_space=pltpu.VMEM)
    hbm = pl.BlockSpec(memory_space=pltpu.HBM)
    field = jax.ShapeDtypeStruct((1, N, R, B), f32)
    return pl.pallas_call(
        kernel,
        out_shape=(field, field),
        in_specs=[hbm] * 4,
        out_specs=(vmem, vmem),
        scratch_shapes=[
            pltpu.SMEM((4, 1, N), jnp.int32),
            pltpu.VMEM((N, 1, B), f32),
            pltpu.VMEM((4 * N, B, B), bf16),
            pltpu.VMEM((3 * N + 1, B, B), bf16),
            pltpu.VMEM((4 * N, B), f32),
            pltpu.VMEM((4, 4 * N, B), f32),
            pltpu.VMEM((8 * ST, B), f32),
            pltpu.VMEM((8 * NB, B), f32),
            pltpu.VMEM((N, 2 * B, 2 * B), bf16),
            pltpu.VMEM((N, 8 * B, 2 * B), bf16),
            pltpu.VMEM((N, 2 * B, 2 * B), bf16),
            pltpu.VMEM((2, 3, N + 2, R, B), f32),
            pltpu.VMEM((3, N + 2, R, B), f32),
            pltpu.VMEM((3, N + 2, R, B), f32),
            pltpu.VMEM((1, N, R, B), f32),
            pltpu.VMEM((N, R, B), f32),
            pltpu.VMEM((N, R, B), f32),
            pltpu.VMEM((N, R, B), f32),
            pltpu.VMEM((8, B), f32),
            pltpu.VMEM((2, PLANE, B), f32),
            pltpu.SemaphoreType.DMA((4,)),
            pltpu.SemaphoreType.DMA((16,)),
            pltpu.SemaphoreType.DMA((16,)),
            pltpu.SemaphoreType.DMA((8,)),
            pltpu.SemaphoreType.DMA((2, 8)),
            pltpu.SemaphoreType.DMA,
            pltpu.SemaphoreType.DMA((2,)),
        ],
        compiler_params=pltpu.CompilerParams(collective_id=0, has_side_effects=True),
        name="solve",
    )(links, load, factors.reshape(4 * N, B, B), shift.reshape(N, 1, B))


def solution(mesh):
    placed = (
        P(("case", "gx"), "gy", None, None),
        P(None, ("case", "gx"), "gy", None, None),
        P(None, ("case", "gx"), "gy"),
        P(("case", "gx"), "gy", None),
    )
    return jax.shard_map(
        local,
        mesh=mesh,
        in_specs=placed,
        out_specs=(P(("case", "gx"), "gy", None, None), P(("case", "gx"), "gy", None, None)),
        check_vma=False,
    )
```

```python
import functools

import jax
import jax.numpy as jnp
from jax import lax
from jax.experimental import pallas as pl
from jax.experimental.pallas import tpu as pltpu
from jax.sharding import PartitionSpec as P

B = 128
N = 6
R = 32
ITERS = 8
NB = 8
ST = 136
GXN = 8
GYN = 4
PLANE = GXN * GYN
OFFSETS = ((1, 0), (0, 1), (1, 1), (1, -1))
SIDES = ((1, 1), (1, -1), (-1, 1), (-1, -1), (1, 0), (-1, 0), (0, 1), (0, -1))
f32 = jnp.float32
bf16 = jnp.bfloat16


def split3(x):
    a = x.astype(bf16)
    left = x - a.astype(f32)
    b = left.astype(bf16)
    c = (left - b.astype(f32)).astype(bf16)
    return a, b, c


def split2(x):
    a = x.astype(bf16)
    return a, (x - a.astype(f32)).astype(bf16)


def invert(mats, rpan):
    lane = lax.broadcasted_iota(jnp.int32, (8, B), 1)
    def step(b, carry):
        base = b * NB
        rows = [mats[pl.ds(base + i, 8, stride=ST), :] for i in range(NB)]
        inside = (lane >= base) & (lane < base + NB)
        sign = jnp.where(lane < base, -1.0, jnp.where(inside, 0.0, 1.0))
        cols = []
        for m in range(N):
            c0, c1, c2 = split3(mats[pl.ds(pl.multiple_of(m * ST + base, 8), 8), :] * sign)
            cols.append(jnp.concatenate([c0, c0, c1, c1, c0, c2], axis=0))
        e = {}
        for j in range(NB):
            for i in range(j + 1):
                e[i, j] = jnp.sum(jnp.where(lane == base + j, rows[i], 0.0), axis=1, keepdims=True)
        at = lambda i, j: e[min(i, j), max(i, j)]
        for k in range(NB):
            p = 1.0 / e[k, k]
            col = [at(i, k) for i in range(NB)]
            scaled = [c * p for c in col]
            for i in range(NB):
                for j in range(i, NB):
                    if i != k and j != k:
                        e[i, j] = e[i, j] - scaled[i] * col[j]
            for i in range(NB):
                if i != k:
                    e[min(i, k), max(i, k)] = scaled[i]
            e[k, k] = -p
        panel = [jnp.where(lane == base + i, 1.0, jnp.where(inside, 0.0, rows[i])) for i in range(NB)]
        for j in range(NB):
            total = None
            for i in range(NB):
                term = at(i, j) * panel[i]
                total = term if total is None else total + term
            rpan[pl.ds(j, 8, stride=NB), :] = -total
        ups = []
        for m in range(N):
            r0, r1, r2 = split3(rpan[m * NB : (m + 1) * NB, :])
            right = jnp.concatenate([r0, r1, r0, r1, r2, r0], axis=0)
            ups.append(lax.dot_general(cols[m], right, (((0,), (0,)), ((), ())), preferred_element_type=f32))
        new = [jnp.where(inside[0:1, :], 0.0, mats[m * ST : m * ST + B, :]) - ups[m] for m in range(N)]
        for m in range(N):
            mats[m * ST : m * ST + B, :] = new[m]
        for m in range(N):
            mats[pl.ds(pl.multiple_of(m * ST + base, 8), 8), :] = rpan[m * NB : (m + 1) * NB, :]
        return carry
    lax.fori_loop(0, B // NB, step, 0)


def kernel(links_in, load, factors, shift_in, x_out, r_out, links, shift, fac, rem, lm, rlm, mats, rpan, dpan, wts, pre, ext,
           pre_u, push, qdir, zdir, res, dirn, along, img, dsend, drecv, lsem, fsend, frecv, hsend, hrecv, ssend, srecv):
    case = lax.axis_index("case")
    gx = lax.axis_index("gx")
    gy = lax.axis_index("gy")
    me = gx * GYN + gy

    def device(x, y):
        return (case, x, y)

    def exists(sx, sy):
        ok = None
        for pos, step, count in ((gx, sx, GXN), (gy, sy, GYN)):
            if step == 0:
                continue
            here = (pos + step >= 0) & (pos + step < count)
            ok = here if ok is None else ok & here
        return ok

    barrier = pltpu.get_barrier_semaphore()
    peers = []
    for a in (4, 3, 5, 2, 6, 1, 7, 0):
        for c in (2, 1, 3, 0):
            if a or c:
                peers.append(device(lax.rem(gx + a, GXN), lax.rem(gy + c, GYN)))

    ext[...] = jnp.zeros_like(ext)
    rem[...] = jnp.zeros_like(rem)
    rlm[...] = jnp.zeros_like(rlm)
    for peer in peers:
        pl.semaphore_signal(barrier, inc=1, device_id=peer, device_id_type=pl.DeviceIdType.MESH)
    copies = [
        pltpu.make_async_copy(factors, fac, lsem.at[0]),
        pltpu.make_async_copy(links_in, links, lsem.at[1]),
        pltpu.make_async_copy(shift_in, shift, lsem.at[2]),
        pltpu.make_async_copy(load, res, lsem.at[3]),
    ]
    for copy in copies:
        copy.start()
    copies[1].wait()
    for d in range(4):
        for j in range(N):
            lm[d * N + j : d * N + j + 1, :] = jnp.full((1, B), links[d, 0, j], jnp.int32).astype(f32) * (1.0 / B)
    copies[0].wait()
    pl.semaphore_wait(barrier, PLANE - 1)

    def remote(src, dst, ss, rs, sx, sy):
        return pltpu.make_async_remote_copy(
            src_ref=src, dst_ref=dst, send_sem=ss, recv_sem=rs,
            device_id=device(gx + sx, gy + sy), device_id_type=pl.DeviceIdType.MESH)

    moves = (
        (1, 1, ((17, 1, 6),), 1),
        (1, -1, ((18, 1, 17),), 2),
        (0, 1, ((11, 1, 18),), 3),
        (1, 0, ((0, 6, 0), (12, 5, 7), (19, 5, 12)), 0),
    )

    def rim_copies(sx, sy, blocks, n, low=0, high=4):
        parts = [(lm, rlm.at[n], n * 4 + 3)]
        for i, (src, count, dst) in enumerate(blocks):
            parts.append((fac.at[pl.ds(src, count)], rem.at[pl.ds(dst, count)], n * 4 + i))
        return [remote(src, dst, fsend.at[i], frecv.at[i], sx, sy) for src, dst, i in parts[low:high]]

    for sx, sy, blocks, n in moves:
        @pl.when(exists(sx, sy))
        def _():
            for copy in rim_copies(sx, sy, blocks, n):
                copy.start()

    copies[2].wait()

    def square(block):
        return lax.dot_general(block, block, (((1,), (1,)), ((), ())), preferred_element_type=f32)

    def place(j, slot, s):
        a, b = split2(s)
        wts[j, slot * B : (slot + 1) * B, 0:B] = a
        wts[j, slot * B : (slot + 1) * B, B : 2 * B] = b
        return a.astype(f32) + b.astype(f32)

    row_id = lax.broadcasted_iota(jnp.int32, (B, B), 0)
    lane_id = lax.broadcasted_iota(jnp.int32, (B, B), 1)
    eye = row_id == lane_id

    def diag_at(j):
        return pl.ds(pl.multiple_of(j * ST, 8), B)

    for m in range(N):
        mats[m * ST : m * ST + B, :] = jnp.where(eye, shift[m], 0.0)
    for m in range(N, 8):
        mats[m * ST : m * ST + B, :] = jnp.where(eye, 1.0, 0.0)

    def own(j, carry):
        total = mats[diag_at(j), :]
        for d in range(4):
            s = square(fac[d * N + j]) * lm[pl.ds(d * N + j, 1), :]
            s = place(j, d, s)
            total = total + s
            if d == 1:
                after = lax.rem(j + 1, N)
                place(after, 5, s)
                keep = jnp.where(j < N - 1, 1.0, 0.0)
                mats[diag_at(after), :] = mats[diag_at(after), :] + s * keep
        mats[diag_at(j), :] = total
        return carry

    lax.fori_loop(0, N, own, 0)

    def arrived(n, low, high):
        sx, sy, blocks, _ = moves[n]
        @pl.when(exists(-sx, -sy))
        def _():
            for copy in rim_copies(*moves[n], low, high):
                copy.wait_recv()

    def term(j, slot, block, scale):
        return j, place(j, slot, square(rem[block]) * scale)

    def collect(terms):
        for j, s in terms:
            mats[j * ST : j * ST + B, :] = mats[j * ST : j * ST + B, :] + s

    arrived(0, 0, 2)
    arrived(1, 0, 2)
    arrived(2, 0, 2)
    collect([
        term(0, 6, N, rlm[1, 3 * N - 1 : 3 * N, :]),
        term(N - 1, 7, 3 * N - 1, rlm[2, 3 * N : 3 * N + 1, :]),
        term(0, 5, 3 * N, rlm[3, 2 * N - 1 : 2 * N, :]),
    ])
    arrived(3, 0, 2)
    collect([term(j, 4, j, rlm[0, j : j + 1, :]) for j in range(N)])
    arrived(3, 2, 3)
    collect([term(j, 6, N + j, rlm[0, 2 * N + j - 1 : 2 * N + j, :]) for j in range(1, N)])
    arrived(3, 3, 4)
    collect([term(j, 7, 2 * N + j, rlm[0, 3 * N + j + 1 : 3 * N + j + 2, :]) for j in range(N - 1)])

    for m in range(N):
        a, b, c = split3(mats[m * ST : m * ST + B, :])
        dpan[m, 0:B, 0:B] = a
        dpan[m, 0:B, B : 2 * B] = b
        dpan[m, B : 2 * B, 0:B] = c
        dpan[m, B : 2 * B, B : 2 * B] = jnp.zeros((B, B), bf16)
    invert(mats, rpan)

    def pairs(terms):
        return jnp.concatenate([jnp.concatenate([t, t], axis=1) for t in terms], axis=0)

    def fold(out, h):
        small = (out[2 * h :, 0:B] + out[2 * h :, B:]) + out[h : 2 * h, B:]
        return out[0:h, 0:B] + (out[h : 2 * h, 0:B] + (out[0:h, B:] + small))

    better = []
    for m in range(N):
        inv = mats[m * ST : m * ST + B, :]
        terms = split3(inv)
        product = fold(jnp.dot(pairs(terms), dpan[m], preferred_element_type=f32), B)
        error = (jnp.where(eye, 1.0, 0.0) - product).astype(bf16)
        fix = jnp.dot(error, jnp.concatenate(terms[0:2], axis=1), preferred_element_type=f32)
        better.append(inv + (fix[:, 0:B] + fix[:, B:]))
    for m in range(N):
        a, b, c = split3(better[m])
        pre[m, 0:B, 0:B] = a
        pre[m, 0:B, B : 2 * B] = b
        pre[m, B : 2 * B, 0:B] = c
        pre[m, B : 2 * B, B : 2 * B] = jnp.zeros((B, B), bf16)

    for sx, sy, blocks, n in moves:
        @pl.when(exists(sx, sy))
        def _():
            for copy in rim_copies(sx, sy, blocks, n):
                copy.wait_send()

    copies[3].wait()
    x_out[...] = jnp.zeros_like(x_out)
    dirn[...] = jnp.zeros_like(dirn)
    along[...] = jnp.zeros_like(along)
    qdir[...] = jnp.zeros_like(qdir)
    zdir[...] = jnp.zeros_like(zdir)

    def precondition(v, m):
        return fold(jnp.dot(pairs(split3(v)), pre[m], preferred_element_type=f32), R)

    def operate(par, j):
        centre = ext[par, 1, 1 + j]
        terms = []
        for sign in (1, -1):
            for sx, sy in OFFSETS:
                terms.append(split3(centre - ext[par, 1 + sign * sx, 1 + j + sign * sy]))
        left = jnp.concatenate(
            [jnp.concatenate([t[i] for t in terms], axis=1) for i in range(3)], axis=0)
        out = fold(jnp.dot(left, wts[j], preferred_element_type=f32), R)
        return out + shift[j] * centre

    def halo(par):
        for n, (sx, sy) in enumerate(SIDES):
            if sy == 0:
                src = ext.at[par, 1, pl.ds(1, N)]
                dst = ext.at[par, 1 - sx, pl.ds(1, N)]
            else:
                src = ext.at[par, 1, N if sy == 1 else 1]
                dst = ext.at[par, 1 - sx, 0 if sy == 1 else N + 1]
            yield sx, sy, remote(src, dst, hsend.at[n], hrecv.at[par, n], sx, sy)

    def halo_start(par):
        for sx, sy, copy in halo(par):
            pl.when(exists(sx, sy))(copy.start)

    def halo_wait(par):
        for sx, sy, copy in halo(par):
            pl.when(exists(-sx, -sy))(copy.wait_recv)

    def halo_sent(par):
        for sx, sy, copy in halo(par):
            pl.when(exists(sx, sy))(copy.wait_send)

    lane = lax.broadcasted_iota(jnp.int32, (R, B), 1)
    rhs = lax.broadcasted_iota(jnp.int32, (R, B), 0)

    def contribution(par, peer):
        return pltpu.make_async_remote_copy(
            src_ref=dsend.at[pl.ds(par, 1)], dst_ref=drecv.at[par, pl.ds(me, 1)],
            send_sem=ssend, recv_sem=srecv.at[par],
            device_id=peer, device_id_type=pl.DeviceIdType.MESH)

    def products(par, triples):
        gsum, dsum = None, None
        for r, u, w in triples:
            g, d = u * r, u * w
            gsum = g if gsum is None else gsum + g
            dsum = d if dsum is None else dsum + d
        gcol = jnp.sum(gsum, axis=1, keepdims=True)
        dcol = jnp.sum(dsum, axis=1, keepdims=True)
        spread = jnp.where(lane == rhs, gcol, jnp.where(lane == rhs + R, dcol, 0.0))
        row = jnp.sum(spread, axis=0, keepdims=True)
        dsend[pl.ds(par, 1), :] = row
        drecv[par, pl.ds(me, 1), :] = row
        for peer in peers:
            contribution(par, peer).start()

    def totals(par, first, gamma_old, alpha_old):
        everything = drecv.at[par, pl.ds(0, PLANE - 1)]
        pltpu.make_async_copy(everything, everything, srecv.at[par]).wait()
        pltpu.make_async_copy(everything, everything, ssend).wait()
        total = jnp.sum(drecv[par], axis=0, keepdims=True)
        gamma = jnp.sum(jnp.where(lane == rhs, total, 0.0), axis=1, keepdims=True)
        delta = jnp.sum(jnp.where(lane == rhs + R, total, 0.0), axis=1, keepdims=True)
        ratio = jnp.where(first, 0.0, gamma / gamma_old)
        alpha = gamma / (delta - ratio * gamma / alpha_old)
        return gamma, ratio, alpha

    for j in range(N):
        ext[1, 1, 1 + j] = precondition(res[0, j], j)
    halo_start(1)
    halo_wait(1)
    triples = []
    for j in range(N):
        u, w = ext[1, 1, 1 + j], operate(1, j)
        pre_u[j], img[j] = u, w
        triples.append((res[0, j], u, w))
    products(0, triples)
    halo_sent(1)

    def iterate(it, carry):
        gamma_old, alpha_old = carry
        par = lax.rem(it, 2)
        for j in range(N):
            ext[par, 1, 1 + j] = precondition(img[j], j)
        halo_start(par)
        halo_wait(par)
        for j in range(N):
            push[j] = operate(par, j)
        gamma, ratio, alpha = totals(par, it == 0, gamma_old, alpha_old)
        triples = []
        for j in range(N):
            u, w = pre_u[j], img[j]
            z = push[j] + ratio * zdir[j]
            q = ext[par, 1, 1 + j] + ratio * qdir[j]
            s = w + ratio * along[j]
            p = u + ratio * dirn[j]
            zdir[j], qdir[j], along[j], dirn[j] = z, q, s, p
            x_out[0, j] = x_out[0, j] + alpha * p
            r = res[0, j] - alpha * s
            u = u - alpha * q
            w = w - alpha * z
            res[0, j], pre_u[j], img[j] = r, u, w
            triples.append((r, u, w))
        products(1 - par, triples)
        halo_sent(par)
        return gamma, alpha

    one = jnp.ones((R, 1), f32)
    gamma_old, alpha_old = lax.fori_loop(0, ITERS - 1, iterate, (one, one))
    gamma, ratio, alpha = totals((ITERS - 1) % 2, ITERS == 1, gamma_old, alpha_old)
    for j in range(N):
        x_out[0, j] = x_out[0, j] + alpha * (pre_u[j] + ratio * dirn[j])
        r_out[0, j] = res[0, j] - alpha * (img[j] + ratio * along[j])


def local(load, factors, links, shift):
    vmem = pl.BlockSpec(memory_space=pltpu.VMEM)
    hbm = pl.BlockSpec(memory_space=pltpu.HBM)
    field = jax.ShapeDtypeStruct((1, N, R, B), f32)
    return pl.pallas_call(
        kernel,
        out_shape=(field, field),
        in_specs=[hbm] * 4,
        out_specs=(vmem, vmem),
        scratch_shapes=[
            pltpu.SMEM((4, 1, N), jnp.int32),
            pltpu.VMEM((N, 1, B), f32),
            pltpu.VMEM((4 * N, B, B), bf16),
            pltpu.VMEM((3 * N + 1, B, B), bf16),
            pltpu.VMEM((4 * N, B), f32),
            pltpu.VMEM((4, 4 * N, B), f32),
            pltpu.VMEM((8 * ST, B), f32),
            pltpu.VMEM((8 * NB, B), f32),
            pltpu.VMEM((N, 2 * B, 2 * B), bf16),
            pltpu.VMEM((N, 8 * B, 2 * B), bf16),
            pltpu.VMEM((N, 2 * B, 2 * B), bf16),
            pltpu.VMEM((2, 3, N + 2, R, B), f32),
            pltpu.VMEM((N, R, B), f32),
            pltpu.VMEM((N, R, B), f32),
            pltpu.VMEM((N, R, B), f32),
            pltpu.VMEM((N, R, B), f32),
            pltpu.VMEM((1, N, R, B), f32),
            pltpu.VMEM((N, R, B), f32),
            pltpu.VMEM((N, R, B), f32),
            pltpu.VMEM((N, R, B), f32),
            pltpu.VMEM((8, B), f32),
            pltpu.VMEM((2, PLANE, B), f32),
            pltpu.SemaphoreType.DMA((4,)),
            pltpu.SemaphoreType.DMA((16,)),
            pltpu.SemaphoreType.DMA((16,)),
            pltpu.SemaphoreType.DMA((8,)),
            pltpu.SemaphoreType.DMA((2, 8)),
            pltpu.SemaphoreType.DMA,
            pltpu.SemaphoreType.DMA((2,)),
        ],
        compiler_params=pltpu.CompilerParams(collective_id=0, has_side_effects=True, vmem_limit_bytes=24 * 1024 * 1024),
        name="solve",
    )(*[pltpu.with_memory_space_constraint(t, pltpu.HBM) for t in (links, load, factors.reshape(4 * N, B, B), shift.reshape(N, 1, B))])


def solution(mesh):
    placed = (
        P(("case", "gx"), "gy", None, None),
        P(None, ("case", "gx"), "gy", None, None),
        P(None, ("case", "gx"), "gy"),
        P(("case", "gx"), "gy", None),
    )
    return jax.shard_map(
        local,
        mesh=mesh,
        in_specs=placed,
        out_specs=(P(("case", "gx"), "gy", None, None), P(("case", "gx"), "gy", None, None)),
        check_vma=False,
    )
```

```python
import functools

import jax
import jax.numpy as jnp
from jax import lax
from jax.experimental import pallas as pl
from jax.experimental.pallas import tpu as pltpu
from jax.sharding import PartitionSpec as P

B = 128
N = 6
R = 32
ITERS = 8
NB = 8
ST = 136
GXN = 8
GYN = 4
PLANE = GXN * GYN
OFFSETS = ((1, 0), (0, 1), (1, 1), (1, -1))
SIDES = ((1, 1), (1, -1), (-1, 1), (-1, -1), (1, 0), (-1, 0), (0, 1), (0, -1))
f32 = jnp.float32
bf16 = jnp.bfloat16


def split3(x):
    a = x.astype(bf16)
    left = x - a.astype(f32)
    b = left.astype(bf16)
    c = (left - b.astype(f32)).astype(bf16)
    return a, b, c


def split2(x):
    a = x.astype(bf16)
    return a, (x - a.astype(f32)).astype(bf16)


def invert(mats, rpan):
    lane = lax.broadcasted_iota(jnp.int32, (8, B), 1)
    def step(b, carry):
        base = b * NB
        rows = [mats[pl.ds(base + i, 8, stride=ST), :] for i in range(NB)]
        inside = (lane >= base) & (lane < base + NB)
        sign = jnp.where(lane < base, -1.0, jnp.where(inside, 0.0, 1.0))
        cols = []
        for m in range(N):
            c0, c1, c2 = split3(mats[pl.ds(pl.multiple_of(m * ST + base, 8), 8), :] * sign)
            cols.append(jnp.concatenate([c0, c0, c1, c1, c0, c2], axis=0))
        e = {}
        for j in range(NB):
            for i in range(j + 1):
                e[i, j] = jnp.sum(jnp.where(lane == base + j, rows[i], 0.0), axis=1, keepdims=True)
        at = lambda i, j: e[min(i, j), max(i, j)]
        for k in range(NB):
            p = 1.0 / e[k, k]
            col = [at(i, k) for i in range(NB)]
            scaled = [c * p for c in col]
            for i in range(NB):
                for j in range(i, NB):
                    if i != k and j != k:
                        e[i, j] = e[i, j] - scaled[i] * col[j]
            for i in range(NB):
                if i != k:
                    e[min(i, k), max(i, k)] = scaled[i]
            e[k, k] = -p
        panel = [jnp.where(lane == base + i, 1.0, jnp.where(inside, 0.0, rows[i])) for i in range(NB)]
        for j in range(NB):
            total = None
            for i in range(NB):
                term = at(i, j) * panel[i]
                total = term if total is None else total + term
            rpan[pl.ds(j, 8, stride=NB), :] = -total
        ups = []
        for m in range(N):
            r0, r1, r2 = split3(rpan[m * NB : (m + 1) * NB, :])
            right = jnp.concatenate([r0, r1, r0, r1, r2, r0], axis=0)
            ups.append(lax.dot_general(cols[m], right, (((0,), (0,)), ((), ())), preferred_element_type=f32))
        new = [jnp.where(inside[0:1, :], 0.0, mats[m * ST : m * ST + B, :]) - ups[m] for m in range(N)]
        for m in range(N):
            mats[m * ST : m * ST + B, :] = new[m]
        for m in range(N):
            mats[pl.ds(pl.multiple_of(m * ST + base, 8), 8), :] = rpan[m * NB : (m + 1) * NB, :]
        return carry
    lax.fori_loop(0, B // NB, step, 0)


def kernel(links_in, load, factors, shift_in, x_out, r_out, links, shift, fac, rem, lm, rlm, mats, rpan, dpan, wts, pre, ext,
           pre_u, push, qdir, zdir, res, dirn, along, img, dsend, drecv, lsem, fsend, frecv, hsend, hrecv, ssend, srecv, known):
    case = lax.axis_index("case")
    gx = lax.axis_index("gx")
    gy = lax.axis_index("gy")
    me = gx * GYN + gy

    def device(x, y):
        return (case, x, y)

    def exists(sx, sy):
        ok = None
        for pos, step, count in ((gx, sx, GXN), (gy, sy, GYN)):
            if step == 0:
                continue
            here = (pos + step >= 0) & (pos + step < count)
            ok = here if ok is None else ok & here
        return ok

    barrier = pltpu.get_barrier_semaphore()
    peers = []
    for a in (4, 3, 5, 2, 6, 1, 7, 0):
        for c in (2, 1, 3, 0):
            if a or c:
                peers.append(device(lax.rem(gx + a, GXN), lax.rem(gy + c, GYN)))

    ext[...] = jnp.zeros_like(ext)
    rem[...] = jnp.zeros_like(rem)
    rlm[...] = jnp.zeros_like(rlm)
    flip_x = [gx + d - 2 * d * lax.rem(gx // d, 2) for d in (1, 2, 4)]
    flip_y = [gy + d - 2 * d * lax.rem(gy // d, 2) for d in (1, 2)]
    partners = [device(x, gy) for x in flip_x] + [device(gx, y) for y in flip_y]
    greeted = [device(lax.rem(gx + sx + GXN, GXN), lax.rem(gy + sy + GYN, GYN)) for sx, sy in SIDES]
    greeted += [partners[1], partners[2], partners[4]]
    for peer in greeted:
        pl.semaphore_signal(barrier, inc=1, device_id=peer, device_id_type=pl.DeviceIdType.MESH)

    def tell(i):
        pl.semaphore_signal(known.at[i], inc=1, device_id=partners[i], device_id_type=pl.DeviceIdType.MESH)

    def hear(i):
        pl.semaphore_wait(known.at[i], 1)

    copies = [
        pltpu.make_async_copy(factors, fac, lsem.at[0]),
        pltpu.make_async_copy(links_in, links, lsem.at[1]),
        pltpu.make_async_copy(shift_in, shift, lsem.at[2]),
        pltpu.make_async_copy(load, res, lsem.at[3]),
    ]
    for copy in copies:
        copy.start()
    copies[1].wait()
    for d in range(4):
        for j in range(N):
            lm[d * N + j : d * N + j + 1, :] = jnp.full((1, B), links[d, 0, j], jnp.int32).astype(f32) * (1.0 / B)
    copies[0].wait()
    pl.semaphore_wait(barrier, len(greeted))

    def remote(src, dst, ss, rs, sx, sy):
        return pltpu.make_async_remote_copy(
            src_ref=src, dst_ref=dst, send_sem=ss, recv_sem=rs,
            device_id=device(gx + sx, gy + sy), device_id_type=pl.DeviceIdType.MESH)

    moves = (
        (1, 1, ((17, 1, 6),), 1),
        (1, -1, ((18, 1, 17),), 2),
        (0, 1, ((11, 1, 18),), 3),
        (1, 0, ((0, 6, 0), (12, 5, 7), (19, 5, 12)), 0),
    )

    def rim_copies(sx, sy, blocks, n, low=0, high=4):
        parts = [(lm, rlm.at[n], n * 4 + 3)]
        for i, (src, count, dst) in enumerate(blocks):
            parts.append((fac.at[pl.ds(src, count)], rem.at[pl.ds(dst, count)], n * 4 + i))
        return [remote(src, dst, fsend.at[i], frecv.at[i], sx, sy) for src, dst, i in parts[low:high]]

    for sx, sy, blocks, n in moves:
        @pl.when(exists(sx, sy))
        def _():
            for copy in rim_copies(sx, sy, blocks, n):
                copy.start()

    tell(0)
    copies[2].wait()

    def square(block):
        return lax.dot_general(block, block, (((1,), (1,)), ((), ())), preferred_element_type=f32)

    def place(j, slot, s):
        a, b = split2(s)
        wts[j, slot * B : (slot + 1) * B, 0:B] = a
        wts[j, slot * B : (slot + 1) * B, B : 2 * B] = b
        return a.astype(f32) + b.astype(f32)

    row_id = lax.broadcasted_iota(jnp.int32, (B, B), 0)
    lane_id = lax.broadcasted_iota(jnp.int32, (B, B), 1)
    eye = row_id == lane_id

    def diag_at(j):
        return pl.ds(pl.multiple_of(j * ST, 8), B)

    for m in range(N):
        mats[m * ST : m * ST + B, :] = jnp.where(eye, shift[m], 0.0)
    for m in range(N, 8):
        mats[m * ST : m * ST + B, :] = jnp.where(eye, 1.0, 0.0)

    def own(j, carry):
        total = mats[diag_at(j), :]
        for d in range(4):
            s = square(fac[d * N + j]) * lm[pl.ds(d * N + j, 1), :]
            s = place(j, d, s)
            total = total + s
            if d == 1:
                after = lax.rem(j + 1, N)
                place(after, 5, s)
                keep = jnp.where(j < N - 1, 1.0, 0.0)
                mats[diag_at(after), :] = mats[diag_at(after), :] + s * keep
        mats[diag_at(j), :] = total
        return carry

    lax.fori_loop(0, N, own, 0)
    hear(0)
    tell(1)

    def arrived(n, low, high):
        sx, sy, blocks, _ = moves[n]
        @pl.when(exists(-sx, -sy))
        def _():
            for copy in rim_copies(*moves[n], low, high):
                copy.wait_recv()

    def term(j, slot, block, scale):
        return j, place(j, slot, square(rem[block]) * scale)

    def collect(terms):
        for j, s in terms:
            mats[j * ST : j * ST + B, :] = mats[j * ST : j * ST + B, :] + s

    arrived(0, 0, 2)
    arrived(1, 0, 2)
    arrived(2, 0, 2)
    collect([
        term(0, 6, N, rlm[1, 3 * N - 1 : 3 * N, :]),
        term(N - 1, 7, 3 * N - 1, rlm[2, 3 * N : 3 * N + 1, :]),
        term(0, 5, 3 * N, rlm[3, 2 * N - 1 : 2 * N, :]),
    ])
    hear(1)
    tell(2)
    arrived(3, 0, 2)
    collect([term(j, 4, j, rlm[0, j : j + 1, :]) for j in range(N)])
    hear(2)
    tell(3)
    arrived(3, 2, 3)
    collect([term(j, 6, N + j, rlm[0, 2 * N + j - 1 : 2 * N + j, :]) for j in range(1, N)])
    hear(3)
    tell(4)
    arrived(3, 3, 4)
    collect([term(j, 7, 2 * N + j, rlm[0, 3 * N + j + 1 : 3 * N + j + 2, :]) for j in range(N - 1)])

    for m in range(N):
        a, b, c = split3(mats[m * ST : m * ST + B, :])
        dpan[m, 0:B, 0:B] = a
        dpan[m, 0:B, B : 2 * B] = b
        dpan[m, B : 2 * B, 0:B] = c
        dpan[m, B : 2 * B, B : 2 * B] = jnp.zeros((B, B), bf16)
    invert(mats, rpan)
    hear(4)

    def pairs(terms):
        return jnp.concatenate([jnp.concatenate([t, t], axis=1) for t in terms], axis=0)

    def fold(out, h):
        small = (out[2 * h :, 0:B] + out[2 * h :, B:]) + out[h : 2 * h, B:]
        return out[0:h, 0:B] + (out[h : 2 * h, 0:B] + (out[0:h, B:] + small))

    better = []
    for m in range(N):
        inv = mats[m * ST : m * ST + B, :]
        terms = split3(inv)
        product = fold(jnp.dot(pairs(terms), dpan[m], preferred_element_type=f32), B)
        error = (jnp.where(eye, 1.0, 0.0) - product).astype(bf16)
        fix = jnp.dot(error, jnp.concatenate(terms[0:2], axis=1), preferred_element_type=f32)
        better.append(inv + (fix[:, 0:B] + fix[:, B:]))
    for m in range(N):
        a, b, c = split3(better[m])
        pre[m, 0:B, 0:B] = a
        pre[m, 0:B, B : 2 * B] = b
        pre[m, B : 2 * B, 0:B] = c
        pre[m, B : 2 * B, B : 2 * B] = jnp.zeros((B, B), bf16)

    for sx, sy, blocks, n in moves:
        @pl.when(exists(sx, sy))
        def _():
            for copy in rim_copies(sx, sy, blocks, n):
                copy.wait_send()

    copies[3].wait()
    x_out[...] = jnp.zeros_like(x_out)
    dirn[...] = jnp.zeros_like(dirn)
    along[...] = jnp.zeros_like(along)
    qdir[...] = jnp.zeros_like(qdir)
    zdir[...] = jnp.zeros_like(zdir)

    def precondition(v, m):
        return fold(jnp.dot(pairs(split3(v)), pre[m], preferred_element_type=f32), R)

    def operate(par, j):
        centre = ext[par, 1, 1 + j]
        terms = []
        for sign in (1, -1):
            for sx, sy in OFFSETS:
                terms.append(split3(centre - ext[par, 1 + sign * sx, 1 + j + sign * sy]))
        left = jnp.concatenate(
            [jnp.concatenate([t[i] for t in terms], axis=1) for i in range(3)], axis=0)
        out = fold(jnp.dot(left, wts[j], preferred_element_type=f32), R)
        return out + shift[j] * centre

    def halo(par):
        for n, (sx, sy) in enumerate(SIDES):
            if sy == 0:
                src = ext.at[par, 1, pl.ds(1, N)]
                dst = ext.at[par, 1 - sx, pl.ds(1, N)]
            else:
                src = ext.at[par, 1, N if sy == 1 else 1]
                dst = ext.at[par, 1 - sx, 0 if sy == 1 else N + 1]
            yield sx, sy, remote(src, dst, hsend.at[n], hrecv.at[par, n], sx, sy)

    def halo_start(par):
        for sx, sy, copy in halo(par):
            pl.when(exists(sx, sy))(copy.start)

    def halo_wait(par):
        for sx, sy, copy in halo(par):
            pl.when(exists(-sx, -sy))(copy.wait_recv)

    def halo_sent(par):
        for sx, sy, copy in halo(par):
            pl.when(exists(sx, sy))(copy.wait_send)

    lane = lax.broadcasted_iota(jnp.int32, (R, B), 1)
    rhs = lax.broadcasted_iota(jnp.int32, (R, B), 0)

    def contribution(par, peer):
        return pltpu.make_async_remote_copy(
            src_ref=dsend.at[pl.ds(par, 1)], dst_ref=drecv.at[par, pl.ds(me, 1)],
            send_sem=ssend, recv_sem=srecv.at[par],
            device_id=peer, device_id_type=pl.DeviceIdType.MESH)

    def products(par, triples):
        gsum, dsum = None, None
        for r, u, w in triples:
            g, d = u * r, u * w
            gsum = g if gsum is None else gsum + g
            dsum = d if dsum is None else dsum + d
        gcol = jnp.sum(gsum, axis=1, keepdims=True)
        dcol = jnp.sum(dsum, axis=1, keepdims=True)
        spread = jnp.where(lane == rhs, gcol, jnp.where(lane == rhs + R, dcol, 0.0))
        row = jnp.sum(spread, axis=0, keepdims=True)
        dsend[pl.ds(par, 1), :] = row
        drecv[par, pl.ds(me, 1), :] = row
        for peer in peers:
            contribution(par, peer).start()

    def totals(par, first, gamma_old, alpha_old):
        everything = drecv.at[par, pl.ds(0, PLANE - 1)]
        pltpu.make_async_copy(everything, everything, srecv.at[par]).wait()
        pltpu.make_async_copy(everything, everything, ssend).wait()
        total = jnp.sum(drecv[par], axis=0, keepdims=True)
        gamma = jnp.sum(jnp.where(lane == rhs, total, 0.0), axis=1, keepdims=True)
        delta = jnp.sum(jnp.where(lane == rhs + R, total, 0.0), axis=1, keepdims=True)
        ratio = jnp.where(first, 0.0, gamma / gamma_old)
        alpha = gamma / (delta - ratio * gamma / alpha_old)
        return gamma, ratio, alpha

    for j in range(N):
        ext[1, 1, 1 + j] = precondition(res[0, j], j)
    halo_start(1)
    halo_wait(1)
    triples = []
    for j in range(N):
        u, w = ext[1, 1, 1 + j], operate(1, j)
        pre_u[j], img[j] = u, w
        triples.append((res[0, j], u, w))
    products(0, triples)
    halo_sent(1)

    def iterate(it, carry):
        gamma_old, alpha_old = carry
        par = lax.rem(it, 2)
        for j in range(N):
            ext[par, 1, 1 + j] = precondition(img[j], j)
        halo_start(par)
        halo_wait(par)
        for j in range(N):
            push[j] = operate(par, j)
        gamma, ratio, alpha = totals(par, it == 0, gamma_old, alpha_old)
        triples = []
        for j in range(N):
            u, w = pre_u[j], img[j]
            z = push[j] + ratio * zdir[j]
            q = ext[par, 1, 1 + j] + ratio * qdir[j]
            s = w + ratio * along[j]
            p = u + ratio * dirn[j]
            zdir[j], qdir[j], along[j], dirn[j] = z, q, s, p
            x_out[0, j] = x_out[0, j] + alpha * p
            r = res[0, j] - alpha * s
            u = u - alpha * q
            w = w - alpha * z
            res[0, j], pre_u[j], img[j] = r, u, w
            triples.append((r, u, w))
        products(1 - par, triples)
        halo_sent(par)
        return gamma, alpha

    one = jnp.ones((R, 1), f32)
    gamma_old, alpha_old = lax.fori_loop(0, ITERS - 1, iterate, (one, one))
    gamma, ratio, alpha = totals((ITERS - 1) % 2, ITERS == 1, gamma_old, alpha_old)
    for j in range(N):
        x_out[0, j] = x_out[0, j] + alpha * (pre_u[j] + ratio * dirn[j])
        r_out[0, j] = res[0, j] - alpha * (img[j] + ratio * along[j])


def local(load, factors, links, shift):
    vmem = pl.BlockSpec(memory_space=pltpu.VMEM)
    hbm = pl.BlockSpec(memory_space=pltpu.HBM)
    field = jax.ShapeDtypeStruct((1, N, R, B), f32)
    return pl.pallas_call(
        kernel,
        out_shape=(field, field),
        in_specs=[hbm] * 4,
        out_specs=(vmem, vmem),
        scratch_shapes=[
            pltpu.SMEM((4, 1, N), jnp.int32),
            pltpu.VMEM((N, 1, B), f32),
            pltpu.VMEM((4 * N, B, B), bf16),
            pltpu.VMEM((3 * N + 1, B, B), bf16),
            pltpu.VMEM((4 * N, B), f32),
            pltpu.VMEM((4, 4 * N, B), f32),
            pltpu.VMEM((8 * ST, B), f32),
            pltpu.VMEM((8 * NB, B), f32),
            pltpu.VMEM((N, 2 * B, 2 * B), bf16),
            pltpu.VMEM((N, 8 * B, 2 * B), bf16),
            pltpu.VMEM((N, 2 * B, 2 * B), bf16),
            pltpu.VMEM((2, 3, N + 2, R, B), f32),
            pltpu.VMEM((N, R, B), f32),
            pltpu.VMEM((N, R, B), f32),
            pltpu.VMEM((N, R, B), f32),
            pltpu.VMEM((N, R, B), f32),
            pltpu.VMEM((1, N, R, B), f32),
            pltpu.VMEM((N, R, B), f32),
            pltpu.VMEM((N, R, B), f32),
            pltpu.VMEM((N, R, B), f32),
            pltpu.VMEM((8, B), f32),
            pltpu.VMEM((2, PLANE, B), f32),
            pltpu.SemaphoreType.DMA((4,)),
            pltpu.SemaphoreType.DMA((16,)),
            pltpu.SemaphoreType.DMA((16,)),
            pltpu.SemaphoreType.DMA((8,)),
            pltpu.SemaphoreType.DMA((2, 8)),
            pltpu.SemaphoreType.DMA,
            pltpu.SemaphoreType.DMA((2,)),
            pltpu.SemaphoreType.REGULAR((5,)),
        ],
        compiler_params=pltpu.CompilerParams(collective_id=0, has_side_effects=True, vmem_limit_bytes=24 * 1024 * 1024),
        name="solve",
    )(*[pltpu.with_memory_space_constraint(t, pltpu.HBM) for t in (links, load, factors.reshape(4 * N, B, B), shift.reshape(N, 1, B))])


def solution(mesh):
    placed = (
        P(("case", "gx"), "gy", None, None),
        P(None, ("case", "gx"), "gy", None, None),
        P(None, ("case", "gx"), "gy"),
        P(("case", "gx"), "gy", None),
    )
    return jax.shard_map(
        local,
        mesh=mesh,
        in_specs=placed,
        out_specs=(P(("case", "gx"), "gy", None, None), P(("case", "gx"), "gy", None, None)),
        check_vma=False,
    )
```

```python
import functools

import jax
import jax.numpy as jnp
from jax import lax
from jax.experimental import pallas as pl
from jax.experimental.pallas import tpu as pltpu
from jax.sharding import PartitionSpec as P

B = 128
N = 6
R = 32
ITERS = 8
NB = 8
ST = 136
GXN = 8
GYN = 4
PLANE = GXN * GYN
OFFSETS = ((1, 0), (0, 1), (1, 1), (1, -1))
SIDES = ((1, 1), (1, -1), (-1, 1), (-1, -1), (1, 0), (-1, 0), (0, 1), (0, -1))
f32 = jnp.float32
bf16 = jnp.bfloat16


def split3(x):
    a = x.astype(bf16)
    left = x - a.astype(f32)
    b = left.astype(bf16)
    c = (left - b.astype(f32)).astype(bf16)
    return a, b, c


def split2(x):
    a = x.astype(bf16)
    return a, (x - a.astype(f32)).astype(bf16)


def invert(mats, rpan):
    lane = lax.broadcasted_iota(jnp.int32, (8, B), 1)
    def step(b, carry):
        base = b * NB
        rows = [mats[pl.ds(base + i, 8, stride=ST), :] for i in range(NB)]
        inside = (lane >= base) & (lane < base + NB)
        sign = jnp.where(lane < base, -1.0, jnp.where(inside, 0.0, 1.0))
        cols = []
        for m in range(N):
            c0, c1, c2 = split3(mats[pl.ds(pl.multiple_of(m * ST + base, 8), 8), :] * sign)
            cols.append(jnp.concatenate([c0, c0, c1, c1, c0, c2], axis=0))
        e = {}
        for j in range(NB):
            for i in range(j + 1):
                e[i, j] = jnp.sum(jnp.where(lane == base + j, rows[i], 0.0), axis=1, keepdims=True)
        at = lambda i, j: e[min(i, j), max(i, j)]
        for k in range(NB):
            p = 1.0 / e[k, k]
            col = [at(i, k) for i in range(NB)]
            scaled = [c * p for c in col]
            for i in range(NB):
                for j in range(i, NB):
                    if i != k and j != k:
                        e[i, j] = e[i, j] - scaled[i] * col[j]
            for i in range(NB):
                if i != k:
                    e[min(i, k), max(i, k)] = scaled[i]
            e[k, k] = -p
        panel = [jnp.where(lane == base + i, 1.0, jnp.where(inside, 0.0, rows[i])) for i in range(NB)]
        for j in range(NB):
            total = None
            for i in range(NB):
                term = at(i, j) * panel[i]
                total = term if total is None else total + term
            rpan[pl.ds(j, 8, stride=NB), :] = -total
        ups = []
        for m in range(N):
            r0, r1, r2 = split3(rpan[m * NB : (m + 1) * NB, :])
            right = jnp.concatenate([r0, r1, r0, r1, r2, r0], axis=0)
            ups.append(lax.dot_general(cols[m], right, (((0,), (0,)), ((), ())), preferred_element_type=f32))
        new = [jnp.where(inside[0:1, :], 0.0, mats[m * ST : m * ST + B, :]) - ups[m] for m in range(N)]
        for m in range(N):
            mats[m * ST : m * ST + B, :] = new[m]
        for m in range(N):
            mats[pl.ds(pl.multiple_of(m * ST + base, 8), 8), :] = rpan[m * NB : (m + 1) * NB, :]
        return carry
    lax.fori_loop(0, B // NB, step, 0)


def kernel(links_in, load, factors, shift_in, x_out, r_out, links, shift, fac, rem, lm, rlm, mats, rpan, dpan, wts, pre, ext,
           pre_u, push, qdir, zdir, res, dirn, along, img, dsend, drecv, lsem, fsend, frecv, hsend, hrecv, ssend, srecv, known,
           acc, tsend, trecv, tsems):
    case = lax.axis_index("case")
    gx = lax.axis_index("gx")
    gy = lax.axis_index("gy")
    me = gx * GYN + gy

    def device(x, y):
        return (case, x, y)

    def exists(sx, sy):
        ok = None
        for pos, step, count in ((gx, sx, GXN), (gy, sy, GYN)):
            if step == 0:
                continue
            here = (pos + step >= 0) & (pos + step < count)
            ok = here if ok is None else ok & here
        return ok

    barrier = pltpu.get_barrier_semaphore()
    peers = []
    for a in (4, 3, 5, 2, 6, 1, 7, 0):
        for c in (2, 1, 3, 0):
            if a or c:
                peers.append(device(lax.rem(gx + a, GXN), lax.rem(gy + c, GYN)))

    ext[...] = jnp.zeros_like(ext)
    rem[...] = jnp.zeros_like(rem)
    rlm[...] = jnp.zeros_like(rlm)
    trecv[...] = jnp.zeros_like(trecv)
    def ring(dx, dy):
        return device(lax.rem(gx + dx + GXN, GXN), lax.rem(gy + dy + GYN, GYN))

    greeted = [ring(1, 0), ring(-1, 0), ring(0, 1), ring(0, -1)]
    rounds = [greeted, [ring(2, 0), ring(-2, 0), ring(0, 2)], [ring(d, 0) for d in range(1, GXN)]]
    for peer in greeted:
        pl.semaphore_signal(barrier, inc=1, device_id=peer, device_id_type=pl.DeviceIdType.MESH)

    def tell(i):
        for peer in rounds[i]:
            pl.semaphore_signal(known.at[i], inc=1, device_id=peer, device_id_type=pl.DeviceIdType.MESH)

    def hear(i):
        pl.semaphore_wait(known.at[i], len(rounds[i]))

    copies = [
        pltpu.make_async_copy(factors, fac, lsem.at[0]),
        pltpu.make_async_copy(links_in, links, lsem.at[1]),
        pltpu.make_async_copy(shift_in, shift, lsem.at[2]),
        pltpu.make_async_copy(load, res, lsem.at[3]),
    ]
    for copy in copies:
        copy.start()
    copies[1].wait()
    for d in range(4):
        for j in range(N):
            lm[d * N + j : d * N + j + 1, :] = jnp.full((1, B), links[d, 0, j], jnp.int32).astype(f32) * (1.0 / B)
    copies[0].wait()
    pl.semaphore_wait(barrier, len(greeted))

    def remote(src, dst, ss, rs, sx, sy):
        return pltpu.make_async_remote_copy(
            src_ref=src, dst_ref=dst, send_sem=ss, recv_sem=rs,
            device_id=device(gx + sx, gy + sy), device_id_type=pl.DeviceIdType.MESH)

    moves = (
        (1, 1, ((17, 1, 6),), 1),
        (1, -1, ((18, 1, 17),), 2),
        (0, 1, ((11, 1, 18),), 3),
        (1, 0, ((0, 6, 0), (12, 5, 7), (19, 5, 12)), 0),
    )

    def rim_copies(sx, sy, blocks, n, low=0, high=4):
        parts = [(lm, rlm.at[n], n * 4 + 3)]
        for i, (src, count, dst) in enumerate(blocks):
            parts.append((fac.at[pl.ds(src, count)], rem.at[pl.ds(dst, count)], n * 4 + i))
        return [remote(src, dst, fsend.at[i], frecv.at[i], sx, sy) for src, dst, i in parts[low:high]]

    def depart(n, low, high):
        sx, sy, _, _ = moves[n]
        @pl.when(exists(sx, sy))
        def _():
            for copy in rim_copies(*moves[n], low, high):
                copy.start()

    depart(2, 0, 2)
    tell(0)
    copies[2].wait()

    def square(block):
        return lax.dot_general(block, block, (((1,), (1,)), ((), ())), preferred_element_type=f32)

    def place(j, slot, s):
        a, b = split2(s)
        wts[j, slot * B : (slot + 1) * B, 0:B] = a
        wts[j, slot * B : (slot + 1) * B, B : 2 * B] = b
        return a.astype(f32) + b.astype(f32)

    row_id = lax.broadcasted_iota(jnp.int32, (B, B), 0)
    lane_id = lax.broadcasted_iota(jnp.int32, (B, B), 1)
    eye = row_id == lane_id

    for m in range(N):
        mats[m * ST : m * ST + B, :] = jnp.where(eye, shift[m], 0.0)
    for m in range(N, 8):
        mats[m * ST : m * ST + B, :] = jnp.where(eye, 1.0, 0.0)

    def ahead(n):
        return remote(tsend.at[n], trecv.at[n], tsems.at[0, n], tsems.at[1, n], 1, 0)

    half = B // 2
    low_lanes = lax.broadcasted_iota(jnp.int32, (half // 2, B), 1) < half

    def own(j):
        s = [place(j, d, square(fac[d * N + j]) * lm[d * N + j : d * N + j + 1, :]) for d in range(4)]
        if j < N - 1:
            place(j + 1, 5, s[1])
        return s

    def send_ahead(n, t):
        tsend[n, 0:half, :] = t[0:half]
        tsend[n, half : half + half // 2, :] = jnp.where(
            low_lanes, pltpu.roll(t[half : half + half // 2], half, 1), t[half + half // 2 :])
        pl.when(exists(1, 0))(ahead(n).start)

    def arrived(n, low, high):
        sx, sy, _, _ = moves[n]
        @pl.when(exists(-sx, -sy))
        def _():
            for copy in rim_copies(*moves[n], low, high):
                copy.wait_recv()

    def term(j, slot, block, scale):
        return j, place(j, slot, square(rem[block]) * scale)

    def collect(terms):
        for j, s in terms:
            mats[j * ST : j * ST + B, :] = mats[j * ST : j * ST + B, :] + s

    prev = None
    for j in range(N):
        s = own(j)
        mats[j * ST : j * ST + B, :] = mats[j * ST : j * ST + B, :] + ((s[0] + s[1]) + (s[2] + s[3]))
        if j < N - 1:
            mats[(j + 1) * ST : (j + 1) * ST + B, :] = mats[(j + 1) * ST : (j + 1) * ST + B, :] + s[1]
        if j > 0:
            send_ahead(j - 1, acc[j - 1] + s[3])
        acc[j] = s[0] if prev is None else s[0] + prev
        prev = s[2]
        if j == 1:
            hear(0)
            depart(0, 0, 2)
            depart(1, 0, 2)
            tell(1)
    send_ahead(N - 1, acc[N - 1])
    depart(3, 0, 4)
    hear(1)
    tell(2)

    arrived(2, 0, 2)
    arrived(0, 0, 2)
    arrived(1, 0, 2)
    collect([
        term(0, 6, N, rlm[1, 3 * N - 1 : 3 * N, :]),
        term(N - 1, 7, 3 * N - 1, rlm[2, 3 * N : 3 * N + 1, :]),
        term(0, 5, 3 * N, rlm[3, 2 * N - 1 : 2 * N, :]),
    ])

    for n in range(N):
        pl.when(exists(-1, 0))(ahead(n).wait_recv)
    for n in range(N):
        top, packed = trecv[n, 0:half, :], trecv[n, half : half + half // 2, :]
        turned = jnp.concatenate([top, jnp.zeros_like(top)], axis=0).T
        base = n * ST
        mats[base : base + half, :] = mats[base : base + half, :] + top
        for k, part in enumerate((pltpu.roll(packed, half, 1), packed)):
            at = half + k * half // 2
            span = slice(base + at, base + at + half // 2)
            mats[span, :] = mats[span, :] + jnp.where(low_lanes, turned[at : at + half // 2], part)

    for m in range(N):
        a, b, c = split3(mats[m * ST : m * ST + B, :])
        dpan[m, 0:B, 0:B] = a
        dpan[m, 0:B, B : 2 * B] = b
        dpan[m, B : 2 * B, 0:B] = c
        dpan[m, B : 2 * B, B : 2 * B] = jnp.zeros((B, B), bf16)
    invert(mats, rpan)
    hear(2)

    def pairs(terms):
        return jnp.concatenate([jnp.concatenate([t, t], axis=1) for t in terms], axis=0)

    def fold(out, h):
        small = (out[2 * h :, 0:B] + out[2 * h :, B:]) + out[h : 2 * h, B:]
        return out[0:h, 0:B] + (out[h : 2 * h, 0:B] + (out[0:h, B:] + small))

    better = []
    for m in range(N):
        inv = mats[m * ST : m * ST + B, :]
        terms = split3(inv)
        product = fold(jnp.dot(pairs(terms), dpan[m], preferred_element_type=f32), B)
        error = (jnp.where(eye, 1.0, 0.0) - product).astype(bf16)
        fix = jnp.dot(error, jnp.concatenate(terms[0:2], axis=1), preferred_element_type=f32)
        better.append(inv + (fix[:, 0:B] + fix[:, B:]))
    for m in range(N):
        a, b, c = split3(better[m])
        pre[m, 0:B, 0:B] = a
        pre[m, 0:B, B : 2 * B] = b
        pre[m, B : 2 * B, 0:B] = c
        pre[m, B : 2 * B, B : 2 * B] = jnp.zeros((B, B), bf16)

    copies[3].wait()
    x_out[...] = jnp.zeros_like(x_out)
    dirn[...] = jnp.zeros_like(dirn)
    along[...] = jnp.zeros_like(along)
    qdir[...] = jnp.zeros_like(qdir)
    zdir[...] = jnp.zeros_like(zdir)

    def precondition(v, m):
        return fold(jnp.dot(pairs(split3(v)), pre[m], preferred_element_type=f32), R)

    def operate(par, j):
        centre = ext[par, 1, 1 + j]
        terms = []
        for sign in (1, -1):
            for sx, sy in OFFSETS:
                terms.append(split3(centre - ext[par, 1 + sign * sx, 1 + j + sign * sy]))
        left = jnp.concatenate(
            [jnp.concatenate([t[i] for t in terms], axis=1) for i in range(3)], axis=0)
        out = fold(jnp.dot(left, wts[j], preferred_element_type=f32), R)
        return out + shift[j] * centre

    def halo(par):
        for n, (sx, sy) in enumerate(SIDES):
            if sy == 0:
                src = ext.at[par, 1, pl.ds(1, N)]
                dst = ext.at[par, 1 - sx, pl.ds(1, N)]
            else:
                src = ext.at[par, 1, N if sy == 1 else 1]
                dst = ext.at[par, 1 - sx, 0 if sy == 1 else N + 1]
            yield sx, sy, remote(src, dst, hsend.at[n], hrecv.at[par, n], sx, sy)

    def halo_start(par):
        for sx, sy, copy in halo(par):
            pl.when(exists(sx, sy))(copy.start)

    def halo_wait(par):
        for sx, sy, copy in halo(par):
            pl.when(exists(-sx, -sy))(copy.wait_recv)

    def halo_sent(par):
        for sx, sy, copy in halo(par):
            pl.when(exists(sx, sy))(copy.wait_send)

    lane = lax.broadcasted_iota(jnp.int32, (R, B), 1)
    rhs = lax.broadcasted_iota(jnp.int32, (R, B), 0)

    def contribution(par, peer):
        return pltpu.make_async_remote_copy(
            src_ref=dsend.at[pl.ds(par, 1)], dst_ref=drecv.at[par, pl.ds(me, 1)],
            send_sem=ssend, recv_sem=srecv.at[par],
            device_id=peer, device_id_type=pl.DeviceIdType.MESH)

    def products(par, triples):
        gsum, dsum = None, None
        for r, u, w in triples:
            g, d = u * r, u * w
            gsum = g if gsum is None else gsum + g
            dsum = d if dsum is None else dsum + d
        gcol = jnp.sum(gsum, axis=1, keepdims=True)
        dcol = jnp.sum(dsum, axis=1, keepdims=True)
        spread = jnp.where(lane == rhs, gcol, jnp.where(lane == rhs + R, dcol, 0.0))
        row = jnp.sum(spread, axis=0, keepdims=True)
        dsend[pl.ds(par, 1), :] = row
        drecv[par, pl.ds(me, 1), :] = row
        for peer in peers:
            contribution(par, peer).start()

    def totals(par, first, gamma_old, alpha_old):
        everything = drecv.at[par, pl.ds(0, PLANE - 1)]
        pltpu.make_async_copy(everything, everything, srecv.at[par]).wait()
        pltpu.make_async_copy(everything, everything, ssend).wait()
        total = jnp.sum(drecv[par], axis=0, keepdims=True)
        gamma = jnp.sum(jnp.where(lane == rhs, total, 0.0), axis=1, keepdims=True)
        delta = jnp.sum(jnp.where(lane == rhs + R, total, 0.0), axis=1, keepdims=True)
        ratio = jnp.where(first, 0.0, gamma / gamma_old)
        alpha = gamma / (delta - ratio * gamma / alpha_old)
        return gamma, ratio, alpha

    for j in range(N):
        ext[1, 1, 1 + j] = precondition(res[0, j], j)
    halo_start(1)
    arrived(3, 0, 2)
    for j in range(N):
        term(j, 4, j, rlm[0, j : j + 1, :])
    arrived(3, 2, 3)
    for j in range(1, N):
        term(j, 6, N + j, rlm[0, 2 * N + j - 1 : 2 * N + j, :])
    arrived(3, 3, 4)
    for j in range(N - 1):
        term(j, 7, 2 * N + j, rlm[0, 3 * N + j + 1 : 3 * N + j + 2, :])
    halo_wait(1)
    triples = []
    for j in range(N):
        u, w = ext[1, 1, 1 + j], operate(1, j)
        pre_u[j], img[j] = u, w
        triples.append((res[0, j], u, w))
    products(0, triples)
    halo_sent(1)
    for sx, sy, blocks, n in moves:
        @pl.when(exists(sx, sy))
        def _():
            for copy in rim_copies(sx, sy, blocks, n):
                copy.wait_send()
    for n in range(N):
        pl.when(exists(1, 0))(ahead(n).wait_send)

    def iterate(it, carry):
        gamma_old, alpha_old = carry
        par = lax.rem(it, 2)
        for j in range(N):
            ext[par, 1, 1 + j] = precondition(img[j], j)
        halo_start(par)
        halo_wait(par)
        for j in range(N):
            push[j] = operate(par, j)
        gamma, ratio, alpha = totals(par, it == 0, gamma_old, alpha_old)
        triples = []
        for j in range(N):
            u, w = pre_u[j], img[j]
            z = push[j] + ratio * zdir[j]
            q = ext[par, 1, 1 + j] + ratio * qdir[j]
            s = w + ratio * along[j]
            p = u + ratio * dirn[j]
            zdir[j], qdir[j], along[j], dirn[j] = z, q, s, p
            x_out[0, j] = x_out[0, j] + alpha * p
            r = res[0, j] - alpha * s
            u = u - alpha * q
            w = w - alpha * z
            res[0, j], pre_u[j], img[j] = r, u, w
            triples.append((r, u, w))
        products(1 - par, triples)
        halo_sent(par)
        return gamma, alpha

    one = jnp.ones((R, 1), f32)
    gamma_old, alpha_old = lax.fori_loop(0, ITERS - 1, iterate, (one, one))
    gamma, ratio, alpha = totals((ITERS - 1) % 2, ITERS == 1, gamma_old, alpha_old)
    for j in range(N):
        x_out[0, j] = x_out[0, j] + alpha * (pre_u[j] + ratio * dirn[j])
        r_out[0, j] = res[0, j] - alpha * (img[j] + ratio * along[j])


def local(load, factors, links, shift):
    vmem = pl.BlockSpec(memory_space=pltpu.VMEM)
    hbm = pl.BlockSpec(memory_space=pltpu.HBM)
    field = jax.ShapeDtypeStruct((1, N, R, B), f32)
    return pl.pallas_call(
        kernel,
        out_shape=(field, field),
        in_specs=[hbm] * 4,
        out_specs=(vmem, vmem),
        scratch_shapes=[
            pltpu.SMEM((4, 1, N), jnp.int32),
            pltpu.VMEM((N, 1, B), f32),
            pltpu.VMEM((4 * N, B, B), bf16),
            pltpu.VMEM((3 * N + 1, B, B), bf16),
            pltpu.VMEM((4 * N, B), f32),
            pltpu.VMEM((4, 4 * N, B), f32),
            pltpu.VMEM((8 * ST, B), f32),
            pltpu.VMEM((8 * NB, B), f32),
            pltpu.VMEM((N, 2 * B, 2 * B), bf16),
            pltpu.VMEM((N, 8 * B, 2 * B), bf16),
            pltpu.VMEM((N, 2 * B, 2 * B), bf16),
            pltpu.VMEM((2, 3, N + 2, R, B), f32),
            pltpu.VMEM((N, R, B), f32),
            pltpu.VMEM((N, R, B), f32),
            pltpu.VMEM((N, R, B), f32),
            pltpu.VMEM((N, R, B), f32),
            pltpu.VMEM((1, N, R, B), f32),
            pltpu.VMEM((N, R, B), f32),
            pltpu.VMEM((N, R, B), f32),
            pltpu.VMEM((N, R, B), f32),
            pltpu.VMEM((8, B), f32),
            pltpu.VMEM((2, PLANE, B), f32),
            pltpu.SemaphoreType.DMA((4,)),
            pltpu.SemaphoreType.DMA((16,)),
            pltpu.SemaphoreType.DMA((16,)),
            pltpu.SemaphoreType.DMA((8,)),
            pltpu.SemaphoreType.DMA((2, 8)),
            pltpu.SemaphoreType.DMA,
            pltpu.SemaphoreType.DMA((2,)),
            pltpu.SemaphoreType.REGULAR((3,)),
            pltpu.VMEM((N, B, B), f32),
            pltpu.VMEM((N, 3 * B // 4, B), f32),
            pltpu.VMEM((N, 3 * B // 4, B), f32),
            pltpu.SemaphoreType.DMA((2, N)),
        ],
        compiler_params=pltpu.CompilerParams(collective_id=0, has_side_effects=True, vmem_limit_bytes=24 * 1024 * 1024),
        name="solve",
    )(*[pltpu.with_memory_space_constraint(t, pltpu.HBM) for t in (links, load, factors.reshape(4 * N, B, B), shift.reshape(N, 1, B))])


def solution(mesh):
    placed = (
        P(("case", "gx"), "gy", None, None),
        P(None, ("case", "gx"), "gy", None, None),
        P(None, ("case", "gx"), "gy"),
        P(("case", "gx"), "gy", None),
    )
    return jax.shard_map(
        local,
        mesh=mesh,
        in_specs=placed,
        out_specs=(P(("case", "gx"), "gy", None, None), P(("case", "gx"), "gy", None, None)),
        check_vma=False,
    )
```

```python
import functools

import jax
import jax.numpy as jnp
from jax import lax
from jax.experimental import pallas as pl
from jax.experimental.pallas import tpu as pltpu
from jax.sharding import PartitionSpec as P

B = 128
N = 6
R = 32
ITERS = 8
NB = 8
ST = 136
GXN = 8
GYN = 4
PLANE = GXN * GYN
OFFSETS = ((1, 0), (0, 1), (1, 1), (1, -1))
SIDES = ((1, 1), (1, -1), (-1, 1), (-1, -1), (1, 0), (-1, 0), (0, 1), (0, -1))
f32 = jnp.float32
bf16 = jnp.bfloat16


def split3(x):
    a = x.astype(bf16)
    left = x - a.astype(f32)
    b = left.astype(bf16)
    c = (left - b.astype(f32)).astype(bf16)
    return a, b, c


def split2(x):
    a = x.astype(bf16)
    return a, (x - a.astype(f32)).astype(bf16)


def invert(mats, rpan, cpan):
    lane = lax.broadcasted_iota(jnp.int32, (8, B), 1)

    def packed(base):
        return [mats[pl.ds(base + i, 8, stride=ST), :] for i in range(NB)]

    def pick(row, k):
        return jnp.sum(jnp.where(lane == k, row, 0.0), axis=1, keepdims=True)

    def pivot(rows, base):
        e = {}
        for j in range(NB):
            for i in range(j + 1):
                e[i, j] = pick(rows[i], base + j)
        ahead = [[pick(rows[k], base + NB + i) for k in range(NB)] for i in range(NB)]
        inside = (lane >= base) & (lane < base + NB)
        sign = jnp.where(lane < base, -1.0, jnp.where(inside, 0.0, 1.0))
        at = lambda i, j: e[min(i, j), max(i, j)]
        for k in range(NB):
            p = 1.0 / e[k, k]
            col = [at(i, k) for i in range(NB)]
            scaled = [c * p for c in col]
            for i in range(NB):
                for j in range(i, NB):
                    if i != k and j != k:
                        e[i, j] = e[i, j] - scaled[i] * col[j]
            for i in range(NB):
                if i != k:
                    e[min(i, k), max(i, k)] = scaled[i]
            e[k, k] = -p
        panel = [jnp.where(lane == base + i, 1.0, jnp.where(inside, 0.0, rows[i])) for i in range(NB)]
        right = []
        for j in range(NB):
            total = None
            for i in range(NB):
                term = at(i, j) * panel[i]
                total = term if total is None else total + term
            right.append(-total)
        following = packed(jnp.minimum(base + NB, B - NB))
        after = []
        for i in range(NB):
            row = jnp.where(inside, 0.0, following[i])
            for k in range(NB):
                row = row - ahead[i][k] * right[k]
            after.append(row)
        for k in range(NB):
            cpan[pl.ds(k, 8, stride=NB), :] = rows[k] * sign
            rpan[pl.ds(k, 8, stride=NB), :] = right[k]
        return tuple(after)

    def trail(base):
        inside = (lane >= base) & (lane < base + NB)
        rows = [rpan[m * NB : (m + 1) * NB, :] for m in range(N)]
        ups = []
        for m in range(N):
            c0, c1, c2 = split3(cpan[m * NB : (m + 1) * NB, :])
            r0, r1, r2 = split3(rows[m])
            ups.append(lax.dot_general(
                jnp.concatenate([c0, c0, c1, c1, c0, c2], axis=0),
                jnp.concatenate([r0, r1, r0, r1, r2, r0], axis=0),
                (((0,), (0,)), ((), ())), preferred_element_type=f32))
        new = [jnp.where(inside[0:1, :], 0.0, mats[m * ST : m * ST + B, :]) - ups[m] for m in range(N)]
        for m in range(N):
            mats[m * ST : m * ST + B, :] = new[m]
        for m in range(N):
            mats[pl.ds(pl.multiple_of(m * ST + base, 8), 8), :] = rows[m]

    def step(b, rows):
        trail((b - 1) * NB)
        return pivot(rows, b * NB)

    rows = pivot(packed(0), 0)
    lax.fori_loop(1, B // NB, step, rows)
    trail(B - NB)


def kernel(links_in, load, factors, shift_in, x_out, r_out, links, shift, fac, rem, lm, rlm, mats, rpan, cpan, dpan, errs, wts, pre, ext,
           pre_u, push, qdir, zdir, res, dirn, along, img, dsend, drecv, lsem, fsend, frecv, hsend, hrecv, ssend, srecv, known,
           tsend, trecv, tsems):
    case = lax.axis_index("case")
    gx = lax.axis_index("gx")
    gy = lax.axis_index("gy")
    me = gx * GYN + gy

    def device(x, y):
        return (case, x, y)

    def exists(sx, sy):
        ok = None
        for pos, step, count in ((gx, sx, GXN), (gy, sy, GYN)):
            if step == 0:
                continue
            here = (pos + step >= 0) & (pos + step < count)
            ok = here if ok is None else ok & here
        return ok

    barrier = pltpu.get_barrier_semaphore()
    peers = []
    for a in (4, 3, 5, 2, 6, 1, 7, 0):
        for c in (2, 1, 3, 0):
            if a or c:
                peers.append(device(lax.rem(gx + a, GXN), lax.rem(gy + c, GYN)))

    ext[...] = jnp.zeros_like(ext)
    rem[...] = jnp.zeros_like(rem)
    rlm[...] = jnp.zeros_like(rlm)
    trecv[...] = jnp.zeros_like(trecv)
    def ring(dx, dy):
        return device(lax.rem(gx + dx + GXN, GXN), lax.rem(gy + dy + GYN, GYN))

    greeted = [ring(1, 0), ring(-1, 0), ring(0, 1), ring(0, -1)]
    rounds = [greeted, [ring(2, 0), ring(-2, 0), ring(0, 2)], [ring(d, 0) for d in range(1, GXN)]]
    for peer in greeted:
        pl.semaphore_signal(barrier, inc=1, device_id=peer, device_id_type=pl.DeviceIdType.MESH)

    def tell(i):
        for peer in rounds[i]:
            pl.semaphore_signal(known.at[i], inc=1, device_id=peer, device_id_type=pl.DeviceIdType.MESH)

    def hear(i):
        pl.semaphore_wait(known.at[i], len(rounds[i]))

    copies = [
        pltpu.make_async_copy(factors, fac, lsem.at[0]),
        pltpu.make_async_copy(links_in, links, lsem.at[1]),
        pltpu.make_async_copy(shift_in, shift, lsem.at[2]),
        pltpu.make_async_copy(load, res, lsem.at[3]),
    ]
    for copy in copies:
        copy.start()
    copies[1].wait()
    for d in range(4):
        for j in range(N):
            lm[d * N + j : d * N + j + 1, :] = jnp.full((1, B), links[d, 0, j], jnp.int32).astype(f32) * (1.0 / B)
    copies[0].wait()
    pl.semaphore_wait(barrier, len(greeted))

    def remote(src, dst, ss, rs, sx, sy):
        return pltpu.make_async_remote_copy(
            src_ref=src, dst_ref=dst, send_sem=ss, recv_sem=rs,
            device_id=device(gx + sx, gy + sy), device_id_type=pl.DeviceIdType.MESH)

    moves = (
        (1, 1, ((17, 1, 6),), 1),
        (1, -1, ((18, 1, 17),), 2),
        (0, 1, ((11, 1, 18),), 3),
        (1, 0, ((0, 6, 0), (12, 5, 7), (19, 5, 12)), 0),
    )

    def rim_copies(sx, sy, blocks, n, low=0, high=4):
        parts = [(lm, rlm.at[n], n * 4 + 3)]
        for i, (src, count, dst) in enumerate(blocks):
            parts.append((fac.at[pl.ds(src, count)], rem.at[pl.ds(dst, count)], n * 4 + i))
        return [remote(src, dst, fsend.at[i], frecv.at[i], sx, sy) for src, dst, i in parts[low:high]]

    def depart(n, low, high):
        sx, sy, _, _ = moves[n]
        @pl.when(exists(sx, sy))
        def _():
            for copy in rim_copies(*moves[n], low, high):
                copy.start()

    depart(2, 0, 2)
    tell(0)
    copies[2].wait()

    def square(block):
        return lax.dot_general(block, block, (((1,), (1,)), ((), ())), preferred_element_type=f32)

    def place(j, slot, s):
        a, b = split2(s)
        wts[j, slot * B : (slot + 1) * B, 0:B] = a
        wts[j, slot * B : (slot + 1) * B, B : 2 * B] = b
        return a.astype(f32) + b.astype(f32)

    row_id = lax.broadcasted_iota(jnp.int32, (B, B), 0)
    lane_id = lax.broadcasted_iota(jnp.int32, (B, B), 1)
    eye = row_id == lane_id

    for m in range(N):
        mats[m * ST : m * ST + B, :] = jnp.where(eye, shift[m], 0.0)
    for m in range(N, 8):
        mats[m * ST : m * ST + B, :] = jnp.where(eye, 1.0, 0.0)

    def ahead(n):
        return remote(tsend.at[n], trecv.at[n], tsems.at[0, n], tsems.at[1, n], 1, 0)

    quarter = B // 4
    lane_q = lax.broadcasted_iota(jnp.int32, (quarter, B), 1)
    lane_h = lax.broadcasted_iota(jnp.int32, (quarter // 2, B), 1)
    above = row_id // quarter <= lane_id // quarter

    def own(j, d):
        s = place(j, d, square(fac[d * N + j]) * lm[d * N + j : d * N + j + 1, :])
        mats[j * ST : j * ST + B, :] = mats[j * ST : j * ST + B, :] + s
        return s

    def send_ahead(n, t):
        q = [t[k * quarter : (k + 1) * quarter] for k in range(4)]
        tsend[n, 0:quarter, :] = q[0]
        tsend[n, quarter : 2 * quarter, :] = jnp.where(lane_q < quarter, pltpu.roll(q[3], quarter, 1), q[1])
        tsend[n, 2 * quarter :, :] = jnp.where(
            lane_h < 2 * quarter, pltpu.roll(q[2][: quarter // 2], 2 * quarter, 1), q[2][quarter // 2 :])
        pl.when(exists(1, 0))(ahead(n).start)

    def unpack(n):
        p0, p1, p2 = trecv[n, 0:quarter, :], trecv[n, quarter : 2 * quarter, :], trecv[n, 2 * quarter :, :]
        upper = jnp.concatenate(
            [p0, p1, pltpu.roll(p2, 2 * quarter, 1), p2, pltpu.roll(p1, 3 * quarter, 1)], axis=0)
        return jnp.where(above, upper, upper.T)

    def arrived(n, low, high):
        sx, sy, _, _ = moves[n]
        @pl.when(exists(-sx, -sy))
        def _():
            for copy in rim_copies(*moves[n], low, high):
                copy.wait_recv()

    def term(j, slot, block, scale):
        return j, place(j, slot, square(rem[block]) * scale)

    def collect(terms):
        for j, s in terms:
            mats[j * ST : j * ST + B, :] = mats[j * ST : j * ST + B, :] + s

    for n in range(N):
        t = own(n, 0)
        if n > 0:
            t = t + own(n - 1, 2)
        if n < N - 1:
            t = t + own(n + 1, 3)
        send_ahead(n, t)
        if n == 1:
            hear(0)
            depart(0, 0, 2)
            depart(1, 0, 2)
            tell(1)
    depart(3, 0, 4)
    hear(1)
    tell(2)
    own(N - 1, 2)
    own(0, 3)
    for j in range(N):
        t = own(j, 1)
        if j < N - 1:
            place(j + 1, 5, t)
            mats[(j + 1) * ST : (j + 1) * ST + B, :] = mats[(j + 1) * ST : (j + 1) * ST + B, :] + t

    arrived(2, 0, 2)
    arrived(0, 0, 2)
    arrived(1, 0, 2)
    collect([
        term(0, 6, N, rlm[1, 3 * N - 1 : 3 * N, :]),
        term(N - 1, 7, 3 * N - 1, rlm[2, 3 * N : 3 * N + 1, :]),
        term(0, 5, 3 * N, rlm[3, 2 * N - 1 : 2 * N, :]),
    ])

    for n in range(N):
        pl.when(exists(-1, 0))(ahead(n).wait_recv)
    for n in range(N):
        mats[n * ST : n * ST + B, :] = mats[n * ST : n * ST + B, :] + unpack(n)

    for m in range(N):
        a, b, c = split3(mats[m * ST : m * ST + B, :])
        dpan[m, 0:B, 0:B] = a
        dpan[m, 0:B, B : 2 * B] = b
        dpan[m, B : 2 * B, 0:B] = b
        dpan[m, B : 2 * B, B : 2 * B] = a
        dpan[m, 0:B, 2 * B :] = a
        dpan[m, B : 2 * B, 2 * B :] = c
    invert(mats, rpan, cpan)
    hear(2)

    def pairs(terms):
        return jnp.concatenate([jnp.concatenate([t, t], axis=1) for t in terms], axis=0)

    def fold(out, h):
        small = (out[2 * h :, 0:B] + out[2 * h :, B:]) + out[h : 2 * h, B:]
        return out[0:h, 0:B] + (out[h : 2 * h, 0:B] + (out[0:h, B:] + small))

    for m in range(N):
        a, b, c = split3(mats[m * ST : m * ST + B, :])
        pre[m, 0:B, 0:B] = a
        pre[m, 0:B, B : 2 * B] = b
        large = jnp.dot(jnp.concatenate([a, b], axis=1), dpan[m, :, 0 : 2 * B], preferred_element_type=f32)
        small = jnp.dot(jnp.concatenate([c, a], axis=1), dpan[m, :, 2 * B :], preferred_element_type=f32)
        product = (small + large[:, B:]) + large[:, 0:B]
        errs[m] = (jnp.where(eye, 1.0, 0.0) - product).astype(bf16)
    better = []
    for m in range(N):
        fix = jnp.dot(errs[m], pre[m, 0:B, :], preferred_element_type=f32)
        better.append(mats[m * ST : m * ST + B, :] + (fix[:, 0:B] + fix[:, B:]))
    for m in range(N):
        a, b, c = split3(better[m])
        pre[m, 0:B, 0:B] = a
        pre[m, 0:B, B : 2 * B] = b
        pre[m, B : 2 * B, 0:B] = c
        pre[m, B : 2 * B, B : 2 * B] = jnp.zeros((B, B), bf16)

    copies[3].wait()
    x_out[...] = jnp.zeros_like(x_out)
    dirn[...] = jnp.zeros_like(dirn)
    along[...] = jnp.zeros_like(along)
    qdir[...] = jnp.zeros_like(qdir)
    zdir[...] = jnp.zeros_like(zdir)

    def precondition(v, m):
        return fold(jnp.dot(pairs(split3(v)), pre[m], preferred_element_type=f32), R)

    def operate(par, j):
        centre = ext[par, 1, 1 + j]
        terms = []
        for sign in (1, -1):
            for sx, sy in OFFSETS:
                terms.append(split3(centre - ext[par, 1 + sign * sx, 1 + j + sign * sy]))
        left = jnp.concatenate(
            [jnp.concatenate([t[i] for t in terms], axis=1) for i in range(3)], axis=0)
        out = fold(jnp.dot(left, wts[j], preferred_element_type=f32), R)
        return out + shift[j] * centre

    def halo(par):
        for n, (sx, sy) in enumerate(SIDES):
            if sy == 0:
                src = ext.at[par, 1, pl.ds(1, N)]
                dst = ext.at[par, 1 - sx, pl.ds(1, N)]
            else:
                src = ext.at[par, 1, N if sy == 1 else 1]
                dst = ext.at[par, 1 - sx, 0 if sy == 1 else N + 1]
            yield sx, sy, remote(src, dst, hsend.at[n], hrecv.at[par, n], sx, sy)

    def halo_start(par):
        for sx, sy, copy in halo(par):
            pl.when(exists(sx, sy))(copy.start)

    def halo_wait(par):
        for sx, sy, copy in halo(par):
            pl.when(exists(-sx, -sy))(copy.wait_recv)

    def halo_sent(par):
        for sx, sy, copy in halo(par):
            pl.when(exists(sx, sy))(copy.wait_send)

    lane = lax.broadcasted_iota(jnp.int32, (R, B), 1)
    rhs = lax.broadcasted_iota(jnp.int32, (R, B), 0)

    def contribution(par, peer):
        return pltpu.make_async_remote_copy(
            src_ref=dsend.at[pl.ds(par, 1)], dst_ref=drecv.at[par, pl.ds(me, 1)],
            send_sem=ssend, recv_sem=srecv.at[par],
            device_id=peer, device_id_type=pl.DeviceIdType.MESH)

    def products(par, triples):
        gsum, dsum = None, None
        for r, u, w in triples:
            g, d = u * r, u * w
            gsum = g if gsum is None else gsum + g
            dsum = d if dsum is None else dsum + d
        gcol = jnp.sum(gsum, axis=1, keepdims=True)
        dcol = jnp.sum(dsum, axis=1, keepdims=True)
        spread = jnp.where(lane == rhs, gcol, jnp.where(lane == rhs + R, dcol, 0.0))
        row = jnp.sum(spread, axis=0, keepdims=True)
        dsend[pl.ds(par, 1), :] = row
        drecv[par, pl.ds(me, 1), :] = row
        for peer in peers:
            contribution(par, peer).start()

    def totals(par, first, gamma_old, alpha_old):
        everything = drecv.at[par, pl.ds(0, PLANE - 1)]
        pltpu.make_async_copy(everything, everything, srecv.at[par]).wait()
        pltpu.make_async_copy(everything, everything, ssend).wait()
        total = jnp.sum(drecv[par], axis=0, keepdims=True)
        gamma = jnp.sum(jnp.where(lane == rhs, total, 0.0), axis=1, keepdims=True)
        delta = jnp.sum(jnp.where(lane == rhs + R, total, 0.0), axis=1, keepdims=True)
        ratio = jnp.where(first, 0.0, gamma / gamma_old)
        alpha = gamma / (delta - ratio * gamma / alpha_old)
        return gamma, ratio, alpha

    for j in range(N):
        ext[1, 1, 1 + j] = precondition(res[0, j], j)
    halo_start(1)
    arrived(3, 0, 2)
    for j in range(N):
        term(j, 4, j, rlm[0, j : j + 1, :])
    arrived(3, 2, 3)
    for j in range(1, N):
        term(j, 6, N + j, rlm[0, 2 * N + j - 1 : 2 * N + j, :])
    arrived(3, 3, 4)
    for j in range(N - 1):
        term(j, 7, 2 * N + j, rlm[0, 3 * N + j + 1 : 3 * N + j + 2, :])
    halo_wait(1)
    triples = []
    for j in range(N):
        u, w = ext[1, 1, 1 + j], operate(1, j)
        pre_u[j], img[j] = u, w
        triples.append((res[0, j], u, w))
    products(0, triples)
    halo_sent(1)
    for sx, sy, blocks, n in moves:
        @pl.when(exists(sx, sy))
        def _():
            for copy in rim_copies(sx, sy, blocks, n):
                copy.wait_send()
    for n in range(N):
        pl.when(exists(1, 0))(ahead(n).wait_send)

    def iterate(it, carry):
        gamma_old, alpha_old = carry
        par = lax.rem(it, 2)
        for j in range(N):
            ext[par, 1, 1 + j] = precondition(img[j], j)
        halo_start(par)
        halo_wait(par)
        for j in range(N):
            push[j] = operate(par, j)
        gamma, ratio, alpha = totals(par, it == 0, gamma_old, alpha_old)
        triples = []
        for j in range(N):
            u, w = pre_u[j], img[j]
            z = push[j] + ratio * zdir[j]
            q = ext[par, 1, 1 + j] + ratio * qdir[j]
            s = w + ratio * along[j]
            p = u + ratio * dirn[j]
            zdir[j], qdir[j], along[j], dirn[j] = z, q, s, p
            x_out[0, j] = x_out[0, j] + alpha * p
            r = res[0, j] - alpha * s
            u = u - alpha * q
            w = w - alpha * z
            res[0, j], pre_u[j], img[j] = r, u, w
            triples.append((r, u, w))
        products(1 - par, triples)
        halo_sent(par)
        return gamma, alpha

    one = jnp.ones((R, 1), f32)
    gamma_old, alpha_old = lax.fori_loop(0, ITERS - 1, iterate, (one, one))
    gamma, ratio, alpha = totals((ITERS - 1) % 2, ITERS == 1, gamma_old, alpha_old)
    for j in range(N):
        x_out[0, j] = x_out[0, j] + alpha * (pre_u[j] + ratio * dirn[j])
        r_out[0, j] = res[0, j] - alpha * (img[j] + ratio * along[j])


def local(load, factors, links, shift):
    vmem = pl.BlockSpec(memory_space=pltpu.VMEM)
    hbm = pl.BlockSpec(memory_space=pltpu.HBM)
    field = jax.ShapeDtypeStruct((1, N, R, B), f32)
    return pl.pallas_call(
        kernel,
        out_shape=(field, field),
        in_specs=[hbm] * 4,
        out_specs=(vmem, vmem),
        scratch_shapes=[
            pltpu.SMEM((4, 1, N), jnp.int32),
            pltpu.VMEM((N, 1, B), f32),
            pltpu.VMEM((4 * N, B, B), bf16),
            pltpu.VMEM((3 * N + 1, B, B), bf16),
            pltpu.VMEM((4 * N, B), f32),
            pltpu.VMEM((4, 4 * N, B), f32),
            pltpu.VMEM((8 * ST, B), f32),
            pltpu.VMEM((8 * NB, B), f32),
            pltpu.VMEM((8 * NB, B), f32),
            pltpu.VMEM((N, 2 * B, 3 * B), bf16),
            pltpu.VMEM((N, B, B), bf16),
            pltpu.VMEM((N, 8 * B, 2 * B), bf16),
            pltpu.VMEM((N, 2 * B, 2 * B), bf16),
            pltpu.VMEM((2, 3, N + 2, R, B), f32),
            pltpu.VMEM((N, R, B), f32),
            pltpu.VMEM((N, R, B), f32),
            pltpu.VMEM((N, R, B), f32),
            pltpu.VMEM((N, R, B), f32),
            pltpu.VMEM((1, N, R, B), f32),
            pltpu.VMEM((N, R, B), f32),
            pltpu.VMEM((N, R, B), f32),
            pltpu.VMEM((N, R, B), f32),
            pltpu.VMEM((8, B), f32),
            pltpu.VMEM((2, PLANE, B), f32),
            pltpu.SemaphoreType.DMA((4,)),
            pltpu.SemaphoreType.DMA((16,)),
            pltpu.SemaphoreType.DMA((16,)),
            pltpu.SemaphoreType.DMA((8,)),
            pltpu.SemaphoreType.DMA((2, 8)),
            pltpu.SemaphoreType.DMA,
            pltpu.SemaphoreType.DMA((2,)),
            pltpu.SemaphoreType.REGULAR((3,)),
            pltpu.VMEM((N, 5 * B // 8, B), f32),
            pltpu.VMEM((N, 5 * B // 8, B), f32),
            pltpu.SemaphoreType.DMA((2, N)),
        ],
        compiler_params=pltpu.CompilerParams(collective_id=0, has_side_effects=True, vmem_limit_bytes=24 * 1024 * 1024),
        name="solve",
    )(*[pltpu.with_memory_space_constraint(t, pltpu.HBM) for t in (links, load, factors.reshape(4 * N, B, B), shift.reshape(N, 1, B))])


def solution(mesh):
    placed = (
        P(("case", "gx"), "gy", None, None),
        P(None, ("case", "gx"), "gy", None, None),
        P(None, ("case", "gx"), "gy"),
        P(("case", "gx"), "gy", None),
    )
    return jax.shard_map(
        local,
        mesh=mesh,
        in_specs=placed,
        out_specs=(P(("case", "gx"), "gy", None, None), P(("case", "gx"), "gy", None, None)),
        check_vma=False,
    )
```

```python
import functools

import jax
import jax.numpy as jnp
from jax import lax
from jax.experimental import pallas as pl
from jax.experimental.pallas import tpu as pltpu
from jax.sharding import PartitionSpec as P

B = 128
N = 6
R = 32
ITERS = 8
NB = 8
ST = 136
GXN = 8
GYN = 4
PLANE = GXN * GYN
OFFSETS = ((1, 0), (0, 1), (1, 1), (1, -1))
SIDES = ((1, 1), (1, -1), (-1, 1), (-1, -1), (1, 0), (-1, 0), (0, 1), (0, -1))
f32 = jnp.float32
bf16 = jnp.bfloat16


def split3(x):
    a = x.astype(bf16)
    left = x - a.astype(f32)
    b = left.astype(bf16)
    c = (left - b.astype(f32)).astype(bf16)
    return a, b, c


def split2(x):
    a = x.astype(bf16)
    return a, (x - a.astype(f32)).astype(bf16)


def invert(mats, rpan, cpan):
    lane = lax.broadcasted_iota(jnp.int32, (8, B), 1)

    def packed(base):
        return [mats[pl.ds(base + i, 8, stride=ST), :] for i in range(NB)]

    def pick(row, k):
        return jnp.sum(jnp.where(lane == k, row, 0.0), axis=1, keepdims=True)

    def pivot(rows, base):
        e = {}
        for j in range(NB):
            for i in range(j + 1):
                e[i, j] = pick(rows[i], base + j)
        ahead = [[pick(rows[k], base + NB + i) for k in range(NB)] for i in range(NB)]
        inside = (lane >= base) & (lane < base + NB)
        sign = jnp.where(lane < base, -1.0, jnp.where(inside, 0.0, 1.0))
        at = lambda i, j: e[min(i, j), max(i, j)]
        for k in range(NB):
            p = 1.0 / e[k, k]
            col = [at(i, k) for i in range(NB)]
            scaled = [c * p for c in col]
            for i in range(NB):
                for j in range(i, NB):
                    if i != k and j != k:
                        e[i, j] = e[i, j] - scaled[i] * col[j]
            for i in range(NB):
                if i != k:
                    e[min(i, k), max(i, k)] = scaled[i]
            e[k, k] = -p
        panel = [jnp.where(lane == base + i, 1.0, jnp.where(inside, 0.0, rows[i])) for i in range(NB)]
        right = []
        for j in range(NB):
            total = None
            for i in range(NB):
                term = at(i, j) * panel[i]
                total = term if total is None else total + term
            right.append(-total)
        following = packed(jnp.minimum(base + NB, B - NB))
        after = []
        for i in range(NB):
            row = jnp.where(inside, 0.0, following[i])
            for k in range(NB):
                row = row - ahead[i][k] * right[k]
            after.append(row)
        for k in range(NB):
            cpan[pl.ds(k, 8, stride=NB), :] = rows[k] * sign
            rpan[pl.ds(k, 8, stride=NB), :] = right[k]
        return tuple(after)

    def trail(base):
        inside = (lane >= base) & (lane < base + NB)
        rows = [rpan[m * NB : (m + 1) * NB, :] for m in range(N)]
        ups = []
        for m in range(N):
            c0, c1, c2 = split3(cpan[m * NB : (m + 1) * NB, :])
            r0, r1, r2 = split3(rows[m])
            ups.append(lax.dot_general(
                jnp.concatenate([c0, c0, c1, c1, c0, c2], axis=0),
                jnp.concatenate([r0, r1, r0, r1, r2, r0], axis=0),
                (((0,), (0,)), ((), ())), preferred_element_type=f32))
        new = [jnp.where(inside[0:1, :], 0.0, mats[m * ST : m * ST + B, :]) - ups[m] for m in range(N)]
        for m in range(N):
            mats[m * ST : m * ST + B, :] = new[m]
        for m in range(N):
            mats[pl.ds(pl.multiple_of(m * ST + base, 8), 8), :] = rows[m]

    def step(b, rows):
        trail((b - 1) * NB)
        return pivot(rows, b * NB)

    rows = pivot(packed(0), 0)
    lax.fori_loop(1, B // NB, step, rows)
    trail(B - NB)


def kernel(links_in, load, factors, shift_in, x_out, r_out, links, shift, fac, rem, lm, rlm, mats, rpan, cpan, dpan, errs, wts, pre, ext,
           pre_u, push, qdir, zdir, res, dirn, along, img, dsend, drecv, lsem, fsend, frecv, hsend, hrecv, ssend, srecv, known,
           tsend, trecv, tsems):
    case = lax.axis_index("case")
    gx = lax.axis_index("gx")
    gy = lax.axis_index("gy")
    me = gx * GYN + gy

    def device(x, y):
        return (case, x, y)

    def exists(sx, sy):
        ok = None
        for pos, step, count in ((gx, sx, GXN), (gy, sy, GYN)):
            if step == 0:
                continue
            here = (pos + step >= 0) & (pos + step < count)
            ok = here if ok is None else ok & here
        return ok

    barrier = pltpu.get_barrier_semaphore()
    peers = []
    hops = lambda a, c: -(min((a + 1) // 2, (GXN - a + 1) // 2) + min(c, GYN - c))
    for a, c in sorted([(a, c) for a in range(GXN) for c in range(GYN)], key=lambda t: hops(*t)):
        if a or c:
            peers.append(device(lax.rem(gx + a, GXN), lax.rem(gy + c, GYN)))

    def ring(dx, dy):
        return device(lax.rem(gx + dx + GXN, GXN), lax.rem(gy + dy + GYN, GYN))

    greeted = [ring(1, 0), ring(-1, 0), ring(0, 1), ring(0, -1)]
    rounds = [greeted, [ring(2, 0), ring(-2, 0), ring(0, 2)], [ring(d, 0) for d in range(1, GXN)]]
    for peer in greeted:
        pl.semaphore_signal(barrier, inc=1, device_id=peer, device_id_type=pl.DeviceIdType.MESH)

    def tell(i):
        for peer in rounds[i]:
            pl.semaphore_signal(known.at[i], inc=1, device_id=peer, device_id_type=pl.DeviceIdType.MESH)

    def hear(i):
        pl.semaphore_wait(known.at[i], len(rounds[i]))

    copies = [
        pltpu.make_async_copy(factors, fac, lsem.at[0]),
        pltpu.make_async_copy(links_in, links, lsem.at[1]),
        pltpu.make_async_copy(shift_in, shift, lsem.at[2]),
        pltpu.make_async_copy(load, res, lsem.at[3]),
    ]
    for copy in copies:
        copy.start()
    copies[1].wait()
    for d in range(4):
        for j in range(N):
            lm[d * N + j : d * N + j + 1, :] = jnp.full((1, B), links[d, 0, j], jnp.int32).astype(f32) * (1.0 / B)
    copies[0].wait()

    def remote(src, dst, ss, rs, sx, sy):
        return pltpu.make_async_remote_copy(
            src_ref=src, dst_ref=dst, send_sem=ss, recv_sem=rs,
            device_id=device(gx + sx, gy + sy), device_id_type=pl.DeviceIdType.MESH)

    moves = (
        (1, 1, ((17, 1, 6),), 1),
        (1, -1, ((18, 1, 17),), 2),
        (0, 1, ((11, 1, 18),), 3),
        (1, 0, ((0, 6, 0), (12, 5, 7), (19, 5, 12)), 0),
    )

    def rim_copies(sx, sy, blocks, n, low=0, high=4):
        parts = [(lm, rlm.at[n], n * 4 + 3)]
        for i, (src, count, dst) in enumerate(blocks):
            parts.append((fac.at[pl.ds(src, count)], rem.at[pl.ds(dst, count)], n * 4 + i))
        return [remote(src, dst, fsend.at[i], frecv.at[i], sx, sy) for src, dst, i in parts[low:high]]

    def depart(n, low, high):
        sx, sy, _, _ = moves[n]
        @pl.when(exists(sx, sy))
        def _():
            for copy in rim_copies(*moves[n], low, high):
                copy.start()

    copies[2].wait()

    def square(block):
        return lax.dot_general(block, block, (((1,), (1,)), ((), ())), preferred_element_type=f32)

    def place(j, slot, s):
        a, b = split2(s)
        wts[j, slot * B : (slot + 1) * B, 0:B] = a
        wts[j, slot * B : (slot + 1) * B, B : 2 * B] = b
        return a.astype(f32) + b.astype(f32)

    row_id = lax.broadcasted_iota(jnp.int32, (B, B), 0)
    lane_id = lax.broadcasted_iota(jnp.int32, (B, B), 1)
    eye = row_id == lane_id

    for m in range(N):
        mats[m * ST : m * ST + B, :] = jnp.where(eye, shift[m], 0.0)
    for m in range(N, 8):
        mats[m * ST : m * ST + B, :] = jnp.where(eye, 1.0, 0.0)

    def ahead(n):
        return remote(tsend.at[n], trecv.at[n], tsems.at[0, n], tsems.at[1, n], 1, 0)

    quarter = B // 4
    lane_q = lax.broadcasted_iota(jnp.int32, (quarter, B), 1)
    lane_h = lax.broadcasted_iota(jnp.int32, (quarter // 2, B), 1)
    above = row_id // quarter <= lane_id // quarter

    def own(j, d):
        s = place(j, d, square(fac[d * N + j]) * lm[d * N + j : d * N + j + 1, :])
        mats[j * ST : j * ST + B, :] = mats[j * ST : j * ST + B, :] + s
        return s

    def send_ahead(n, t):
        q = [t[k * quarter : (k + 1) * quarter] for k in range(4)]
        tsend[n, 0:quarter, :] = q[0]
        tsend[n, quarter : 2 * quarter, :] = jnp.where(lane_q < quarter, pltpu.roll(q[3], quarter, 1), q[1])
        tsend[n, 2 * quarter :, :] = jnp.where(
            lane_h < 2 * quarter, pltpu.roll(q[2][: quarter // 2], 2 * quarter, 1), q[2][quarter // 2 :])

    def unpack(n):
        p0, p1, p2 = trecv[n, 0:quarter, :], trecv[n, quarter : 2 * quarter, :], trecv[n, 2 * quarter :, :]
        upper = jnp.concatenate(
            [p0, p1, pltpu.roll(p2, 2 * quarter, 1), p2, pltpu.roll(p1, 3 * quarter, 1)], axis=0)
        return jnp.where(above, upper, upper.T)

    def arrived(n, low, high):
        sx, sy, _, _ = moves[n]
        @pl.when(exists(-sx, -sy))
        def _():
            for copy in rim_copies(*moves[n], low, high):
                copy.wait_recv()

    def term(j, slot, block, scale):
        return j, place(j, slot, square(rem[block]) * scale)

    def collect(terms):
        for j, s in terms:
            mats[j * ST : j * ST + B, :] = mats[j * ST : j * ST + B, :] + s

    def first(n):
        t = own(n, 0)
        if n > 0:
            t = t + own(n - 1, 2)
        if n < N - 1:
            t = t + own(n + 1, 3)
        send_ahead(n, t)

    early = 2
    for n in range(early):
        first(n)
    pl.semaphore_wait(barrier, len(greeted))
    for n in range(early):
        pl.when(exists(1, 0))(ahead(n).start)
    depart(2, 0, 2)
    tell(0)
    for n in range(early, N):
        first(n)
        pl.when(exists(1, 0))(ahead(n).start)
        if n == early:
            hear(0)
            depart(0, 0, 2)
            depart(1, 0, 2)
            tell(1)
    depart(3, 0, 4)
    hear(1)
    tell(2)
    own(N - 1, 2)
    own(0, 3)
    for j in range(N):
        t = own(j, 1)
        if j < N - 1:
            place(j + 1, 5, t)
            mats[(j + 1) * ST : (j + 1) * ST + B, :] = mats[(j + 1) * ST : (j + 1) * ST + B, :] + t

    def clear(ref, *spans):
        for span in spans:
            ref[span] = jnp.zeros_like(ref[span])

    @pl.when(gx == 0)
    def _():
        clear(ext, (slice(None), 0))
        clear(rem, slice(0, 3 * N))
        clear(rlm, slice(0, 3))
        clear(trecv, slice(None))

    @pl.when(gx == GXN - 1)
    def _():
        clear(ext, (slice(None), 2))

    @pl.when(gy == 0)
    def _():
        clear(ext, (slice(None), slice(None), 0))
        clear(rem, N, 3 * N)
        clear(rlm, 1, 3)

    @pl.when(gy == GYN - 1)
    def _():
        clear(ext, (slice(None), slice(None), N + 1))
        clear(rem, 3 * N - 1)
        clear(rlm, 2)

    arrived(2, 0, 2)
    arrived(0, 0, 2)
    arrived(1, 0, 2)
    collect([
        term(0, 6, N, rlm[1, 3 * N - 1 : 3 * N, :]),
        term(N - 1, 7, 3 * N - 1, rlm[2, 3 * N : 3 * N + 1, :]),
        term(0, 5, 3 * N, rlm[3, 2 * N - 1 : 2 * N, :]),
    ])

    for n in range(N):
        pl.when(exists(-1, 0))(ahead(n).wait_recv)
    for n in range(N):
        mats[n * ST : n * ST + B, :] = mats[n * ST : n * ST + B, :] + unpack(n)

    for m in range(N):
        a, b, c = split3(mats[m * ST : m * ST + B, :])
        dpan[m, 0:B, 0:B] = a
        dpan[m, 0:B, B : 2 * B] = b
        dpan[m, B : 2 * B, 0:B] = b
        dpan[m, B : 2 * B, B : 2 * B] = a
        dpan[m, 0:B, 2 * B :] = a
        dpan[m, B : 2 * B, 2 * B :] = c
    invert(mats, rpan, cpan)
    hear(2)

    def pairs(terms):
        return jnp.concatenate([jnp.concatenate([t, t], axis=1) for t in terms], axis=0)

    def fold(out, h):
        small = (out[2 * h :, 0:B] + out[2 * h :, B:]) + out[h : 2 * h, B:]
        return out[0:h, 0:B] + (out[h : 2 * h, 0:B] + (out[0:h, B:] + small))

    for m in range(N):
        a, b, c = split3(mats[m * ST : m * ST + B, :])
        pre[m, 0:B, 0:B] = a
        pre[m, 0:B, B : 2 * B] = b
        large = jnp.dot(jnp.concatenate([a, b], axis=1), dpan[m, :, 0 : 2 * B], preferred_element_type=f32)
        small = jnp.dot(jnp.concatenate([c, a], axis=1), dpan[m, :, 2 * B :], preferred_element_type=f32)
        product = (small + large[:, B:]) + large[:, 0:B]
        errs[m] = (jnp.where(eye, 1.0, 0.0) - product).astype(bf16)
    better = []
    for m in range(N):
        fix = jnp.dot(errs[m], pre[m, 0:B, :], preferred_element_type=f32)
        better.append(mats[m * ST : m * ST + B, :] + (fix[:, 0:B] + fix[:, B:]))
    for m in range(N):
        a, b, c = split3(better[m])
        pre[m, 0:B, 0:B] = a
        pre[m, 0:B, B : 2 * B] = b
        pre[m, B : 2 * B, 0:B] = c
        pre[m, B : 2 * B, B : 2 * B] = jnp.zeros((B, B), bf16)

    copies[3].wait()

    def precondition(v, m):
        return fold(jnp.dot(pairs(split3(v)), pre[m], preferred_element_type=f32), R)

    def operate(par, j):
        centre = ext[par, 1, 1 + j]
        terms = []
        for sign in (1, -1):
            for sx, sy in OFFSETS:
                terms.append(split3(centre - ext[par, 1 + sign * sx, 1 + j + sign * sy]))
        left = jnp.concatenate(
            [jnp.concatenate([t[i] for t in terms], axis=1) for i in range(3)], axis=0)
        out = fold(jnp.dot(left, wts[j], preferred_element_type=f32), R)
        return out + shift[j] * centre

    def halo(par):
        for n, (sx, sy) in enumerate(SIDES):
            if sy == 0:
                src = ext.at[par, 1, pl.ds(1, N)]
                dst = ext.at[par, 1 - sx, pl.ds(1, N)]
            else:
                src = ext.at[par, 1, N if sy == 1 else 1]
                dst = ext.at[par, 1 - sx, 0 if sy == 1 else N + 1]
            yield sx, sy, remote(src, dst, hsend.at[n], hrecv.at[par, n], sx, sy)

    def halo_start(par):
        for sx, sy, copy in halo(par):
            pl.when(exists(sx, sy))(copy.start)

    def halo_wait(par):
        for sx, sy, copy in halo(par):
            pl.when(exists(-sx, -sy))(copy.wait_recv)

    def halo_sent(par):
        for sx, sy, copy in halo(par):
            pl.when(exists(sx, sy))(copy.wait_send)

    lane = lax.broadcasted_iota(jnp.int32, (R, B), 1)
    rhs = lax.broadcasted_iota(jnp.int32, (R, B), 0)

    def contribution(par, peer):
        return pltpu.make_async_remote_copy(
            src_ref=dsend.at[pl.ds(par, 1)], dst_ref=drecv.at[par, pl.ds(me, 1)],
            send_sem=ssend, recv_sem=srecv.at[par],
            device_id=peer, device_id_type=pl.DeviceIdType.MESH)

    def scatter(par, sums):
        spread = 0.0
        for k, t in reversed(list(enumerate(sums))):
            spread = jnp.where(lane == rhs + k * R, jnp.sum(t, axis=1, keepdims=True), spread)
        row = jnp.sum(spread, axis=0, keepdims=True)
        dsend[pl.ds(par, 1), :] = row
        drecv[par, pl.ds(me, 1), :] = row
        for peer in peers:
            contribution(par, peer).start()

    def gather(par, count):
        everything = drecv.at[par, pl.ds(0, PLANE - 1)]
        pltpu.make_async_copy(everything, everything, srecv.at[par]).wait()
        pltpu.make_async_copy(everything, everything, ssend).wait()
        total = jnp.sum(drecv[par], axis=0, keepdims=True)
        return [jnp.sum(jnp.where(lane == rhs + k * R, total, 0.0), axis=1, keepdims=True) for k in range(count)]

    def products(par, triples):
        gsum, dsum = None, None
        for r, u, w in triples:
            g, d = u * r, u * w
            gsum = g if gsum is None else gsum + g
            dsum = d if dsum is None else dsum + d
        scatter(par, [gsum, dsum])

    def totals(par, gamma_old, alpha_old):
        gamma, delta = gather(par, 2)
        ratio = gamma / gamma_old
        alpha = gamma / (delta - ratio * gamma / alpha_old)
        return gamma, ratio, alpha

    for j in range(N):
        ext[1, 1, 1 + j] = precondition(res[0, j], j)
    halo_start(1)
    arrived(3, 0, 2)
    for j in range(N):
        term(j, 4, j, rlm[0, j : j + 1, :])
    arrived(3, 2, 3)
    for j in range(1, N):
        term(j, 6, N + j, rlm[0, 2 * N + j - 1 : 2 * N + j, :])
    arrived(3, 3, 4)
    for j in range(N - 1):
        term(j, 7, 2 * N + j, rlm[0, 3 * N + j + 1 : 3 * N + j + 2, :])
    halo_wait(1)
    for j in range(N):
        pre_u[j], img[j] = ext[1, 1, 1 + j], operate(1, j)
    halo_sent(1)

    for j in range(N):
        ext[0, 1, 1 + j] = precondition(img[j], j)
    halo_start(0)
    halo_wait(0)
    groups = []
    for j in range(N):
        u, w, m, n = pre_u[j], img[j], ext[0, 1, 1 + j], operate(0, j)
        push[j] = n
        groups.append((u * res[0, j], u * w, w * m, n * m))
    scatter(1, [sum(g[1:], g[0]) for g in zip(*groups)])
    for j in range(N):
        ext[1, 1, 1 + j] = precondition(push[j], j)
    halo_sent(0)
    halo_start(1)
    halo_wait(1)
    for j in range(N):
        zdir[j] = operate(1, j)
    gamma, delta, wm, nm = gather(1, 4)
    alpha = gamma / delta
    gamma_next = gamma - alpha * (2.0 * delta - alpha * wm)
    delta_next = delta - alpha * (2.0 * wm - alpha * nm)
    ratio = gamma_next / gamma
    alpha_next = gamma_next / (delta_next - ratio * gamma_next / alpha)
    triples = []
    for j in range(N):
        u, w, m, n, o, t = pre_u[j], img[j], ext[0, 1, 1 + j], push[j], ext[1, 1, 1 + j], zdir[j]
        u1, w1, m1, n1 = u - alpha * m, w - alpha * n, m - alpha * o, n - alpha * t
        p, s, q, z = u1 + ratio * u, w1 + ratio * w, m1 + ratio * m, n1 + ratio * n
        zdir[j], qdir[j], along[j], dirn[j] = z, q, s, p
        x_out[0, j] = alpha * u + alpha_next * p
        r = res[0, j] - alpha * w - alpha_next * s
        u2, w2 = u1 - alpha_next * q, w1 - alpha_next * z
        res[0, j], pre_u[j], img[j] = r, u2, w2
        triples.append((r, u2, w2))
    products(0, triples)
    halo_sent(1)
    for sx, sy, blocks, n in moves:
        @pl.when(exists(sx, sy))
        def _():
            for copy in rim_copies(sx, sy, blocks, n):
                copy.wait_send()
    for n in range(N):
        pl.when(exists(1, 0))(ahead(n).wait_send)

    def iterate(it, carry):
        gamma_old, alpha_old = carry
        par = lax.rem(it, 2)
        for j in range(N):
            ext[par, 1, 1 + j] = precondition(img[j], j)
        halo_start(par)
        halo_wait(par)
        for j in range(N):
            push[j] = operate(par, j)
        gamma, ratio, alpha = totals(par, gamma_old, alpha_old)
        triples = []
        for j in range(N):
            u, w = pre_u[j], img[j]
            z = push[j] + ratio * zdir[j]
            q = ext[par, 1, 1 + j] + ratio * qdir[j]
            s = w + ratio * along[j]
            p = u + ratio * dirn[j]
            zdir[j], qdir[j], along[j], dirn[j] = z, q, s, p
            x_out[0, j] = x_out[0, j] + alpha * p
            r = res[0, j] - alpha * s
            u = u - alpha * q
            w = w - alpha * z
            res[0, j], pre_u[j], img[j] = r, u, w
            triples.append((r, u, w))
        products(1 - par, triples)
        halo_sent(par)
        return gamma, alpha

    gamma_old, alpha_old = lax.fori_loop(2, ITERS - 1, iterate, (gamma_next, alpha_next))
    gamma, ratio, alpha = totals((ITERS - 1) % 2, gamma_old, alpha_old)
    for j in range(N):
        x_out[0, j] = x_out[0, j] + alpha * (pre_u[j] + ratio * dirn[j])
        r_out[0, j] = res[0, j] - alpha * (img[j] + ratio * along[j])


def local(load, factors, links, shift):
    vmem = pl.BlockSpec(memory_space=pltpu.VMEM)
    hbm = pl.BlockSpec(memory_space=pltpu.HBM)
    field = jax.ShapeDtypeStruct((1, N, R, B), f32)
    return pl.pallas_call(
        kernel,
        out_shape=(field, field),
        in_specs=[hbm] * 4,
        out_specs=(vmem, vmem),
        scratch_shapes=[
            pltpu.SMEM((4, 1, N), jnp.int32),
            pltpu.VMEM((N, 1, B), f32),
            pltpu.VMEM((4 * N, B, B), bf16),
            pltpu.VMEM((3 * N + 1, B, B), bf16),
            pltpu.VMEM((4 * N, B), f32),
            pltpu.VMEM((4, 4 * N, B), f32),
            pltpu.VMEM((8 * ST, B), f32),
            pltpu.VMEM((8 * NB, B), f32),
            pltpu.VMEM((8 * NB, B), f32),
            pltpu.VMEM((N, 2 * B, 3 * B), bf16),
            pltpu.VMEM((N, B, B), bf16),
            pltpu.VMEM((N, 8 * B, 2 * B), bf16),
            pltpu.VMEM((N, 2 * B, 2 * B), bf16),
            pltpu.VMEM((2, 3, N + 2, R, B), f32),
            pltpu.VMEM((N, R, B), f32),
            pltpu.VMEM((N, R, B), f32),
            pltpu.VMEM((N, R, B), f32),
            pltpu.VMEM((N, R, B), f32),
            pltpu.VMEM((1, N, R, B), f32),
            pltpu.VMEM((N, R, B), f32),
            pltpu.VMEM((N, R, B), f32),
            pltpu.VMEM((N, R, B), f32),
            pltpu.VMEM((8, B), f32),
            pltpu.VMEM((2, PLANE, B), f32),
            pltpu.SemaphoreType.DMA((4,)),
            pltpu.SemaphoreType.DMA((16,)),
            pltpu.SemaphoreType.DMA((16,)),
            pltpu.SemaphoreType.DMA((8,)),
            pltpu.SemaphoreType.DMA((2, 8)),
            pltpu.SemaphoreType.DMA,
            pltpu.SemaphoreType.DMA((2,)),
            pltpu.SemaphoreType.REGULAR((3,)),
            pltpu.VMEM((N, 5 * B // 8, B), f32),
            pltpu.VMEM((N, 5 * B // 8, B), f32),
            pltpu.SemaphoreType.DMA((2, N)),
        ],
        compiler_params=pltpu.CompilerParams(collective_id=0, has_side_effects=True, vmem_limit_bytes=24 * 1024 * 1024),
        name="solve",
    )(*[pltpu.with_memory_space_constraint(t, pltpu.HBM) for t in (links, load, factors.reshape(4 * N, B, B), shift.reshape(N, 1, B))])


def solution(mesh):
    placed = (
        P(("case", "gx"), "gy", None, None),
        P(None, ("case", "gx"), "gy", None, None),
        P(None, ("case", "gx"), "gy"),
        P(("case", "gx"), "gy", None),
    )
    return jax.shard_map(
        local,
        mesh=mesh,
        in_specs=placed,
        out_specs=(P(("case", "gx"), "gy", None, None), P(("case", "gx"), "gy", None, None)),
        check_vma=False,
    )
```

```python
import functools

import jax
import jax.numpy as jnp
from jax import lax
from jax.experimental import pallas as pl
from jax.experimental.pallas import tpu as pltpu
from jax.sharding import PartitionSpec as P

B = 128
N = 6
R = 32
ITERS = 8
NB = 8
ST = 136
GXN = 8
GYN = 4
PLANE = GXN * GYN
CUT = 3
OFFSETS = ((1, 0), (0, 1), (1, 1), (1, -1))
SIDES = ((1, 1), (1, -1), (-1, 1), (-1, -1), (1, 0), (-1, 0), (0, 1), (0, -1))
f32 = jnp.float32
bf16 = jnp.bfloat16


def split3(x):
    a = x.astype(bf16)
    left = x - a.astype(f32)
    b = left.astype(bf16)
    c = (left - b.astype(f32)).astype(bf16)
    return a, b, c


def split2(x):
    a = x.astype(bf16)
    return a, (x - a.astype(f32)).astype(bf16)


def invert(mats, rpan, cpan):
    lane = lax.broadcasted_iota(jnp.int32, (8, B), 1)

    def packed(base):
        return [mats[pl.ds(base + i, 8, stride=ST), :] for i in range(NB)]

    def pick(row, k):
        return jnp.sum(jnp.where(lane == k, row, 0.0), axis=1, keepdims=True)

    def pivot(rows, base):
        e = {}
        for j in range(NB):
            for i in range(j + 1):
                e[i, j] = pick(rows[i], base + j)
        ahead = [[pick(rows[k], base + NB + i) for k in range(NB)] for i in range(NB)]
        inside = (lane >= base) & (lane < base + NB)
        sign = jnp.where(lane < base, -1.0, jnp.where(inside, 0.0, 1.0))
        at = lambda i, j: e[min(i, j), max(i, j)]
        for k in range(NB):
            p = 1.0 / e[k, k]
            col = [at(i, k) for i in range(NB)]
            scaled = [c * p for c in col]
            for i in range(NB):
                for j in range(i, NB):
                    if i != k and j != k:
                        e[i, j] = e[i, j] - scaled[i] * col[j]
            for i in range(NB):
                if i != k:
                    e[min(i, k), max(i, k)] = scaled[i]
            e[k, k] = -p
        panel = [jnp.where(lane == base + i, 1.0, jnp.where(inside, 0.0, rows[i])) for i in range(NB)]
        right = []
        for j in range(NB):
            total = None
            for i in range(NB):
                term = at(i, j) * panel[i]
                total = term if total is None else total + term
            right.append(-total)
        following = packed(jnp.minimum(base + NB, B - NB))
        after = []
        for i in range(NB):
            row = jnp.where(inside, 0.0, following[i])
            for k in range(NB):
                row = row - ahead[i][k] * right[k]
            after.append(row)
        for k in range(NB):
            cpan[pl.ds(k, 8, stride=NB), :] = rows[k] * sign
            rpan[pl.ds(k, 8, stride=NB), :] = right[k]
        return tuple(after)

    def trail(base):
        inside = (lane >= base) & (lane < base + NB)
        rows = [rpan[m * NB : (m + 1) * NB, :] for m in range(N)]
        ups = []
        for m in range(N):
            c0, c1, c2 = split3(cpan[m * NB : (m + 1) * NB, :])
            r0, r1, r2 = split3(rows[m])
            ups.append(lax.dot_general(
                jnp.concatenate([c0, c0, c1, c1, c0, c2], axis=0),
                jnp.concatenate([r0, r1, r0, r1, r2, r0], axis=0),
                (((0,), (0,)), ((), ())), preferred_element_type=f32))
        new = [jnp.where(inside[0:1, :], 0.0, mats[m * ST : m * ST + B, :]) - ups[m] for m in range(N)]
        for m in range(N):
            mats[m * ST : m * ST + B, :] = new[m]
        for m in range(N):
            mats[pl.ds(pl.multiple_of(m * ST + base, 8), 8), :] = rows[m]

    def step(b, rows):
        trail((b - 1) * NB)
        return pivot(rows, b * NB)

    rows = pivot(packed(0), 0)
    lax.fori_loop(1, B // NB, step, rows)
    trail(B - NB)


def kernel(links_in, load, factors, shift_in, x_out, r_out, links, shift, fac, rem, lm, rlm, mats, rpan, cpan, dpan, errs, wts, pre, ext,
           pre_u, push, qdir, zdir, res, dirn, along, img, dsend, drecv, lsem, fsend, frecv, hsend, hrecv, ssend, srecv, known,
           tsend, trecv, tsems):
    case = lax.axis_index("case")
    gx = lax.axis_index("gx")
    gy = lax.axis_index("gy")
    me = gx * GYN + gy

    def device(x, y):
        return (case, x, y)

    def exists(sx, sy):
        ok = None
        for pos, step, count in ((gx, sx, GXN), (gy, sy, GYN)):
            if step == 0:
                continue
            here = (pos + step >= 0) & (pos + step < count)
            ok = here if ok is None else ok & here
        return ok

    barrier = pltpu.get_barrier_semaphore()
    peers = []
    hops = lambda a, c: -(min((a + 1) // 2, (GXN - a + 1) // 2) + min(c, GYN - c))
    for a, c in sorted([(a, c) for a in range(GXN) for c in range(GYN)], key=lambda t: hops(*t)):
        if a or c:
            peers.append(device(lax.rem(gx + a, GXN), lax.rem(gy + c, GYN)))

    def ring(dx, dy):
        return device(lax.rem(gx + dx + GXN, GXN), lax.rem(gy + dy + GYN, GYN))

    greeted = [ring(1, 0), ring(-1, 0), ring(0, 1), ring(0, -1)]
    rounds = [greeted, [ring(2, 0), ring(-2, 0), ring(0, 2)], [ring(d, 0) for d in range(1, GXN)]]
    for peer in greeted:
        pl.semaphore_signal(barrier, inc=1, device_id=peer, device_id_type=pl.DeviceIdType.MESH)

    def tell(i):
        for peer in rounds[i]:
            pl.semaphore_signal(known.at[i], inc=1, device_id=peer, device_id_type=pl.DeviceIdType.MESH)

    def hear(i):
        pl.semaphore_wait(known.at[i], len(rounds[i]))

    copies = [
        pltpu.make_async_copy(factors, fac, lsem.at[0]),
        pltpu.make_async_copy(links_in, links, lsem.at[1]),
        pltpu.make_async_copy(shift_in, shift, lsem.at[2]),
        pltpu.make_async_copy(load, res, lsem.at[3]),
    ]
    for copy in copies:
        copy.start()
    copies[1].wait()
    for d in range(4):
        for j in range(N):
            lm[d * N + j : d * N + j + 1, :] = jnp.full((1, B), links[d, 0, j], jnp.int32).astype(f32) * (1.0 / B)
    copies[0].wait()

    def remote(src, dst, ss, rs, sx, sy):
        return pltpu.make_async_remote_copy(
            src_ref=src, dst_ref=dst, send_sem=ss, recv_sem=rs,
            device_id=device(gx + sx, gy + sy), device_id_type=pl.DeviceIdType.MESH)

    moves = (
        (1, 1, ((17, 1, 6),), 1),
        (1, -1, ((18, 1, 17),), 2),
        (0, 1, ((11, 1, 18),), 3),
        (1, 0, ((0, 6, 0), (12, 5, 7), (19, 5, 12)), 0),
    )

    def rim_copies(sx, sy, blocks, n, low=0, high=4):
        parts = [(lm, rlm.at[n], n * 4 + 3)]
        for i, (src, count, dst) in enumerate(blocks):
            parts.append((fac.at[pl.ds(src, count)], rem.at[pl.ds(dst, count)], n * 4 + i))
        return [remote(src, dst, fsend.at[i], frecv.at[i], sx, sy) for src, dst, i in parts[low:high]]

    def depart(n, low, high):
        sx, sy, _, _ = moves[n]
        @pl.when(exists(sx, sy))
        def _():
            for copy in rim_copies(*moves[n], low, high):
                copy.start()

    copies[2].wait()

    def square(block):
        return lax.dot_general(block, block, (((1,), (1,)), ((), ())), preferred_element_type=f32)

    def place(j, slot, s):
        a, b = split2(s)
        wts[j, slot * B : (slot + 1) * B, 0:B] = a
        wts[j, slot * B : (slot + 1) * B, B : 2 * B] = b
        return a.astype(f32) + b.astype(f32)

    row_id = lax.broadcasted_iota(jnp.int32, (B, B), 0)
    lane_id = lax.broadcasted_iota(jnp.int32, (B, B), 1)
    eye = row_id == lane_id

    for m in range(N):
        mats[m * ST : m * ST + B, :] = jnp.where(eye, shift[m], 0.0)
    for m in range(N, 8):
        mats[m * ST : m * ST + B, :] = jnp.where(eye, 1.0, 0.0)

    def ahead(n):
        return remote(tsend.at[n], trecv.at[n], tsems.at[0, n], tsems.at[1, n], 1, 0)

    quarter = B // 4
    lane_q = lax.broadcasted_iota(jnp.int32, (quarter, B), 1)
    lane_h = lax.broadcasted_iota(jnp.int32, (quarter // 2, B), 1)
    above = row_id // quarter <= lane_id // quarter

    def own(j, d):
        s = place(j, d, square(fac[d * N + j]) * lm[d * N + j : d * N + j + 1, :])
        mats[j * ST : j * ST + B, :] = mats[j * ST : j * ST + B, :] + s
        return s

    def send_ahead(n, t):
        q = [t[k * quarter : (k + 1) * quarter] for k in range(4)]
        tsend[n, 0:quarter, :] = q[0]
        tsend[n, quarter : 2 * quarter, :] = jnp.where(lane_q < quarter, pltpu.roll(q[3], quarter, 1), q[1])
        tsend[n, 2 * quarter :, :] = jnp.where(
            lane_h < 2 * quarter, pltpu.roll(q[2][: quarter // 2], 2 * quarter, 1), q[2][quarter // 2 :])

    def unpack(n):
        p0, p1, p2 = trecv[n, 0:quarter, :], trecv[n, quarter : 2 * quarter, :], trecv[n, 2 * quarter :, :]
        upper = jnp.concatenate(
            [p0, p1, pltpu.roll(p2, 2 * quarter, 1), p2, pltpu.roll(p1, 3 * quarter, 1)], axis=0)
        return jnp.where(above, upper, upper.T)

    def arrived(n, low, high):
        sx, sy, _, _ = moves[n]
        @pl.when(exists(-sx, -sy))
        def _():
            for copy in rim_copies(*moves[n], low, high):
                copy.wait_recv()

    def term(j, slot, block, scale):
        return j, place(j, slot, square(rem[block]) * scale)

    def collect(terms):
        for j, s in terms:
            mats[j * ST : j * ST + B, :] = mats[j * ST : j * ST + B, :] + s

    def first(n):
        t = own(n, 0)
        if n > 0:
            t = t + own(n - 1, 2)
        if n < N - 1:
            t = t + own(n + 1, 3)
        send_ahead(n, t)

    early = 2
    for n in range(early):
        first(n)
    pl.semaphore_wait(barrier, len(greeted))
    for n in range(early):
        pl.when(exists(1, 0))(ahead(n).start)
    depart(2, 0, 2)
    tell(0)
    for n in range(early, N):
        first(n)
        pl.when(exists(1, 0))(ahead(n).start)
        if n == early:
            hear(0)
            depart(0, 0, 2)
            depart(1, 0, 2)
            tell(1)
    depart(3, 0, 4)
    hear(1)
    tell(2)
    own(N - 1, 2)
    own(0, 3)
    for j in range(N):
        t = own(j, 1)
        if j < N - 1:
            place(j + 1, 5, t)
            mats[(j + 1) * ST : (j + 1) * ST + B, :] = mats[(j + 1) * ST : (j + 1) * ST + B, :] + t

    def clear(ref, *spans):
        for span in spans:
            ref[span] = jnp.zeros_like(ref[span])

    @pl.when(gx == 0)
    def _():
        clear(ext, (slice(None), 0))
        clear(rem, slice(0, 3 * N))
        clear(rlm, slice(0, 3))
        clear(trecv, slice(None))

    @pl.when(gx == GXN - 1)
    def _():
        clear(ext, (slice(None), 2))

    @pl.when(gy == 0)
    def _():
        clear(ext, (slice(None), slice(None), 0))
        clear(rem, N, 3 * N)
        clear(rlm, 1, 3)

    @pl.when(gy == GYN - 1)
    def _():
        clear(ext, (slice(None), slice(None), N + 1))
        clear(rem, 3 * N - 1)
        clear(rlm, 2)

    arrived(2, 0, 2)
    arrived(0, 0, 2)
    arrived(1, 0, 2)
    collect([
        term(0, 6, N, rlm[1, 3 * N - 1 : 3 * N, :]),
        term(N - 1, 7, 3 * N - 1, rlm[2, 3 * N : 3 * N + 1, :]),
        term(0, 5, 3 * N, rlm[3, 2 * N - 1 : 2 * N, :]),
    ])

    for n in range(N):
        pl.when(exists(-1, 0))(ahead(n).wait_recv)
    for n in range(N):
        mats[n * ST : n * ST + B, :] = mats[n * ST : n * ST + B, :] + unpack(n)

    for m in range(N):
        a, b, c = split3(mats[m * ST : m * ST + B, :])
        dpan[m, 0:B, 0:B] = a
        dpan[m, 0:B, B : 2 * B] = b
        dpan[m, B : 2 * B, 0:B] = b
        dpan[m, B : 2 * B, B : 2 * B] = a
        dpan[m, 0:B, 2 * B :] = a
        dpan[m, B : 2 * B, 2 * B :] = c
    invert(mats, rpan, cpan)
    hear(2)

    def pairs(terms):
        return jnp.concatenate([jnp.concatenate([t, t], axis=1) for t in terms], axis=0)

    def fold(out, h):
        small = (out[2 * h :, 0:B] + out[2 * h :, B:]) + out[h : 2 * h, B:]
        return out[0:h, 0:B] + (out[h : 2 * h, 0:B] + (out[0:h, B:] + small))

    for m in range(N):
        a, b, c = split3(mats[m * ST : m * ST + B, :])
        pre[m, 0:B, 0:B] = a
        pre[m, 0:B, B : 2 * B] = b
        large = jnp.dot(jnp.concatenate([a, b], axis=1), dpan[m, :, 0 : 2 * B], preferred_element_type=f32)
        small = jnp.dot(jnp.concatenate([c, a], axis=1), dpan[m, :, 2 * B :], preferred_element_type=f32)
        product = (small + large[:, B:]) + large[:, 0:B]
        errs[m] = (jnp.where(eye, 1.0, 0.0) - product).astype(bf16)
    better = []
    for m in range(N):
        fix = jnp.dot(errs[m], pre[m, 0:B, :], preferred_element_type=f32)
        better.append(mats[m * ST : m * ST + B, :] + (fix[:, 0:B] + fix[:, B:]))
    for m in range(N):
        a, b, c = split3(better[m])
        pre[m, 0:B, 0:B] = a
        pre[m, 0:B, B : 2 * B] = b
        pre[m, B : 2 * B, 0:B] = c
        pre[m, B : 2 * B, B : 2 * B] = jnp.zeros((B, B), bf16)

    copies[3].wait()

    def precondition(v, m):
        return fold(jnp.dot(pairs(split3(v)), pre[m], preferred_element_type=f32), R)

    def operate(par, j):
        centre = ext[par, 1, 1 + j]
        terms = []
        for sign in (1, -1):
            for sx, sy in OFFSETS:
                terms.append(split3(centre - ext[par, 1 + sign * sx, 1 + j + sign * sy]))
        left = jnp.concatenate(
            [jnp.concatenate([t[i] for t in terms], axis=1) for i in range(3)], axis=0)
        out = fold(jnp.dot(left, wts[j], preferred_element_type=f32), R)
        return out + shift[j] * centre

    def halo(par, part=None):
        n = 0
        for sx, sy in SIDES:
            if sy == 0:
                pieces = [(pl.ds(1 + low, high - low), pl.ds(1 + low, high - low)) for low, high in ((0, CUT), (CUT, N))]
            else:
                pieces = [(N if sy == 1 else 1, 0 if sy == 1 else N + 1)]
            for k, (src, dst) in enumerate(pieces):
                if part is None or part == k:
                    yield sx, sy, remote(ext.at[par, 1, src], ext.at[par, 1 - sx, dst],
                                         hsend.at[n], hrecv.at[par, n], sx, sy)
                n += 1

    def halo_start(par):
        for part in range(2):
            for sx, sy, copy in halo(par, part):
                pl.when(exists(sx, sy))(copy.start)

    def halo_wait(par, part):
        for sx, sy, copy in halo(par, part):
            pl.when(exists(-sx, -sy))(copy.wait_recv)

    def halo_sent(par):
        for sx, sy, copy in halo(par):
            pl.when(exists(sx, sy))(copy.wait_send)

    def apply(par, out):
        halo_wait(par, 0)
        for j in range(CUT - 1):
            out[j] = operate(par, j)
        halo_wait(par, 1)
        for j in range(CUT - 1, N):
            out[j] = operate(par, j)

    lane = lax.broadcasted_iota(jnp.int32, (R, B), 1)
    rhs = lax.broadcasted_iota(jnp.int32, (R, B), 0)

    def contribution(par, peer):
        return pltpu.make_async_remote_copy(
            src_ref=dsend.at[pl.ds(par, 1)], dst_ref=drecv.at[par, pl.ds(me, 1)],
            send_sem=ssend, recv_sem=srecv.at[par],
            device_id=peer, device_id_type=pl.DeviceIdType.MESH)

    def scatter(par, sums):
        spread = 0.0
        for k, t in reversed(list(enumerate(sums))):
            spread = jnp.where(lane == rhs + k * R, jnp.sum(t, axis=1, keepdims=True), spread)
        row = jnp.sum(spread, axis=0, keepdims=True)
        dsend[pl.ds(par, 1), :] = row
        drecv[par, pl.ds(me, 1), :] = row
        for peer in peers:
            contribution(par, peer).start()

    def gather(par, count):
        everything = drecv.at[par, pl.ds(0, PLANE - 1)]
        pltpu.make_async_copy(everything, everything, srecv.at[par]).wait()
        pltpu.make_async_copy(everything, everything, ssend).wait()
        total = jnp.sum(drecv[par], axis=0, keepdims=True)
        return [jnp.sum(jnp.where(lane == rhs + k * R, total, 0.0), axis=1, keepdims=True) for k in range(count)]

    def products(par, triples):
        gsum, dsum = None, None
        for r, u, w in triples:
            g, d = u * r, u * w
            gsum = g if gsum is None else gsum + g
            dsum = d if dsum is None else dsum + d
        scatter(par, [gsum, dsum])

    def totals(par, gamma_old, alpha_old):
        gamma, delta = gather(par, 2)
        ratio = gamma / gamma_old
        alpha = gamma / (delta - ratio * gamma / alpha_old)
        return gamma, ratio, alpha

    for j in range(N):
        ext[1, 1, 1 + j] = precondition(res[0, j], j)
    halo_start(1)
    arrived(3, 0, 2)
    for j in range(N):
        term(j, 4, j, rlm[0, j : j + 1, :])
    arrived(3, 2, 3)
    for j in range(1, N):
        term(j, 6, N + j, rlm[0, 2 * N + j - 1 : 2 * N + j, :])
    arrived(3, 3, 4)
    for j in range(N - 1):
        term(j, 7, 2 * N + j, rlm[0, 3 * N + j + 1 : 3 * N + j + 2, :])
    apply(1, img)
    for j in range(N):
        pre_u[j] = ext[1, 1, 1 + j]
    halo_sent(1)

    for j in range(N):
        ext[0, 1, 1 + j] = precondition(img[j], j)
    halo_start(0)
    apply(0, push)
    groups = []
    for j in range(N):
        u, w, m, n = pre_u[j], img[j], ext[0, 1, 1 + j], push[j]
        groups.append((u * res[0, j], u * w, w * m, n * m))
    scatter(1, [sum(g[1:], g[0]) for g in zip(*groups)])
    for j in range(N):
        ext[1, 1, 1 + j] = precondition(push[j], j)
    halo_sent(0)
    halo_start(1)
    apply(1, zdir)
    gamma, delta, wm, nm = gather(1, 4)
    alpha = gamma / delta
    gamma_next = gamma - alpha * (2.0 * delta - alpha * wm)
    delta_next = delta - alpha * (2.0 * wm - alpha * nm)
    ratio = gamma_next / gamma
    alpha_next = gamma_next / (delta_next - ratio * gamma_next / alpha)
    triples = []
    for j in range(N):
        u, w, m, n, o, t = pre_u[j], img[j], ext[0, 1, 1 + j], push[j], ext[1, 1, 1 + j], zdir[j]
        u1, w1, m1, n1 = u - alpha * m, w - alpha * n, m - alpha * o, n - alpha * t
        p, s, q, z = u1 + ratio * u, w1 + ratio * w, m1 + ratio * m, n1 + ratio * n
        zdir[j], qdir[j], along[j], dirn[j] = z, q, s, p
        x_out[0, j] = alpha * u + alpha_next * p
        r = res[0, j] - alpha * w - alpha_next * s
        u2, w2 = u1 - alpha_next * q, w1 - alpha_next * z
        res[0, j], pre_u[j], img[j] = r, u2, w2
        triples.append((r, u2, w2))
    products(0, triples)
    halo_sent(1)
    for sx, sy, blocks, n in moves:
        @pl.when(exists(sx, sy))
        def _():
            for copy in rim_copies(sx, sy, blocks, n):
                copy.wait_send()
    for n in range(N):
        pl.when(exists(1, 0))(ahead(n).wait_send)

    def iterate(it, carry):
        gamma_old, alpha_old = carry
        par = lax.rem(it, 2)
        for j in range(N):
            ext[par, 1, 1 + j] = precondition(img[j], j)
        halo_start(par)
        apply(par, push)
        gamma, ratio, alpha = totals(par, gamma_old, alpha_old)
        triples = []
        for j in range(N):
            u, w = pre_u[j], img[j]
            z = push[j] + ratio * zdir[j]
            q = ext[par, 1, 1 + j] + ratio * qdir[j]
            s = w + ratio * along[j]
            p = u + ratio * dirn[j]
            zdir[j], qdir[j], along[j], dirn[j] = z, q, s, p
            x_out[0, j] = x_out[0, j] + alpha * p
            r = res[0, j] - alpha * s
            u = u - alpha * q
            w = w - alpha * z
            res[0, j], pre_u[j], img[j] = r, u, w
            triples.append((r, u, w))
        products(1 - par, triples)
        halo_sent(par)
        return gamma, alpha

    gamma_old, alpha_old = lax.fori_loop(2, ITERS - 1, iterate, (gamma_next, alpha_next))
    gamma, ratio, alpha = totals((ITERS - 1) % 2, gamma_old, alpha_old)
    for j in range(N):
        x_out[0, j] = x_out[0, j] + alpha * (pre_u[j] + ratio * dirn[j])
        r_out[0, j] = res[0, j] - alpha * (img[j] + ratio * along[j])


def local(load, factors, links, shift):
    vmem = pl.BlockSpec(memory_space=pltpu.VMEM)
    hbm = pl.BlockSpec(memory_space=pltpu.HBM)
    field = jax.ShapeDtypeStruct((1, N, R, B), f32)
    return pl.pallas_call(
        kernel,
        out_shape=(field, field),
        in_specs=[hbm] * 4,
        out_specs=(vmem, vmem),
        scratch_shapes=[
            pltpu.SMEM((4, 1, N), jnp.int32),
            pltpu.VMEM((N, 1, B), f32),
            pltpu.VMEM((4 * N, B, B), bf16),
            pltpu.VMEM((3 * N + 1, B, B), bf16),
            pltpu.VMEM((4 * N, B), f32),
            pltpu.VMEM((4, 4 * N, B), f32),
            pltpu.VMEM((8 * ST, B), f32),
            pltpu.VMEM((8 * NB, B), f32),
            pltpu.VMEM((8 * NB, B), f32),
            pltpu.VMEM((N, 2 * B, 3 * B), bf16),
            pltpu.VMEM((N, B, B), bf16),
            pltpu.VMEM((N, 8 * B, 2 * B), bf16),
            pltpu.VMEM((N, 2 * B, 2 * B), bf16),
            pltpu.VMEM((2, 3, N + 2, R, B), f32),
            pltpu.VMEM((N, R, B), f32),
            pltpu.VMEM((N, R, B), f32),
            pltpu.VMEM((N, R, B), f32),
            pltpu.VMEM((N, R, B), f32),
            pltpu.VMEM((1, N, R, B), f32),
            pltpu.VMEM((N, R, B), f32),
            pltpu.VMEM((N, R, B), f32),
            pltpu.VMEM((N, R, B), f32),
            pltpu.VMEM((8, B), f32),
            pltpu.VMEM((2, PLANE, B), f32),
            pltpu.SemaphoreType.DMA((4,)),
            pltpu.SemaphoreType.DMA((16,)),
            pltpu.SemaphoreType.DMA((16,)),
            pltpu.SemaphoreType.DMA((10,)),
            pltpu.SemaphoreType.DMA((2, 10)),
            pltpu.SemaphoreType.DMA,
            pltpu.SemaphoreType.DMA((2,)),
            pltpu.SemaphoreType.REGULAR((3,)),
            pltpu.VMEM((N, 5 * B // 8, B), f32),
            pltpu.VMEM((N, 5 * B // 8, B), f32),
            pltpu.SemaphoreType.DMA((2, N)),
        ],
        compiler_params=pltpu.CompilerParams(collective_id=0, has_side_effects=True, vmem_limit_bytes=24 * 1024 * 1024),
        name="solve",
    )(*[pltpu.with_memory_space_constraint(t, pltpu.HBM) for t in (links, load, factors.reshape(4 * N, B, B), shift.reshape(N, 1, B))])


def solution(mesh):
    placed = (
        P(("case", "gx"), "gy", None, None),
        P(None, ("case", "gx"), "gy", None, None),
        P(None, ("case", "gx"), "gy"),
        P(("case", "gx"), "gy", None),
    )
    return jax.shard_map(
        local,
        mesh=mesh,
        in_specs=placed,
        out_specs=(P(("case", "gx"), "gy", None, None), P(("case", "gx"), "gy", None, None)),
        check_vma=False,
    )
```

```python
import functools

import jax
import jax.numpy as jnp
from jax import lax
from jax.experimental import pallas as pl
from jax.experimental.pallas import tpu as pltpu
from jax.sharding import PartitionSpec as P

B = 128
N = 6
R = 32
ITERS = 8
NB = 8
ST = 136
GXN = 8
GYN = 4
PLANE = GXN * GYN
CUT = 3
OFFSETS = ((1, 0), (0, 1), (1, 1), (1, -1))
SIDES = ((1, 1), (1, -1), (-1, 1), (-1, -1), (1, 0), (-1, 0), (0, 1), (0, -1))
f32 = jnp.float32
bf16 = jnp.bfloat16


def split3(x):
    a = x.astype(bf16)
    left = x - a.astype(f32)
    b = left.astype(bf16)
    c = (left - b.astype(f32)).astype(bf16)
    return a, b, c


def split2(x):
    a = x.astype(bf16)
    return a, (x - a.astype(f32)).astype(bf16)


def invert(mats, rpan, cpan):
    lane = lax.broadcasted_iota(jnp.int32, (8, B), 1)

    def packed(base):
        return [mats[pl.ds(base + i, 8, stride=ST), :] for i in range(NB)]

    def pick(row, k):
        return jnp.sum(jnp.where(lane == k, row, 0.0), axis=1, keepdims=True)

    def pivot(rows, base):
        e = {}
        for j in range(NB):
            for i in range(j + 1):
                e[i, j] = pick(rows[i], base + j)
        ahead = [[pick(rows[k], base + NB + i) for k in range(NB)] for i in range(NB)]
        inside = (lane >= base) & (lane < base + NB)
        sign = jnp.where(lane < base, -1.0, jnp.where(inside, 0.0, 1.0))
        at = lambda i, j: e[min(i, j), max(i, j)]
        for k in range(NB):
            p = 1.0 / e[k, k]
            col = [at(i, k) for i in range(NB)]
            scaled = [c * p for c in col]
            for i in range(NB):
                for j in range(i, NB):
                    if i != k and j != k:
                        e[i, j] = e[i, j] - scaled[i] * col[j]
            for i in range(NB):
                if i != k:
                    e[min(i, k), max(i, k)] = scaled[i]
            e[k, k] = -p
        panel = [jnp.where(lane == base + i, 1.0, jnp.where(inside, 0.0, rows[i])) for i in range(NB)]
        right = []
        for j in range(NB):
            total = None
            for i in range(NB):
                term = at(i, j) * panel[i]
                total = term if total is None else total + term
            right.append(-total)
        following = packed(jnp.minimum(base + NB, B - NB))
        after = []
        for i in range(NB):
            row = jnp.where(inside, 0.0, following[i])
            for k in range(NB):
                row = row - ahead[i][k] * right[k]
            after.append(row)
        for k in range(NB):
            cpan[pl.ds(k, 8, stride=NB), :] = rows[k] * sign
            rpan[pl.ds(k, 8, stride=NB), :] = right[k]
        return tuple(after)

    def trail(base):
        inside = (lane >= base) & (lane < base + NB)
        rows = [rpan[m * NB : (m + 1) * NB, :] for m in range(N)]
        ups = []
        for m in range(N):
            c0, c1, c2 = split3(cpan[m * NB : (m + 1) * NB, :])
            r0, r1, r2 = split3(rows[m])
            ups.append(lax.dot_general(
                jnp.concatenate([c0, c0, c1, c1, c0, c2], axis=0),
                jnp.concatenate([r0, r1, r0, r1, r2, r0], axis=0),
                (((0,), (0,)), ((), ())), preferred_element_type=f32))
        new = [jnp.where(inside[0:1, :], 0.0, mats[m * ST : m * ST + B, :]) - ups[m] for m in range(N)]
        for m in range(N):
            mats[m * ST : m * ST + B, :] = new[m]
        for m in range(N):
            mats[pl.ds(pl.multiple_of(m * ST + base, 8), 8), :] = rows[m]

    def step(b, rows):
        trail((b - 1) * NB)
        return pivot(rows, b * NB)

    rows = pivot(packed(0), 0)
    lax.fori_loop(1, B // NB, step, rows)
    trail(B - NB)


def kernel(links_in, load, factors, shift_in, x_out, r_out, links, shift, fac, rem, lm, rlm, mats, rpan, cpan, dpan, errs, wts, pre, ext,
           pre_u, push, qdir, zdir, res, dirn, along, img, dsend, drecv, lsem, fsend, frecv, hsend, hrecv, ssend, srecv, known,
           tsend, trecv, tsems):
    case = lax.axis_index("case")
    gx = lax.axis_index("gx")
    gy = lax.axis_index("gy")
    me = gx * GYN + gy

    def device(x, y):
        return (case, x, y)

    def exists(sx, sy):
        ok = None
        for pos, step, count in ((gx, sx, GXN), (gy, sy, GYN)):
            if step == 0:
                continue
            here = (pos + step >= 0) & (pos + step < count)
            ok = here if ok is None else ok & here
        return ok

    barrier = pltpu.get_barrier_semaphore()
    peers = []
    hops = lambda a, c: -(min((a + 1) // 2, (GXN - a + 1) // 2) + min(c, GYN - c))
    for a, c in sorted([(a, c) for a in range(GXN) for c in range(GYN)], key=lambda t: hops(*t)):
        if a or c:
            peers.append(device(lax.rem(gx + a, GXN), lax.rem(gy + c, GYN)))

    def ring(dx, dy):
        return device(lax.rem(gx + dx + GXN, GXN), lax.rem(gy + dy + GYN, GYN))

    greeted = [ring(1, 0), ring(-1, 0), ring(0, 1), ring(0, -1)]
    rounds = [greeted, [ring(2, 0), ring(-2, 0), ring(0, 2)], [ring(d, 0) for d in range(1, GXN)]]
    for peer in greeted:
        pl.semaphore_signal(barrier, inc=1, device_id=peer, device_id_type=pl.DeviceIdType.MESH)

    def tell(i):
        for peer in rounds[i]:
            pl.semaphore_signal(known.at[i], inc=1, device_id=peer, device_id_type=pl.DeviceIdType.MESH)

    def hear(i):
        pl.semaphore_wait(known.at[i], len(rounds[i]))

    copies = [
        pltpu.make_async_copy(factors, fac, lsem.at[0]),
        pltpu.make_async_copy(links_in, links, lsem.at[1]),
        pltpu.make_async_copy(shift_in, shift, lsem.at[2]),
        pltpu.make_async_copy(load, res, lsem.at[3]),
    ]
    for copy in copies:
        copy.start()
    copies[1].wait()
    for d in range(4):
        for j in range(N):
            lm[d * N + j : d * N + j + 1, :] = jnp.full((1, B), links[d, 0, j], jnp.int32).astype(f32) * (1.0 / B)
    copies[0].wait()

    def remote(src, dst, ss, rs, sx, sy):
        return pltpu.make_async_remote_copy(
            src_ref=src, dst_ref=dst, send_sem=ss, recv_sem=rs,
            device_id=device(gx + sx, gy + sy), device_id_type=pl.DeviceIdType.MESH)

    moves = (
        (1, 1, ((17, 1, 6),), 1),
        (1, -1, ((18, 1, 17),), 2),
        (0, 1, ((11, 1, 18),), 3),
        (1, 0, ((0, 6, 0), (12, 5, 7), (19, 5, 12)), 0),
    )

    def rim_copies(sx, sy, blocks, n, low=0, high=4):
        parts = [(lm, rlm.at[n], n * 4 + 3)]
        for i, (src, count, dst) in enumerate(blocks):
            parts.append((fac.at[pl.ds(src, count)], rem.at[pl.ds(dst, count)], n * 4 + i))
        return [remote(src, dst, fsend.at[i], frecv.at[i], sx, sy) for src, dst, i in parts[low:high]]

    def depart(n, low, high):
        sx, sy, _, _ = moves[n]
        @pl.when(exists(sx, sy))
        def _():
            for copy in rim_copies(*moves[n], low, high):
                copy.start()

    copies[2].wait()

    def square(block):
        return lax.dot_general(block, block, (((1,), (1,)), ((), ())), preferred_element_type=f32)

    def place(j, slot, s):
        a, b = split2(s)
        wts[j, slot * B : (slot + 1) * B, 0:B] = a
        wts[j, slot * B : (slot + 1) * B, B : 2 * B] = b
        return a.astype(f32) + b.astype(f32)

    row_id = lax.broadcasted_iota(jnp.int32, (B, B), 0)
    lane_id = lax.broadcasted_iota(jnp.int32, (B, B), 1)
    eye = row_id == lane_id

    for m in range(N):
        mats[m * ST : m * ST + B, :] = jnp.where(eye, shift[m], 0.0)
    for m in range(N, 8):
        mats[m * ST : m * ST + B, :] = jnp.where(eye, 1.0, 0.0)

    def ahead(n):
        return remote(tsend.at[n], trecv.at[n], tsems.at[0, n], tsems.at[1, n], 1, 0)

    quarter = B // 4
    lane_q = lax.broadcasted_iota(jnp.int32, (quarter, B), 1)
    lane_h = lax.broadcasted_iota(jnp.int32, (quarter // 2, B), 1)
    above = row_id // quarter <= lane_id // quarter

    def own(j, d):
        s = place(j, d, square(fac[d * N + j]) * lm[d * N + j : d * N + j + 1, :])
        mats[j * ST : j * ST + B, :] = mats[j * ST : j * ST + B, :] + s
        return s

    def send_ahead(n, t):
        q = [t[k * quarter : (k + 1) * quarter] for k in range(4)]
        tsend[n, 0:quarter, :] = q[0]
        tsend[n, quarter : 2 * quarter, :] = jnp.where(lane_q < quarter, pltpu.roll(q[3], quarter, 1), q[1])
        tsend[n, 2 * quarter :, :] = jnp.where(
            lane_h < 2 * quarter, pltpu.roll(q[2][: quarter // 2], 2 * quarter, 1), q[2][quarter // 2 :])

    def unpack(n):
        p0, p1, p2 = trecv[n, 0:quarter, :], trecv[n, quarter : 2 * quarter, :], trecv[n, 2 * quarter :, :]
        upper = jnp.concatenate(
            [p0, p1, pltpu.roll(p2, 2 * quarter, 1), p2, pltpu.roll(p1, 3 * quarter, 1)], axis=0)
        return jnp.where(above, upper, upper.T)

    def arrived(n, low, high):
        sx, sy, _, _ = moves[n]
        @pl.when(exists(-sx, -sy))
        def _():
            for copy in rim_copies(*moves[n], low, high):
                copy.wait_recv()

    def term(j, slot, block, scale):
        return j, place(j, slot, square(rem[block]) * scale)

    def collect(terms):
        for j, s in terms:
            mats[j * ST : j * ST + B, :] = mats[j * ST : j * ST + B, :] + s

    def first(n):
        t = own(n, 0)
        if n > 0:
            t = t + own(n - 1, 2)
        if n < N - 1:
            t = t + own(n + 1, 3)
        send_ahead(n, t)

    early = 2
    for n in range(early):
        first(n)
    pl.semaphore_wait(barrier, len(greeted))
    for n in range(early):
        pl.when(exists(1, 0))(ahead(n).start)
    depart(2, 0, 2)
    tell(0)
    for n in range(early, N):
        first(n)
        pl.when(exists(1, 0))(ahead(n).start)
        if n == early:
            hear(0)
            depart(0, 0, 2)
            depart(1, 0, 2)
            tell(1)
    depart(3, 0, 4)
    hear(1)
    tell(2)
    own(N - 1, 2)
    own(0, 3)
    for j in range(N):
        t = own(j, 1)
        if j < N - 1:
            place(j + 1, 5, t)
            mats[(j + 1) * ST : (j + 1) * ST + B, :] = mats[(j + 1) * ST : (j + 1) * ST + B, :] + t

    def clear(ref, *spans):
        for span in spans:
            ref[span] = jnp.zeros_like(ref[span])

    @pl.when(gx == 0)
    def _():
        clear(ext, (slice(None), 0))
        clear(rem, slice(0, 3 * N))
        clear(rlm, slice(0, 3))
        clear(trecv, slice(None))

    @pl.when(gx == GXN - 1)
    def _():
        clear(ext, (slice(None), 2))

    @pl.when(gy == 0)
    def _():
        clear(ext, (slice(None), slice(None), 0))
        clear(rem, N, 3 * N)
        clear(rlm, 1, 3)

    @pl.when(gy == GYN - 1)
    def _():
        clear(ext, (slice(None), slice(None), N + 1))
        clear(rem, 3 * N - 1)
        clear(rlm, 2)

    arrived(2, 0, 2)
    arrived(0, 0, 2)
    arrived(1, 0, 2)
    collect([
        term(0, 6, N, rlm[1, 3 * N - 1 : 3 * N, :]),
        term(N - 1, 7, 3 * N - 1, rlm[2, 3 * N : 3 * N + 1, :]),
        term(0, 5, 3 * N, rlm[3, 2 * N - 1 : 2 * N, :]),
    ])

    for n in range(N):
        pl.when(exists(-1, 0))(ahead(n).wait_recv)
    for n in range(N):
        mats[n * ST : n * ST + B, :] = mats[n * ST : n * ST + B, :] + unpack(n)

    for m in range(N):
        a, b, c = split3(mats[m * ST : m * ST + B, :])
        dpan[m, 0:B, 0:B] = a
        dpan[m, 0:B, B : 2 * B] = b
        dpan[m, B : 2 * B, 0:B] = b
        dpan[m, B : 2 * B, B : 2 * B] = a
        dpan[m, 0:B, 2 * B :] = a
        dpan[m, B : 2 * B, 2 * B :] = c
    invert(mats, rpan, cpan)
    hear(2)

    def pairs(terms):
        return jnp.concatenate([jnp.concatenate([t, t], axis=1) for t in terms], axis=0)

    def fold(out, h):
        small = (out[2 * h :, 0:B] + out[2 * h :, B:]) + out[h : 2 * h, B:]
        return out[0:h, 0:B] + (out[h : 2 * h, 0:B] + (out[0:h, B:] + small))

    for m in range(N):
        a, b, c = split3(mats[m * ST : m * ST + B, :])
        pre[m, 0:B, 0:B] = a
        pre[m, 0:B, B : 2 * B] = b
        large = jnp.dot(jnp.concatenate([a, b], axis=1), dpan[m, :, 0 : 2 * B], preferred_element_type=f32)
        small = jnp.dot(jnp.concatenate([c, a], axis=1), dpan[m, :, 2 * B :], preferred_element_type=f32)
        product = (small + large[:, B:]) + large[:, 0:B]
        errs[m] = (jnp.where(eye, 1.0, 0.0) - product).astype(bf16)
    better = []
    for m in range(N):
        fix = jnp.dot(errs[m], pre[m, 0:B, :], preferred_element_type=f32)
        better.append(mats[m * ST : m * ST + B, :] + (fix[:, 0:B] + fix[:, B:]))
    for m in range(N):
        a, b, c = split3(better[m])
        pre[m, 0:B, 0:B] = a
        pre[m, 0:B, B : 2 * B] = b
        pre[m, B : 2 * B, 0:B] = c
        pre[m, B : 2 * B, B : 2 * B] = jnp.zeros((B, B), bf16)

    for ref in (x_out, dirn, along, qdir, zdir):
        ref[...] = jnp.zeros_like(ref)
    copies[3].wait()

    def precondition(v, m):
        return fold(jnp.dot(pairs(split3(v)), pre[m], preferred_element_type=f32), R)

    def operate(par, j):
        centre = ext[par, 1, 1 + j]
        terms = []
        for sign in (1, -1):
            for sx, sy in OFFSETS:
                terms.append(split3(centre - ext[par, 1 + sign * sx, 1 + j + sign * sy]))
        left = jnp.concatenate(
            [jnp.concatenate([t[i] for t in terms], axis=1) for i in range(3)], axis=0)
        out = fold(jnp.dot(left, wts[j], preferred_element_type=f32), R)
        return out + shift[j] * centre

    def halo(par, part=None):
        n = 0
        for sx, sy in SIDES:
            if sy == 0:
                pieces = [(pl.ds(1 + low, high - low), pl.ds(1 + low, high - low)) for low, high in ((0, CUT), (CUT, N))]
            else:
                pieces = [(N if sy == 1 else 1, 0 if sy == 1 else N + 1)]
            for k, (src, dst) in enumerate(pieces):
                if part is None or part == k:
                    yield sx, sy, remote(ext.at[par, 1, src], ext.at[par, 1 - sx, dst],
                                         hsend.at[n], hrecv.at[par, n], sx, sy)
                n += 1

    def halo_start(par):
        for part in range(2):
            for sx, sy, copy in halo(par, part):
                pl.when(exists(sx, sy))(copy.start)

    def halo_wait(par, part):
        for sx, sy, copy in halo(par, part):
            pl.when(exists(-sx, -sy))(copy.wait_recv)

    def halo_sent(par):
        for sx, sy, copy in halo(par):
            pl.when(exists(sx, sy))(copy.wait_send)

    def apply(par, out):
        halo_wait(par, 0)
        for j in range(CUT - 1):
            out[j] = operate(par, j)
        halo_wait(par, 1)
        for j in range(CUT - 1, N):
            out[j] = operate(par, j)

    lane = lax.broadcasted_iota(jnp.int32, (R, B), 1)
    rhs = lax.broadcasted_iota(jnp.int32, (R, B), 0)

    def contribution(par, peer):
        return pltpu.make_async_remote_copy(
            src_ref=dsend.at[pl.ds(par, 1)], dst_ref=drecv.at[par, pl.ds(me, 1)],
            send_sem=ssend, recv_sem=srecv.at[par],
            device_id=peer, device_id_type=pl.DeviceIdType.MESH)

    def scatter(par, sums):
        spread = 0.0
        for k, t in reversed(list(enumerate(sums))):
            spread = jnp.where(lane == rhs + k * R, jnp.sum(t, axis=1, keepdims=True), spread)
        row = jnp.sum(spread, axis=0, keepdims=True)
        dsend[pl.ds(par, 1), :] = row
        drecv[par, pl.ds(me, 1), :] = row
        for peer in peers:
            contribution(par, peer).start()

    def gather(par, count):
        everything = drecv.at[par, pl.ds(0, PLANE - 1)]
        pltpu.make_async_copy(everything, everything, srecv.at[par]).wait()
        pltpu.make_async_copy(everything, everything, ssend).wait()
        total = jnp.sum(drecv[par], axis=0, keepdims=True)
        return [jnp.sum(jnp.where(lane == rhs + k * R, total, 0.0), axis=1, keepdims=True) for k in range(count)]

    def products(par, triples):
        gsum, dsum = None, None
        for r, u, w in triples:
            g, d = u * r, u * w
            gsum = g if gsum is None else gsum + g
            dsum = d if dsum is None else dsum + d
        scatter(par, [gsum, dsum])

    def totals(par, first, gamma_old, alpha_old):
        gamma, delta = gather(par, 2)
        ratio = jnp.where(first, 0.0, gamma / gamma_old)
        alpha = gamma / (delta - ratio * gamma / alpha_old)
        return gamma, ratio, alpha

    for j in range(N):
        ext[1, 1, 1 + j] = precondition(res[0, j], j)
    halo_start(1)
    arrived(3, 0, 2)
    for j in range(N):
        term(j, 4, j, rlm[0, j : j + 1, :])
    arrived(3, 2, 3)
    for j in range(1, N):
        term(j, 6, N + j, rlm[0, 2 * N + j - 1 : 2 * N + j, :])
    arrived(3, 3, 4)
    for j in range(N - 1):
        term(j, 7, 2 * N + j, rlm[0, 3 * N + j + 1 : 3 * N + j + 2, :])
    apply(1, img)
    for j in range(N):
        pre_u[j] = ext[1, 1, 1 + j]
    halo_sent(1)

    products(0, [(res[0, j], pre_u[j], img[j]) for j in range(N)])
    for sx, sy, blocks, n in moves:
        @pl.when(exists(sx, sy))
        def _():
            for copy in rim_copies(sx, sy, blocks, n):
                copy.wait_send()
    for n in range(N):
        pl.when(exists(1, 0))(ahead(n).wait_send)

    def iterate(it, carry):
        gamma_old, alpha_old = carry
        par = lax.rem(it, 2)
        for j in range(N):
            ext[par, 1, 1 + j] = precondition(img[j], j)
        halo_start(par)
        apply(par, push)
        gamma, ratio, alpha = totals(par, it == 0, gamma_old, alpha_old)
        triples = []
        for j in range(N):
            u, w = pre_u[j], img[j]
            z = push[j] + ratio * zdir[j]
            q = ext[par, 1, 1 + j] + ratio * qdir[j]
            s = w + ratio * along[j]
            p = u + ratio * dirn[j]
            zdir[j], qdir[j], along[j], dirn[j] = z, q, s, p
            x_out[0, j] = x_out[0, j] + alpha * p
            r = res[0, j] - alpha * s
            u = u - alpha * q
            w = w - alpha * z
            res[0, j], pre_u[j], img[j] = r, u, w
            triples.append((r, u, w))
        products(1 - par, triples)
        halo_sent(par)
        return gamma, alpha

    one = jnp.ones((R, 1), f32)
    gamma_old, alpha_old = lax.fori_loop(0, ITERS - 1, iterate, (one, one))
    gamma, ratio, alpha = totals((ITERS - 1) % 2, ITERS == 1, gamma_old, alpha_old)
    for j in range(N):
        x_out[0, j] = x_out[0, j] + alpha * (pre_u[j] + ratio * dirn[j])
        r_out[0, j] = res[0, j] - alpha * (img[j] + ratio * along[j])


def local(load, factors, links, shift):
    vmem = pl.BlockSpec(memory_space=pltpu.VMEM)
    hbm = pl.BlockSpec(memory_space=pltpu.HBM)
    field = jax.ShapeDtypeStruct((1, N, R, B), f32)
    return pl.pallas_call(
        kernel,
        out_shape=(field, field),
        in_specs=[hbm] * 4,
        out_specs=(vmem, vmem),
        scratch_shapes=[
            pltpu.SMEM((4, 1, N), jnp.int32),
            pltpu.VMEM((N, 1, B), f32),
            pltpu.VMEM((4 * N, B, B), bf16),
            pltpu.VMEM((3 * N + 1, B, B), bf16),
            pltpu.VMEM((4 * N, B), f32),
            pltpu.VMEM((4, 4 * N, B), f32),
            pltpu.VMEM((8 * ST, B), f32),
            pltpu.VMEM((8 * NB, B), f32),
            pltpu.VMEM((8 * NB, B), f32),
            pltpu.VMEM((N, 2 * B, 3 * B), bf16),
            pltpu.VMEM((N, B, B), bf16),
            pltpu.VMEM((N, 8 * B, 2 * B), bf16),
            pltpu.VMEM((N, 2 * B, 2 * B), bf16),
            pltpu.VMEM((2, 3, N + 2, R, B), f32),
            pltpu.VMEM((N, R, B), f32),
            pltpu.VMEM((N, R, B), f32),
            pltpu.VMEM((N, R, B), f32),
            pltpu.VMEM((N, R, B), f32),
            pltpu.VMEM((1, N, R, B), f32),
            pltpu.VMEM((N, R, B), f32),
            pltpu.VMEM((N, R, B), f32),
            pltpu.VMEM((N, R, B), f32),
            pltpu.VMEM((8, B), f32),
            pltpu.VMEM((2, PLANE, B), f32),
            pltpu.SemaphoreType.DMA((4,)),
            pltpu.SemaphoreType.DMA((16,)),
            pltpu.SemaphoreType.DMA((16,)),
            pltpu.SemaphoreType.DMA((10,)),
            pltpu.SemaphoreType.DMA((2, 10)),
            pltpu.SemaphoreType.DMA,
            pltpu.SemaphoreType.DMA((2,)),
            pltpu.SemaphoreType.REGULAR((3,)),
            pltpu.VMEM((N, 5 * B // 8, B), f32),
            pltpu.VMEM((N, 5 * B // 8, B), f32),
            pltpu.SemaphoreType.DMA((2, N)),
        ],
        compiler_params=pltpu.CompilerParams(collective_id=0, has_side_effects=True, vmem_limit_bytes=24 * 1024 * 1024),
        name="solve",
    )(*[pltpu.with_memory_space_constraint(t, pltpu.HBM) for t in (links, load, factors.reshape(4 * N, B, B), shift.reshape(N, 1, B))])


def solution(mesh):
    placed = (
        P(("case", "gx"), "gy", None, None),
        P(None, ("case", "gx"), "gy", None, None),
        P(None, ("case", "gx"), "gy"),
        P(("case", "gx"), "gy", None),
    )
    return jax.shard_map(
        local,
        mesh=mesh,
        in_specs=placed,
        out_specs=(P(("case", "gx"), "gy", None, None), P(("case", "gx"), "gy", None, None)),
        check_vma=False,
    )
```

```python
import functools

import jax
import jax.numpy as jnp
from jax import lax
from jax.experimental import pallas as pl
from jax.experimental.pallas import tpu as pltpu
from jax.sharding import PartitionSpec as P

B = 128
N = 6
R = 32
ITERS = 8
NB = 8
ST = 136
GXN = 8
GYN = 4
PLANE = GXN * GYN
CUT = 3
OFFSETS = ((1, 0), (0, 1), (1, 1), (1, -1))
SIDES = ((1, 1), (1, -1), (-1, 1), (-1, -1), (1, 0), (-1, 0), (0, 1), (0, -1))
f32 = jnp.float32
bf16 = jnp.bfloat16


def split3(x):
    a = x.astype(bf16)
    left = x - a.astype(f32)
    b = left.astype(bf16)
    c = (left - b.astype(f32)).astype(bf16)
    return a, b, c


def split2(x):
    a = x.astype(bf16)
    return a, (x - a.astype(f32)).astype(bf16)


def invert(mats, rpan, cpan, turned):
    lane = lax.broadcasted_iota(jnp.int32, (8, B), 1)

    def packed(base):
        return [mats[pl.ds(base + i, 8, stride=ST), :] for i in range(NB)]

    def pick(row, k):
        return jnp.sum(jnp.where(lane == k, row, 0.0), axis=1, keepdims=True)

    def pivot(rows, base):
        e = {}
        for j in range(NB):
            for i in range(j + 1):
                e[i, j] = pick(rows[i], base + j)
        ahead = [[pick(rows[k], base + NB + i) for k in range(NB)] for i in range(NB)]
        inside = (lane >= base) & (lane < base + NB)
        sign = jnp.where(lane < base, -1.0, jnp.where(inside, 0.0, 1.0))
        for k in range(NB):
            cpan[pl.ds(k, 8, stride=NB), :] = rows[k] * sign
        for m in range(N):
            c0, c1, c2 = split3(cpan[m * NB : (m + 1) * NB, :])
            turned[m] = jnp.concatenate([c0, c0, c1, c1, c0, c2], axis=0).T
        at = lambda i, j: e[min(i, j), max(i, j)]
        for k in range(NB):
            p = 1.0 / e[k, k]
            col = [at(i, k) for i in range(NB)]
            scaled = [c * p for c in col]
            for i in range(NB):
                for j in range(i, NB):
                    if i != k and j != k:
                        e[i, j] = e[i, j] - scaled[i] * col[j]
            for i in range(NB):
                if i != k:
                    e[min(i, k), max(i, k)] = scaled[i]
            e[k, k] = -p
        panel = [jnp.where(lane == base + i, 1.0, jnp.where(inside, 0.0, rows[i])) for i in range(NB)]
        right = []
        for j in range(NB):
            total = None
            for i in range(NB):
                term = at(i, j) * panel[i]
                total = term if total is None else total + term
            right.append(-total)
        following = packed(jnp.minimum(base + NB, B - NB))
        after = []
        for i in range(NB):
            row = jnp.where(inside, 0.0, following[i])
            for k in range(NB):
                row = row - ahead[i][k] * right[k]
            after.append(row)
        for k in range(NB):
            rpan[pl.ds(k, 8, stride=NB), :] = right[k]
        return tuple(after)

    def trail(base):
        inside = (lane >= base) & (lane < base + NB)
        rows = [rpan[m * NB : (m + 1) * NB, :] for m in range(N)]
        ups = []
        for m in range(N):
            r0, r1, r2 = split3(rows[m])
            ups.append(jnp.dot(turned[m], jnp.concatenate([r0, r1, r0, r1, r2, r0], axis=0),
                               preferred_element_type=f32))
        new = [jnp.where(inside[0:1, :], 0.0, mats[m * ST : m * ST + B, :]) - ups[m] for m in range(N)]
        for m in range(N):
            mats[m * ST : m * ST + B, :] = new[m]
        for m in range(N):
            mats[pl.ds(pl.multiple_of(m * ST + base, 8), 8), :] = rows[m]

    def step(b, rows):
        trail((b - 1) * NB)
        return pivot(rows, b * NB)

    rows = pivot(packed(0), 0)
    lax.fori_loop(1, B // NB, step, rows)
    trail(B - NB)


def kernel(links_in, load, factors, shift_in, x_out, r_out, links, shift, fac, rem, lm, rlm, mats, rpan, cpan, turned, dpan, errs, wts, pre, ext,
           pre_u, push, qdir, zdir, res, dirn, along, img, dsend, drecv, lsem, fsend, frecv, hsend, hrecv, ssend, srecv, known,
           tsend, trecv, tsems):
    case = lax.axis_index("case")
    gx = lax.axis_index("gx")
    gy = lax.axis_index("gy")
    me = gx * GYN + gy

    def device(x, y):
        return (case, x, y)

    def exists(sx, sy):
        ok = None
        for pos, step, count in ((gx, sx, GXN), (gy, sy, GYN)):
            if step == 0:
                continue
            here = (pos + step >= 0) & (pos + step < count)
            ok = here if ok is None else ok & here
        return ok

    barrier = pltpu.get_barrier_semaphore()
    peers = []
    hops = lambda a, c: -(min((a + 1) // 2, (GXN - a + 1) // 2) + min(c, GYN - c))
    for a, c in sorted([(a, c) for a in range(GXN) for c in range(GYN)], key=lambda t: hops(*t)):
        if a or c:
            peers.append(device(lax.rem(gx + a, GXN), lax.rem(gy + c, GYN)))

    def ring(dx, dy):
        return device(lax.rem(gx + dx + GXN, GXN), lax.rem(gy + dy + GYN, GYN))

    greeted = [ring(1, 0), ring(-1, 0), ring(0, 1), ring(0, -1)]
    rounds = [greeted, [ring(2, 0), ring(-2, 0), ring(0, 2)], [ring(d, 0) for d in range(1, GXN)]]
    for peer in greeted:
        pl.semaphore_signal(barrier, inc=1, device_id=peer, device_id_type=pl.DeviceIdType.MESH)

    def tell(i):
        for peer in rounds[i]:
            pl.semaphore_signal(known.at[i], inc=1, device_id=peer, device_id_type=pl.DeviceIdType.MESH)

    def hear(i):
        pl.semaphore_wait(known.at[i], len(rounds[i]))

    copies = [
        pltpu.make_async_copy(factors, fac, lsem.at[0]),
        pltpu.make_async_copy(links_in, links, lsem.at[1]),
        pltpu.make_async_copy(shift_in, shift, lsem.at[2]),
        pltpu.make_async_copy(load, res, lsem.at[3]),
    ]
    for copy in copies:
        copy.start()
    copies[1].wait()
    for d in range(4):
        for j in range(N):
            lm[d * N + j : d * N + j + 1, :] = jnp.full((1, B), links[d, 0, j], jnp.int32).astype(f32) * (1.0 / B)
    copies[0].wait()

    def remote(src, dst, ss, rs, sx, sy):
        return pltpu.make_async_remote_copy(
            src_ref=src, dst_ref=dst, send_sem=ss, recv_sem=rs,
            device_id=device(gx + sx, gy + sy), device_id_type=pl.DeviceIdType.MESH)

    moves = (
        (1, 1, ((17, 1, 6),), 1),
        (1, -1, ((18, 1, 17),), 2),
        (0, 1, ((11, 1, 18),), 3),
        (1, 0, ((0, 6, 0), (12, 5, 7), (19, 5, 12)), 0),
    )

    def rim_copies(sx, sy, blocks, n, low=0, high=4):
        parts = [(lm, rlm.at[n], n * 4 + 3)]
        for i, (src, count, dst) in enumerate(blocks):
            parts.append((fac.at[pl.ds(src, count)], rem.at[pl.ds(dst, count)], n * 4 + i))
        return [remote(src, dst, fsend.at[i], frecv.at[i], sx, sy) for src, dst, i in parts[low:high]]

    def depart(n, low, high):
        sx, sy, _, _ = moves[n]
        @pl.when(exists(sx, sy))
        def _():
            for copy in rim_copies(*moves[n], low, high):
                copy.start()

    copies[2].wait()

    def square(block):
        return lax.dot_general(block, block, (((1,), (1,)), ((), ())), preferred_element_type=f32)

    def place(j, slot, s):
        a, b = split2(s)
        wts[j, slot * B : (slot + 1) * B, 0:B] = a
        wts[j, slot * B : (slot + 1) * B, B : 2 * B] = b
        return a.astype(f32) + b.astype(f32)

    row_id = lax.broadcasted_iota(jnp.int32, (B, B), 0)
    lane_id = lax.broadcasted_iota(jnp.int32, (B, B), 1)
    eye = row_id == lane_id

    for m in range(N):
        mats[m * ST : m * ST + B, :] = jnp.where(eye, shift[m], 0.0)
    for m in range(N, 8):
        mats[m * ST : m * ST + B, :] = jnp.where(eye, 1.0, 0.0)

    def ahead(n):
        return remote(tsend.at[n], trecv.at[n], tsems.at[0, n], tsems.at[1, n], 1, 0)

    quarter = B // 4
    lane_q = lax.broadcasted_iota(jnp.int32, (quarter, B), 1)
    lane_h = lax.broadcasted_iota(jnp.int32, (quarter // 2, B), 1)
    above = row_id // quarter <= lane_id // quarter

    def own(j, d):
        s = place(j, d, square(fac[d * N + j]) * lm[d * N + j : d * N + j + 1, :])
        mats[j * ST : j * ST + B, :] = mats[j * ST : j * ST + B, :] + s
        return s

    def send_ahead(n, t):
        q = [t[k * quarter : (k + 1) * quarter] for k in range(4)]
        tsend[n, 0:quarter, :] = q[0]
        tsend[n, quarter : 2 * quarter, :] = jnp.where(lane_q < quarter, pltpu.roll(q[3], quarter, 1), q[1])
        tsend[n, 2 * quarter :, :] = jnp.where(
            lane_h < 2 * quarter, pltpu.roll(q[2][: quarter // 2], 2 * quarter, 1), q[2][quarter // 2 :])

    def unpack(n):
        p0, p1, p2 = trecv[n, 0:quarter, :], trecv[n, quarter : 2 * quarter, :], trecv[n, 2 * quarter :, :]
        upper = jnp.concatenate(
            [p0, p1, pltpu.roll(p2, 2 * quarter, 1), p2, pltpu.roll(p1, 3 * quarter, 1)], axis=0)
        return jnp.where(above, upper, upper.T)

    def arrived(n, low, high):
        sx, sy, _, _ = moves[n]
        @pl.when(exists(-sx, -sy))
        def _():
            for copy in rim_copies(*moves[n], low, high):
                copy.wait_recv()

    def term(j, slot, block, scale):
        return j, place(j, slot, square(rem[block]) * scale)

    def collect(terms):
        for j, s in terms:
            mats[j * ST : j * ST + B, :] = mats[j * ST : j * ST + B, :] + s

    def first(n):
        t = own(n, 0)
        if n > 0:
            t = t + own(n - 1, 2)
        if n < N - 1:
            t = t + own(n + 1, 3)
        send_ahead(n, t)

    early = 2
    for n in range(early):
        first(n)
    pl.semaphore_wait(barrier, len(greeted))
    for n in range(early):
        pl.when(exists(1, 0))(ahead(n).start)
    depart(2, 0, 2)
    tell(0)
    for n in range(early, N):
        first(n)
        pl.when(exists(1, 0))(ahead(n).start)
        if n == early:
            hear(0)
            depart(0, 0, 2)
            depart(1, 0, 2)
            tell(1)
    depart(3, 0, 4)
    hear(1)
    tell(2)
    own(N - 1, 2)
    own(0, 3)
    for j in range(N):
        t = own(j, 1)
        if j < N - 1:
            place(j + 1, 5, t)
            mats[(j + 1) * ST : (j + 1) * ST + B, :] = mats[(j + 1) * ST : (j + 1) * ST + B, :] + t

    def clear(ref, *spans):
        for span in spans:
            ref[span] = jnp.zeros_like(ref[span])

    @pl.when(gx == 0)
    def _():
        clear(ext, (slice(None), 0))
        clear(rem, slice(0, 3 * N))
        clear(rlm, slice(0, 3))
        clear(trecv, slice(None))

    @pl.when(gx == GXN - 1)
    def _():
        clear(ext, (slice(None), 2))

    @pl.when(gy == 0)
    def _():
        clear(ext, (slice(None), slice(None), 0))
        clear(rem, N, 3 * N)
        clear(rlm, 1, 3)

    @pl.when(gy == GYN - 1)
    def _():
        clear(ext, (slice(None), slice(None), N + 1))
        clear(rem, 3 * N - 1)
        clear(rlm, 2)

    arrived(2, 0, 2)
    arrived(0, 0, 2)
    arrived(1, 0, 2)
    collect([
        term(0, 6, N, rlm[1, 3 * N - 1 : 3 * N, :]),
        term(N - 1, 7, 3 * N - 1, rlm[2, 3 * N : 3 * N + 1, :]),
        term(0, 5, 3 * N, rlm[3, 2 * N - 1 : 2 * N, :]),
    ])

    for n in range(N):
        pl.when(exists(-1, 0))(ahead(n).wait_recv)
    for n in range(N):
        mats[n * ST : n * ST + B, :] = mats[n * ST : n * ST + B, :] + unpack(n)

    for m in range(N):
        a, b, c = split3(mats[m * ST : m * ST + B, :])
        dpan[m, 0:B, 0:B] = a
        dpan[m, 0:B, B : 2 * B] = b
        dpan[m, B : 2 * B, 0:B] = b
        dpan[m, B : 2 * B, B : 2 * B] = a
        dpan[m, 0:B, 2 * B :] = a
        dpan[m, B : 2 * B, 2 * B :] = c
    invert(mats, rpan, cpan, turned)
    hear(2)

    def pairs(terms):
        return jnp.concatenate([jnp.concatenate([t, t], axis=1) for t in terms], axis=0)

    def fold(out, h):
        small = (out[2 * h :, 0:B] + out[2 * h :, B:]) + out[h : 2 * h, B:]
        return out[0:h, 0:B] + (out[h : 2 * h, 0:B] + (out[0:h, B:] + small))

    for m in range(N):
        a, b, c = split3(mats[m * ST : m * ST + B, :])
        pre[m, 0:B, 0:B] = a
        pre[m, 0:B, B : 2 * B] = b
        large = jnp.dot(jnp.concatenate([a, b], axis=1), dpan[m, :, 0 : 2 * B], preferred_element_type=f32)
        small = jnp.dot(jnp.concatenate([c, a], axis=1), dpan[m, :, 2 * B :], preferred_element_type=f32)
        product = (small + large[:, B:]) + large[:, 0:B]
        errs[m] = (jnp.where(eye, 1.0, 0.0) - product).astype(bf16)
    better = []
    for m in range(N):
        fix = jnp.dot(errs[m], pre[m, 0:B, :], preferred_element_type=f32)
        better.append(mats[m * ST : m * ST + B, :] + (fix[:, 0:B] + fix[:, B:]))
    for m in range(N):
        a, b, c = split3(better[m])
        pre[m, 0:B, 0:B] = a
        pre[m, 0:B, B : 2 * B] = b
        pre[m, B : 2 * B, 0:B] = c
        pre[m, B : 2 * B, B : 2 * B] = jnp.zeros((B, B), bf16)

    for ref in (x_out, dirn, along, qdir, zdir):
        ref[...] = jnp.zeros_like(ref)
    copies[3].wait()

    def precondition(v, m):
        return fold(jnp.dot(pairs(split3(v)), pre[m], preferred_element_type=f32), R)

    def operate(par, j):
        centre = ext[par, 1, 1 + j]
        terms = []
        for sign in (1, -1):
            for sx, sy in OFFSETS:
                terms.append(split3(centre - ext[par, 1 + sign * sx, 1 + j + sign * sy]))
        left = jnp.concatenate(
            [jnp.concatenate([t[i] for t in terms], axis=1) for i in range(3)], axis=0)
        out = fold(jnp.dot(left, wts[j], preferred_element_type=f32), R)
        return out + shift[j] * centre

    def halo(par, part=None):
        n = 0
        for sx, sy in SIDES:
            if sy == 0:
                pieces = [(pl.ds(1 + low, high - low), pl.ds(1 + low, high - low)) for low, high in ((0, CUT), (CUT, N))]
            else:
                pieces = [(N if sy == 1 else 1, 0 if sy == 1 else N + 1)]
            for k, (src, dst) in enumerate(pieces):
                if part is None or part == k:
                    yield sx, sy, remote(ext.at[par, 1, src], ext.at[par, 1 - sx, dst],
                                         hsend.at[n], hrecv.at[par, n], sx, sy)
                n += 1

    def halo_start(par):
        for part in range(2):
            for sx, sy, copy in halo(par, part):
                pl.when(exists(sx, sy))(copy.start)

    def halo_wait(par, part):
        for sx, sy, copy in halo(par, part):
            pl.when(exists(-sx, -sy))(copy.wait_recv)

    def halo_sent(par):
        for sx, sy, copy in halo(par):
            pl.when(exists(sx, sy))(copy.wait_send)

    def apply(par, out):
        halo_wait(par, 0)
        for j in range(CUT - 1):
            out[j] = operate(par, j)
        halo_wait(par, 1)
        for j in range(CUT - 1, N):
            out[j] = operate(par, j)

    lane = lax.broadcasted_iota(jnp.int32, (R, B), 1)
    rhs = lax.broadcasted_iota(jnp.int32, (R, B), 0)

    def contribution(par, peer):
        return pltpu.make_async_remote_copy(
            src_ref=dsend.at[pl.ds(par, 1)], dst_ref=drecv.at[par, pl.ds(me, 1)],
            send_sem=ssend, recv_sem=srecv.at[par],
            device_id=peer, device_id_type=pl.DeviceIdType.MESH)

    def scatter(par, sums):
        spread = 0.0
        for k, t in reversed(list(enumerate(sums))):
            spread = jnp.where(lane == rhs + k * R, jnp.sum(t, axis=1, keepdims=True), spread)
        row = jnp.sum(spread, axis=0, keepdims=True)
        dsend[pl.ds(par, 1), :] = row
        drecv[par, pl.ds(me, 1), :] = row
        for peer in peers:
            contribution(par, peer).start()

    def gather(par, count):
        everything = drecv.at[par, pl.ds(0, PLANE - 1)]
        pltpu.make_async_copy(everything, everything, srecv.at[par]).wait()
        pltpu.make_async_copy(everything, everything, ssend).wait()
        total = jnp.sum(drecv[par], axis=0, keepdims=True)
        return [jnp.sum(jnp.where(lane == rhs + k * R, total, 0.0), axis=1, keepdims=True) for k in range(count)]

    def products(par, triples):
        gsum, dsum = None, None
        for r, u, w in triples:
            g, d = u * r, u * w
            gsum = g if gsum is None else gsum + g
            dsum = d if dsum is None else dsum + d
        scatter(par, [gsum, dsum])

    def totals(par, first, gamma_old, alpha_old):
        gamma, delta = gather(par, 2)
        ratio = jnp.where(first, 0.0, gamma / gamma_old)
        alpha = gamma / (delta - ratio * gamma / alpha_old)
        return gamma, ratio, alpha

    for j in range(N):
        ext[1, 1, 1 + j] = precondition(res[0, j], j)
    halo_start(1)
    arrived(3, 0, 2)
    for j in range(N):
        term(j, 4, j, rlm[0, j : j + 1, :])
    arrived(3, 2, 3)
    for j in range(1, N):
        term(j, 6, N + j, rlm[0, 2 * N + j - 1 : 2 * N + j, :])
    arrived(3, 3, 4)
    for j in range(N - 1):
        term(j, 7, 2 * N + j, rlm[0, 3 * N + j + 1 : 3 * N + j + 2, :])
    apply(1, img)
    for j in range(N):
        pre_u[j] = ext[1, 1, 1 + j]
    halo_sent(1)

    products(0, [(res[0, j], pre_u[j], img[j]) for j in range(N)])
    for sx, sy, blocks, n in moves:
        @pl.when(exists(sx, sy))
        def _():
            for copy in rim_copies(sx, sy, blocks, n):
                copy.wait_send()
    for n in range(N):
        pl.when(exists(1, 0))(ahead(n).wait_send)

    def iterate(it, carry):
        gamma_old, alpha_old = carry
        par = lax.rem(it, 2)
        for j in range(N):
            ext[par, 1, 1 + j] = precondition(img[j], j)
        halo_start(par)
        apply(par, push)
        gamma, ratio, alpha = totals(par, it == 0, gamma_old, alpha_old)
        triples = []
        for j in range(N):
            u, w = pre_u[j], img[j]
            z = push[j] + ratio * zdir[j]
            q = ext[par, 1, 1 + j] + ratio * qdir[j]
            s = w + ratio * along[j]
            p = u + ratio * dirn[j]
            zdir[j], qdir[j], along[j], dirn[j] = z, q, s, p
            r = res[0, j] - alpha * s
            u = u - alpha * q
            w = w - alpha * z
            res[0, j], pre_u[j], img[j] = r, u, w
            triples.append((r, u, w))
        products(1 - par, triples)
        for j in range(N):
            x_out[0, j] = x_out[0, j] + alpha * dirn[j]
        halo_sent(par)
        return gamma, alpha

    one = jnp.ones((R, 1), f32)
    gamma_old, alpha_old = lax.fori_loop(0, ITERS - 1, iterate, (one, one))
    gamma, ratio, alpha = totals((ITERS - 1) % 2, ITERS == 1, gamma_old, alpha_old)
    for j in range(N):
        x_out[0, j] = x_out[0, j] + alpha * (pre_u[j] + ratio * dirn[j])
        r_out[0, j] = res[0, j] - alpha * (img[j] + ratio * along[j])


def local(load, factors, links, shift):
    vmem = pl.BlockSpec(memory_space=pltpu.VMEM)
    hbm = pl.BlockSpec(memory_space=pltpu.HBM)
    field = jax.ShapeDtypeStruct((1, N, R, B), f32)
    return pl.pallas_call(
        kernel,
        out_shape=(field, field),
        in_specs=[hbm] * 4,
        out_specs=(vmem, vmem),
        scratch_shapes=[
            pltpu.SMEM((4, 1, N), jnp.int32),
            pltpu.VMEM((N, 1, B), f32),
            pltpu.VMEM((4 * N, B, B), bf16),
            pltpu.VMEM((3 * N + 1, B, B), bf16),
            pltpu.VMEM((4 * N, B), f32),
            pltpu.VMEM((4, 4 * N, B), f32),
            pltpu.VMEM((8 * ST, B), f32),
            pltpu.VMEM((8 * NB, B), f32),
            pltpu.VMEM((8 * NB, B), f32),
            pltpu.VMEM((N, B, 6 * NB), bf16),
            pltpu.VMEM((N, 2 * B, 3 * B), bf16),
            pltpu.VMEM((N, B, B), bf16),
            pltpu.VMEM((N, 8 * B, 2 * B), bf16),
            pltpu.VMEM((N, 2 * B, 2 * B), bf16),
            pltpu.VMEM((2, 3, N + 2, R, B), f32),
            pltpu.VMEM((N, R, B), f32),
            pltpu.VMEM((N, R, B), f32),
            pltpu.VMEM((N, R, B), f32),
            pltpu.VMEM((N, R, B), f32),
            pltpu.VMEM((1, N, R, B), f32),
            pltpu.VMEM((N, R, B), f32),
            pltpu.VMEM((N, R, B), f32),
            pltpu.VMEM((N, R, B), f32),
            pltpu.VMEM((8, B), f32),
            pltpu.VMEM((2, PLANE, B), f32),
            pltpu.SemaphoreType.DMA((4,)),
            pltpu.SemaphoreType.DMA((16,)),
            pltpu.SemaphoreType.DMA((16,)),
            pltpu.SemaphoreType.DMA((10,)),
            pltpu.SemaphoreType.DMA((2, 10)),
            pltpu.SemaphoreType.DMA,
            pltpu.SemaphoreType.DMA((2,)),
            pltpu.SemaphoreType.REGULAR((3,)),
            pltpu.VMEM((N, 5 * B // 8, B), f32),
            pltpu.VMEM((N, 5 * B // 8, B), f32),
            pltpu.SemaphoreType.DMA((2, N)),
        ],
        compiler_params=pltpu.CompilerParams(collective_id=0, has_side_effects=True, vmem_limit_bytes=24 * 1024 * 1024),
        name="solve",
    )(*[pltpu.with_memory_space_constraint(t, pltpu.HBM) for t in (links, load, factors.reshape(4 * N, B, B), shift.reshape(N, 1, B))])


def solution(mesh):
    placed = (
        P(("case", "gx"), "gy", None, None),
        P(None, ("case", "gx"), "gy", None, None),
        P(None, ("case", "gx"), "gy"),
        P(("case", "gx"), "gy", None),
    )
    return jax.shard_map(
        local,
        mesh=mesh,
        in_specs=placed,
        out_specs=(P(("case", "gx"), "gy", None, None), P(("case", "gx"), "gy", None, None)),
        check_vma=False,
    )
```

```python
import functools

import jax
import jax.numpy as jnp
from jax import lax
from jax.experimental import pallas as pl
from jax.experimental.pallas import tpu as pltpu
from jax.sharding import PartitionSpec as P

B = 128
N = 6
R = 32
ITERS = 8
NB = 8
ST = 136
GXN = 8
GYN = 4
PLANE = GXN * GYN
CUT = 3
OFFSETS = ((1, 0), (0, 1), (1, 1), (1, -1))
SIDES = ((1, 1), (1, -1), (-1, 1), (-1, -1), (1, 0), (-1, 0), (0, 1), (0, -1))
f32 = jnp.float32
bf16 = jnp.bfloat16


def split3(x):
    a = x.astype(bf16)
    left = x - a.astype(f32)
    b = left.astype(bf16)
    c = (left - b.astype(f32)).astype(bf16)
    return a, b, c


def split2(x):
    a = x.astype(bf16)
    return a, (x - a.astype(f32)).astype(bf16)


def invert(mats, rpan, cpan, turned):
    lane = lax.broadcasted_iota(jnp.int32, (8, B), 1)

    def packed(base):
        return [mats[pl.ds(base + i, 8, stride=ST), :] for i in range(NB)]

    def pick(row, k):
        return jnp.sum(jnp.where(lane == k, row, 0.0), axis=1, keepdims=True)

    def pivot(rows, base):
        e = {}
        for j in range(NB):
            for i in range(j + 1):
                e[i, j] = pick(rows[i], base + j)
        ahead = [[pick(rows[k], base + NB + i) for k in range(NB)] for i in range(NB)]
        inside = (lane >= base) & (lane < base + NB)
        sign = jnp.where(lane < base, -1.0, jnp.where(inside, 0.0, 1.0))
        for k in range(NB):
            cpan[pl.ds(k, 8, stride=NB), :] = rows[k] * sign
        for m in range(N):
            c0, c1, c2 = split3(cpan[m * NB : (m + 1) * NB, :])
            turned[m] = jnp.concatenate([c0, c0, c1, c1, c0, c2], axis=0).T
        at = lambda i, j: e[min(i, j), max(i, j)]
        for k in range(NB):
            p = 1.0 / e[k, k]
            col = [at(i, k) for i in range(NB)]
            scaled = [c * p for c in col]
            for i in range(NB):
                for j in range(i, NB):
                    if i != k and j != k:
                        e[i, j] = e[i, j] - scaled[i] * col[j]
            for i in range(NB):
                if i != k:
                    e[min(i, k), max(i, k)] = scaled[i]
            e[k, k] = -p
        panel = [jnp.where(lane == base + i, 1.0, jnp.where(inside, 0.0, rows[i])) for i in range(NB)]
        right = []
        for j in range(NB):
            total = None
            for i in range(NB):
                term = at(i, j) * panel[i]
                total = term if total is None else total + term
            right.append(-total)
        following = packed(jnp.minimum(base + NB, B - NB))
        after = []
        for i in range(NB):
            row = jnp.where(inside, 0.0, following[i])
            for k in range(NB):
                row = row - ahead[i][k] * right[k]
            after.append(row)
        for k in range(NB):
            rpan[pl.ds(k, 8, stride=NB), :] = right[k]
        return tuple(after)

    def trail(base):
        inside = (lane >= base) & (lane < base + NB)
        rows = [rpan[m * NB : (m + 1) * NB, :] for m in range(N)]
        ups = []
        for m in range(N):
            r0, r1, r2 = split3(rows[m])
            ups.append(jnp.dot(turned[m], jnp.concatenate([r0, r1, r0, r1, r2, r0], axis=0),
                               preferred_element_type=f32))
        new = [jnp.where(inside[0:1, :], 0.0, mats[m * ST : m * ST + B, :]) - ups[m] for m in range(N)]
        for m in range(N):
            mats[m * ST : m * ST + B, :] = new[m]
        for m in range(N):
            mats[pl.ds(pl.multiple_of(m * ST + base, 8), 8), :] = rows[m]

    def step(b, rows):
        trail((b - 1) * NB)
        return pivot(rows, b * NB)

    rows = pivot(packed(0), 0)
    lax.fori_loop(1, B // NB, step, rows)
    trail(B - NB)


def kernel(links_in, load, factors, shift_in, x_out, r_out, links, shift, fac, rem, lm, rlm, mats, rpan, cpan, turned, dpan, errs, wts, pre, ext,
           pre_u, push, qdir, zdir, res, dirn, along, img, dsend, drecv, lsem, fsend, frecv, hsend, hrecv, ssend, srecv, known,
           tsend, trecv, tsems):
    case = lax.axis_index("case")
    gx = lax.axis_index("gx")
    gy = lax.axis_index("gy")
    me = gx * GYN + gy

    def device(x, y):
        return (case, x, y)

    def exists(sx, sy):
        ok = None
        for pos, step, count in ((gx, sx, GXN), (gy, sy, GYN)):
            if step == 0:
                continue
            here = (pos + step >= 0) & (pos + step < count)
            ok = here if ok is None else ok & here
        return ok

    barrier = pltpu.get_barrier_semaphore()
    peers = []
    hops = lambda a, c: -(min((a + 1) // 2, (GXN - a + 1) // 2) + min(c, GYN - c))
    for a, c in sorted([(a, c) for a in range(GXN) for c in range(GYN)], key=lambda t: hops(*t)):
        if a or c:
            peers.append(device(lax.rem(gx + a, GXN), lax.rem(gy + c, GYN)))

    def ring(dx, dy):
        return device(lax.rem(gx + dx + GXN, GXN), lax.rem(gy + dy + GYN, GYN))

    greeted = [ring(1, 0), ring(-1, 0), ring(0, 1), ring(0, -1)]
    rounds = [greeted, [ring(2, 0), ring(-2, 0), ring(0, 2)], [ring(d, 0) for d in range(1, GXN)]]
    for peer in greeted:
        pl.semaphore_signal(barrier, inc=1, device_id=peer, device_id_type=pl.DeviceIdType.MESH)

    def tell(i):
        for peer in rounds[i]:
            pl.semaphore_signal(known.at[i], inc=1, device_id=peer, device_id_type=pl.DeviceIdType.MESH)

    def hear(i):
        pl.semaphore_wait(known.at[i], len(rounds[i]))

    copies = [
        pltpu.make_async_copy(factors, fac, lsem.at[0]),
        pltpu.make_async_copy(links_in, links, lsem.at[1]),
        pltpu.make_async_copy(shift_in, shift, lsem.at[2]),
        pltpu.make_async_copy(load, res, lsem.at[3]),
    ]
    for copy in copies:
        copy.start()
    copies[1].wait()
    for d in range(4):
        for j in range(N):
            lm[d * N + j : d * N + j + 1, :] = jnp.full((1, B), links[d, 0, j], jnp.int32).astype(f32) * (1.0 / B)
    copies[0].wait()

    def remote(src, dst, ss, rs, sx, sy):
        return pltpu.make_async_remote_copy(
            src_ref=src, dst_ref=dst, send_sem=ss, recv_sem=rs,
            device_id=device(gx + sx, gy + sy), device_id_type=pl.DeviceIdType.MESH)

    moves = (
        (1, 1, ((17, 1, 6),), 1),
        (1, -1, ((18, 1, 17),), 2),
        (0, 1, ((11, 1, 18),), 3),
        (1, 0, ((0, 6, 0), (12, 5, 7), (19, 5, 12)), 0),
    )

    def rim_copies(sx, sy, blocks, n, low=0, high=4):
        parts = [(lm, rlm.at[n], n * 4 + 3)]
        for i, (src, count, dst) in enumerate(blocks):
            parts.append((fac.at[pl.ds(src, count)], rem.at[pl.ds(dst, count)], n * 4 + i))
        return [remote(src, dst, fsend.at[i], frecv.at[i], sx, sy) for src, dst, i in parts[low:high]]

    def depart(n, low, high):
        sx, sy, _, _ = moves[n]
        @pl.when(exists(sx, sy))
        def _():
            for copy in rim_copies(*moves[n], low, high):
                copy.start()

    copies[2].wait()

    def square(block):
        return lax.dot_general(block, block, (((1,), (1,)), ((), ())), preferred_element_type=f32)

    def place(j, slot, s):
        a, b = split2(s)
        wts[j, slot * B : (slot + 1) * B, 0:B] = a
        wts[j, slot * B : (slot + 1) * B, B : 2 * B] = b
        return a.astype(f32) + b.astype(f32)

    row_id = lax.broadcasted_iota(jnp.int32, (B, B), 0)
    lane_id = lax.broadcasted_iota(jnp.int32, (B, B), 1)
    eye = row_id == lane_id

    for m in range(N):
        mats[m * ST : m * ST + B, :] = jnp.where(eye, shift[m], 0.0)
    for m in range(N, 8):
        mats[m * ST : m * ST + B, :] = jnp.where(eye, 1.0, 0.0)

    def ahead(n):
        return remote(tsend.at[n], trecv.at[n], tsems.at[0, n], tsems.at[1, n], 1, 0)

    quarter = B // 4
    lane_q = lax.broadcasted_iota(jnp.int32, (quarter, B), 1)
    lane_h = lax.broadcasted_iota(jnp.int32, (quarter // 2, B), 1)
    above = row_id // quarter <= lane_id // quarter

    def own(j, d):
        s = place(j, d, square(fac[d * N + j]) * lm[d * N + j : d * N + j + 1, :])
        mats[j * ST : j * ST + B, :] = mats[j * ST : j * ST + B, :] + s
        return s

    def send_ahead(n, t):
        q = [t[k * quarter : (k + 1) * quarter] for k in range(4)]
        tsend[n, 0:quarter, :] = q[0]
        tsend[n, quarter : 2 * quarter, :] = jnp.where(lane_q < quarter, pltpu.roll(q[3], quarter, 1), q[1])
        tsend[n, 2 * quarter :, :] = jnp.where(
            lane_h < 2 * quarter, pltpu.roll(q[2][: quarter // 2], 2 * quarter, 1), q[2][quarter // 2 :])

    def unpack(n):
        p0, p1, p2 = trecv[n, 0:quarter, :], trecv[n, quarter : 2 * quarter, :], trecv[n, 2 * quarter :, :]
        upper = jnp.concatenate(
            [p0, p1, pltpu.roll(p2, 2 * quarter, 1), p2, pltpu.roll(p1, 3 * quarter, 1)], axis=0)
        return jnp.where(above, upper, upper.T)

    def arrived(n, low, high):
        sx, sy, _, _ = moves[n]
        @pl.when(exists(-sx, -sy))
        def _():
            for copy in rim_copies(*moves[n], low, high):
                copy.wait_recv()

    def term(j, slot, block, scale):
        return j, place(j, slot, square(rem[block]) * scale)

    def collect(terms):
        for j, s in terms:
            mats[j * ST : j * ST + B, :] = mats[j * ST : j * ST + B, :] + s

    def first(n):
        t = own(n, 0)
        if n > 0:
            t = t + own(n - 1, 2)
        if n < N - 1:
            t = t + own(n + 1, 3)
        send_ahead(n, t)

    early = 2
    for n in range(early):
        first(n)
    pl.semaphore_wait(barrier, len(greeted))
    for n in range(early):
        pl.when(exists(1, 0))(ahead(n).start)
    depart(2, 0, 2)
    tell(0)
    for n in range(early, N):
        first(n)
        pl.when(exists(1, 0))(ahead(n).start)
        if n == early:
            hear(0)
            depart(0, 0, 2)
            depart(1, 0, 2)
            tell(1)
    depart(3, 0, 4)
    hear(1)
    tell(2)
    own(N - 1, 2)
    own(0, 3)
    for j in range(N):
        t = own(j, 1)
        if j < N - 1:
            place(j + 1, 5, t)
            mats[(j + 1) * ST : (j + 1) * ST + B, :] = mats[(j + 1) * ST : (j + 1) * ST + B, :] + t

    def clear(ref, *spans):
        for span in spans:
            ref[span] = jnp.zeros_like(ref[span])

    @pl.when(gx == 0)
    def _():
        clear(ext, (slice(None), 0))
        clear(rem, slice(0, 3 * N))
        clear(rlm, slice(0, 3))
        clear(trecv, slice(None))

    @pl.when(gx == GXN - 1)
    def _():
        clear(ext, (slice(None), 2))

    @pl.when(gy == 0)
    def _():
        clear(ext, (slice(None), slice(None), 0))
        clear(rem, N, 3 * N)
        clear(rlm, 1, 3)

    @pl.when(gy == GYN - 1)
    def _():
        clear(ext, (slice(None), slice(None), N + 1))
        clear(rem, 3 * N - 1)
        clear(rlm, 2)

    arrived(2, 0, 2)
    arrived(0, 0, 2)
    arrived(1, 0, 2)
    collect([
        term(0, 6, N, rlm[1, 3 * N - 1 : 3 * N, :]),
        term(N - 1, 7, 3 * N - 1, rlm[2, 3 * N : 3 * N + 1, :]),
        term(0, 5, 3 * N, rlm[3, 2 * N - 1 : 2 * N, :]),
    ])

    for n in range(N):
        pl.when(exists(-1, 0))(ahead(n).wait_recv)
    for n in range(N):
        mats[n * ST : n * ST + B, :] = mats[n * ST : n * ST + B, :] + unpack(n)

    for m in range(N):
        a, b, c = split3(mats[m * ST : m * ST + B, :])
        dpan[m, 0:B, 0:B] = a
        dpan[m, 0:B, B : 2 * B] = b
        dpan[m, B : 2 * B, 0:B] = b
        dpan[m, B : 2 * B, B : 2 * B] = a
        dpan[m, 0:B, 2 * B :] = a
        dpan[m, B : 2 * B, 2 * B :] = c
    invert(mats, rpan, cpan, turned)
    hear(2)

    def pairs(terms):
        return jnp.concatenate([jnp.concatenate([t, t], axis=1) for t in terms], axis=0)

    def fold(out, h):
        small = (out[2 * h :, 0:B] + out[2 * h :, B:]) + out[h : 2 * h, B:]
        return out[0:h, 0:B] + (out[h : 2 * h, 0:B] + (out[0:h, B:] + small))

    for m in range(N):
        a, b, c = split3(mats[m * ST : m * ST + B, :])
        pre[m, 0:B, 0:B] = a
        pre[m, 0:B, B : 2 * B] = b
        large = jnp.dot(jnp.concatenate([a, b], axis=1), dpan[m, :, 0 : 2 * B], preferred_element_type=f32)
        small = jnp.dot(jnp.concatenate([c, a], axis=1), dpan[m, :, 2 * B :], preferred_element_type=f32)
        product = (small + large[:, B:]) + large[:, 0:B]
        errs[m] = (jnp.where(eye, 1.0, 0.0) - product).astype(bf16)
    better = []
    for m in range(N):
        fix = jnp.dot(errs[m], pre[m, 0:B, :], preferred_element_type=f32)
        better.append(mats[m * ST : m * ST + B, :] + (fix[:, 0:B] + fix[:, B:]))
    for m in range(N):
        a, b, c = split3(better[m])
        pre[m, 0:B, 0:B] = a
        pre[m, 0:B, B : 2 * B] = b
        pre[m, B : 2 * B, 0:B] = c
        pre[m, B : 2 * B, B : 2 * B] = jnp.zeros((B, B), bf16)

    for ref in (x_out, dirn, along, qdir, zdir):
        ref[...] = jnp.zeros_like(ref)
    copies[3].wait()

    def precondition(v, m):
        return fold(jnp.dot(pairs(split3(v)), pre[m], preferred_element_type=f32), R)

    def operate(par, j):
        centre = ext[par, 1, 1 + j]
        terms = []
        for sign in (1, -1):
            for sx, sy in OFFSETS:
                terms.append(split3(centre - ext[par, 1 + sign * sx, 1 + j + sign * sy]))
        left = jnp.concatenate(
            [jnp.concatenate([t[i] for t in terms], axis=1) for i in range(3)], axis=0)
        out = fold(jnp.dot(left, wts[j], preferred_element_type=f32), R)
        return out + shift[j] * centre

    def halo(par, part=None):
        n = 0
        for sx, sy in SIDES:
            if sy == 0:
                pieces = [(pl.ds(1 + low, high - low), pl.ds(1 + low, high - low)) for low, high in ((0, CUT), (CUT, N))]
            else:
                pieces = [(N if sy == 1 else 1, 0 if sy == 1 else N + 1)]
            for k, (src, dst) in enumerate(pieces):
                if part is None or part == k:
                    yield sx, sy, remote(ext.at[par, 1, src], ext.at[par, 1 - sx, dst],
                                         hsend.at[n], hrecv.at[par, n], sx, sy)
                n += 1

    def halo_start(par):
        for part in range(2):
            for sx, sy, copy in halo(par, part):
                pl.when(exists(sx, sy))(copy.start)

    def halo_wait(par, part):
        for sx, sy, copy in halo(par, part):
            pl.when(exists(-sx, -sy))(copy.wait_recv)

    def halo_sent(par):
        for sx, sy, copy in halo(par):
            pl.when(exists(sx, sy))(copy.wait_send)

    def apply(par, out):
        halo_wait(par, 0)
        for j in range(CUT - 1):
            out[j] = operate(par, j)
        halo_wait(par, 1)
        for j in range(CUT - 1, N):
            out[j] = operate(par, j)

    lane = lax.broadcasted_iota(jnp.int32, (R, B), 1)
    rhs = lax.broadcasted_iota(jnp.int32, (R, B), 0)

    def contribution(par, peer):
        return pltpu.make_async_remote_copy(
            src_ref=dsend.at[pl.ds(par, 1)], dst_ref=drecv.at[par, pl.ds(me, 1)],
            send_sem=ssend, recv_sem=srecv.at[par],
            device_id=peer, device_id_type=pl.DeviceIdType.MESH)

    def scatter(par, sums):
        spread = 0.0
        for k, t in reversed(list(enumerate(sums))):
            spread = jnp.where(lane == rhs + k * R, jnp.sum(t, axis=1, keepdims=True), spread)
        row = jnp.sum(spread, axis=0, keepdims=True)
        dsend[pl.ds(par, 1), :] = row
        drecv[par, pl.ds(me, 1), :] = row
        for peer in peers:
            contribution(par, peer).start()

    def gather(par, count):
        everything = drecv.at[par, pl.ds(0, PLANE - 1)]
        pltpu.make_async_copy(everything, everything, srecv.at[par]).wait()
        pltpu.make_async_copy(everything, everything, ssend).wait()
        total = jnp.sum(drecv[par], axis=0, keepdims=True)
        return [jnp.sum(jnp.where(lane == rhs + k * R, total, 0.0), axis=1, keepdims=True) for k in range(count)]

    def products(par, triples):
        gsum, dsum = None, None
        for r, u, w in triples:
            g, d = u * r, u * w
            gsum = g if gsum is None else gsum + g
            dsum = d if dsum is None else dsum + d
        scatter(par, [gsum, dsum])

    def totals(par, first, gamma_old, alpha_old):
        gamma, delta = gather(par, 2)
        ratio = jnp.where(first, 0.0, gamma / gamma_old)
        alpha = gamma / (delta - ratio * (gamma / alpha_old))
        return gamma, ratio, alpha

    for j in range(N):
        ext[1, 1, 1 + j] = precondition(res[0, j], j)
    halo_start(1)
    arrived(3, 0, 2)
    for j in range(N):
        term(j, 4, j, rlm[0, j : j + 1, :])
    arrived(3, 2, 3)
    for j in range(1, N):
        term(j, 6, N + j, rlm[0, 2 * N + j - 1 : 2 * N + j, :])
    arrived(3, 3, 4)
    for j in range(N - 1):
        term(j, 7, 2 * N + j, rlm[0, 3 * N + j + 1 : 3 * N + j + 2, :])
    apply(1, img)
    for j in range(N):
        pre_u[j] = ext[1, 1, 1 + j]
    halo_sent(1)

    products(0, [(res[0, j], pre_u[j], img[j]) for j in range(N)])
    for sx, sy, blocks, n in moves:
        @pl.when(exists(sx, sy))
        def _():
            for copy in rim_copies(sx, sy, blocks, n):
                copy.wait_send()
    for n in range(N):
        pl.when(exists(1, 0))(ahead(n).wait_send)

    def iterate(it, carry):
        gamma_old, alpha_old = carry
        par = lax.rem(it, 2)
        for j in range(N):
            ext[par, 1, 1 + j] = precondition(img[j], j)
        halo_start(par)
        apply(par, push)
        gamma, ratio, alpha = totals(par, it == 0, gamma_old, alpha_old)
        triples = []
        for j in range(N):
            u, w = pre_u[j], img[j]
            z = push[j] + ratio * zdir[j]
            q = ext[par, 1, 1 + j] + ratio * qdir[j]
            s = w + ratio * along[j]
            p = u + ratio * dirn[j]
            zdir[j], qdir[j], along[j], dirn[j] = z, q, s, p
            r = res[0, j] - alpha * s
            u = u - alpha * q
            w = w - alpha * z
            res[0, j], pre_u[j], img[j] = r, u, w
            triples.append((r, u, w))
        products(1 - par, triples)
        for j in range(N):
            x_out[0, j] = x_out[0, j] + alpha * dirn[j]
        halo_sent(par)
        return gamma, alpha

    one = jnp.ones((R, 1), f32)
    gamma_old, alpha_old = lax.fori_loop(0, ITERS - 1, iterate, (one, one))
    gamma, ratio, alpha = totals((ITERS - 1) % 2, ITERS == 1, gamma_old, alpha_old)
    for j in range(N):
        x_out[0, j] = x_out[0, j] + alpha * (pre_u[j] + ratio * dirn[j])
        r_out[0, j] = res[0, j] - alpha * (img[j] + ratio * along[j])


def local(load, factors, links, shift):
    vmem = pl.BlockSpec(memory_space=pltpu.VMEM)
    hbm = pl.BlockSpec(memory_space=pltpu.HBM)
    field = jax.ShapeDtypeStruct((1, N, R, B), f32)
    return pl.pallas_call(
        kernel,
        out_shape=(field, field),
        in_specs=[hbm] * 4,
        out_specs=(vmem, vmem),
        scratch_shapes=[
            pltpu.SMEM((4, 1, N), jnp.int32),
            pltpu.VMEM((N, 1, B), f32),
            pltpu.VMEM((4 * N, B, B), bf16),
            pltpu.VMEM((3 * N + 1, B, B), bf16),
            pltpu.VMEM((4 * N, B), f32),
            pltpu.VMEM((4, 4 * N, B), f32),
            pltpu.VMEM((8 * ST, B), f32),
            pltpu.VMEM((8 * NB, B), f32),
            pltpu.VMEM((8 * NB, B), f32),
            pltpu.VMEM((N, B, 6 * NB), bf16),
            pltpu.VMEM((N, 2 * B, 3 * B), bf16),
            pltpu.VMEM((N, B, B), bf16),
            pltpu.VMEM((N, 8 * B, 2 * B), bf16),
            pltpu.VMEM((N, 2 * B, 2 * B), bf16),
            pltpu.VMEM((2, 3, N + 2, R, B), f32),
            pltpu.VMEM((N, R, B), f32),
            pltpu.VMEM((N, R, B), f32),
            pltpu.VMEM((N, R, B), f32),
            pltpu.VMEM((N, R, B), f32),
            pltpu.VMEM((1, N, R, B), f32),
            pltpu.VMEM((N, R, B), f32),
            pltpu.VMEM((N, R, B), f32),
            pltpu.VMEM((N, R, B), f32),
            pltpu.VMEM((8, B), f32),
            pltpu.VMEM((2, PLANE, B), f32),
            pltpu.SemaphoreType.DMA((4,)),
            pltpu.SemaphoreType.DMA((16,)),
            pltpu.SemaphoreType.DMA((16,)),
            pltpu.SemaphoreType.DMA((10,)),
            pltpu.SemaphoreType.DMA((2, 10)),
            pltpu.SemaphoreType.DMA,
            pltpu.SemaphoreType.DMA((2,)),
            pltpu.SemaphoreType.REGULAR((3,)),
            pltpu.VMEM((N, 5 * B // 8, B), f32),
            pltpu.VMEM((N, 5 * B // 8, B), f32),
            pltpu.SemaphoreType.DMA((2, N)),
        ],
        compiler_params=pltpu.CompilerParams(collective_id=0, has_side_effects=True, vmem_limit_bytes=24 * 1024 * 1024),
        name="solve",
    )(*[pltpu.with_memory_space_constraint(t, pltpu.HBM) for t in (links, load, factors.reshape(4 * N, B, B), shift.reshape(N, 1, B))])


def solution(mesh):
    placed = (
        P(("case", "gx"), "gy", None, None),
        P(None, ("case", "gx"), "gy", None, None),
        P(None, ("case", "gx"), "gy"),
        P(("case", "gx"), "gy", None),
    )
    return jax.shard_map(
        local,
        mesh=mesh,
        in_specs=placed,
        out_specs=(P(("case", "gx"), "gy", None, None), P(("case", "gx"), "gy", None, None)),
        check_vma=False,
    )
```
